256 devices in a mesh: grp: 2 (over y), slab: 16 (over z), blk: 4 (over x), sub: 2 (over core).
Axes of the slice: x: 4, y: 2, z: 16, core: 2. Of those that a mesh axis runs over, the one named last changes fastest.
The devices are a block of a 4x16x16 slice.
Arguments:
- cell_x: int32 [65536], P(('grp', 'slab', 'blk', 'sub')), parts along dimension 0, may hold values from 0 to 63
- cell_y: int32 [65536], P(('grp', 'slab', 'blk', 'sub')), parts along dimension 0, may hold values from 0 to 127
- cell_z: int32 [65536], P(('grp', 'slab', 'blk', 'sub')), parts along dimension 0, may hold values from 0 to 127
- offsets: float32 [3, 65536], P(None, ('grp', 'slab', 'blk', 'sub')), parts along dimension 1, may hold values from 0 to 1
- charge: float32 [65536], P(('grp', 'slab', 'blk', 'sub')), parts along dimension 0, may hold values from -4 to 4
- block_count: int32 [256], P(('grp', 'slab', 'blk', 'sub')), parts along dimension 0, may hold values from 0 to 256, as said below
- level_amplitude: float32 [4], replicated, may hold values from 0.5 to 2
- density: float32 [512, 256, 256], P(('grp', 'slab'), 'blk', 'sub'), parts along dimension 0, may hold values from 0.3 to 8.2
Outputs:
- field: float32 [512, 256, 256], P(('grp', 'slab'), 'blk', 'sub'), parts along dimension 0
- energy: float32 [2], P('grp'), parts along dimension 0
The draws below stay inside these ranges and needn't reach their ends.
There are 2 independent parts, one for each index of `grp`. The reference program is written for one: setup_inputs(seed, part) draws one part's arguments, and reference() takes and returns one part's arrays. A program takes and returns all parts, laid end to end along the dimension named above; an argument that names none is the same for every part. Nothing has to cross between parts.
Inputs may be any that keep to these rules, and one draw needn't show every extreme that they name: `block_count`: within the 1 block of each device, blocks with a nonzero count come before blocks with count 0; some device has every block full.
All inputs are finite; a program needn't handle non-finite values.
Results may differ from the reference program's by a relative error of at most 0.0021.
Values sent between devices are 32-bit elements; how exact they have to be, the bound alone decides.
A program may use at most 64 MiB of HBM per device.

```python
import math
import jax
import jax.numpy as jnp
from jax import lax

G0X = 64
G0Y = 128
G0Z = 128
FINE_X = 256
FINE_Y = 256
FINE_Z = 256
BQ = 256
BLK_DEV = 1
SLOTS = 32768
NBLOCKS = 128


def draw_block_count(key, part):
    devices_part = NBLOCKS // BLK_DEV
    key_used = jax.random.fold_in(key, 11)
    key_counts = jax.random.fold_in(key, 12)
    key_full = jax.random.fold_in(key, 13)
    used = jax.random.randint(key_used, (devices_part, 1), max(1, BLK_DEV - 1), BLK_DEV + 1)
    counts = jax.random.randint(key_counts, (devices_part, BLK_DEV), BQ // 2, BQ + 1)
    busiest = jax.random.randint(key_full, (), 0, devices_part)
    columns = jnp.arange(BLK_DEV, dtype=jnp.int32)[None, :]
    counts = jnp.where(columns < used, counts, 0)
    counts = jnp.where(jnp.arange(devices_part, dtype=jnp.int32)[:, None] == busiest, BQ, counts)
    return counts.reshape(-1).astype(jnp.int32)


def draw_density(key, part):
    positions = jnp.arange(FINE_X, dtype=jnp.float32)[:, None, None]
    rising = 1.0 + 2.0 * positions / (FINE_X - 1)
    base = jnp.exp(jax.random.uniform(jax.random.fold_in(key, 22), (FINE_X, FINE_Y, FINE_Z), jnp.float32, -1.0, 1.0))
    return (base * rising).astype(jnp.float32)


def set_ends(drawn, rng, smallest, largest):
    longest = drawn.shape.index(max(drawn.shape))
    spots = []
    for shift in (0, 1):
        where = [jax.random.randint(jax.random.fold_in(rng, axis), (), 0, length) for axis, length in enumerate(drawn.shape)]
        where[longest] = (where[longest] + shift) % drawn.shape[longest]
        spots.append(tuple(where))
    return drawn.at[spots[0]].set(smallest).at[spots[1]].set(largest)


def shard_levels(own_key, dims, pieces, smallest, largest):
    level = 1.0
    for axis_at, blocks in pieces:
        draws = jax.random.uniform(jax.random.fold_in(jax.random.fold_in(own_key, 6), axis_at), (blocks,), jnp.float32, smallest / len(pieces), largest / len(pieces))
        level = level * jnp.repeat(jnp.exp(draws), dims[axis_at] // blocks).reshape((-1,) + (1,) * (len(dims) - 1 - axis_at))
    return level


def noise(own_key, extent, scale, most, cuts=(), kind=jnp.bfloat16):
    array = scale * jax.random.normal(own_key, extent, jnp.float32)
    if cuts:
        array = array * shard_levels(own_key, extent, cuts, -0.22, 0.18)
    return jnp.clip(array, -most, most).astype(kind)


def setup_inputs(seed: int = 0, part: int = 0) -> dict:
    keys = jax.random.split(jax.random.key(seed), 9)
    part_keys = jax.random.split(jax.random.fold_in(keys[8], part), 9)
    return {
        "cell_x": set_ends(jax.random.randint(part_keys[0], (SLOTS,), 0, G0X), jax.random.fold_in(part_keys[0], 1), 0, G0X - 1).astype(jnp.int32),
        "cell_y": set_ends(jax.random.randint(part_keys[1], (SLOTS,), 0, G0Y), jax.random.fold_in(part_keys[1], 1), 0, G0Y - 1).astype(jnp.int32),
        "cell_z": set_ends(jax.random.randint(part_keys[2], (SLOTS,), 0, G0Z), jax.random.fold_in(part_keys[2], 1), 0, G0Z - 1).astype(jnp.int32),
        "offsets": jnp.clip(1.0 * jax.random.uniform(part_keys[3], (3, SLOTS), jnp.float32) ** shard_levels(part_keys[3], (3, SLOTS), ((1, 128),), -0.2, 0.2), 0.0, 1.0),
        "charge": noise(part_keys[4], (SLOTS,), 1.0, 4.0, ((0, 128),), jnp.float32),
        "block_count": draw_block_count(jax.random.fold_in(jax.random.fold_in(keys[8], part), 71), part),
        "level_amplitude": jnp.clip(jnp.exp(jax.random.uniform(keys[6], (4,), jnp.float32, math.log(0.5), math.log(2.0))), 0.5, 2.0),
        "density": draw_density(jax.random.fold_in(jax.random.fold_in(keys[8], part), 71), part),
    }


spread_width = 1.25


def axis_weights(cells, shifts, base, coarse):
    position = (cells.astype(jnp.float32) + shifts) * (coarse / base)
    nodes = jnp.arange(coarse, dtype=jnp.float32)
    distance = nodes[None, :] - position[:, None]
    distance = distance - coarse * jnp.floor(distance / coarse + 0.5)
    return jnp.exp(-0.5 * (distance / spread_width) ** 2)


def level_dims():
    return [(G0X * (4 - factor) // 4, G0Y * (4 - factor) // 4, G0Z * (4 - factor) // 4) for factor in range(4)]


def spread_block(weighted, cells_x, cells_y, cells_z, shifts):
    totals = []
    for dim_x, dim_y, dim_z in level_dims():
        along_x = axis_weights(cells_x, shifts[0], G0X, dim_x)
        along_y = axis_weights(cells_y, shifts[1], G0Y, dim_y)
        along_z = axis_weights(cells_z, shifts[2], G0Z, dim_z)
        planes = ((weighted[:, None] * along_x)[:, :, None] * along_y[:, None, :]).reshape(weighted.shape[0], dim_x * dim_y).astype(jnp.bfloat16)
        totals.append(lax.dot_general(planes, along_z.astype(jnp.bfloat16), (((0,), (0,)), ((), ())), preferred_element_type=jnp.float32))
    return totals


def hat_matrix(fine, coarse, first_row, rows):
    fine_rows = first_row + jnp.arange(rows, dtype=jnp.int32)
    nodes = jnp.arange(coarse, dtype=jnp.int32)
    period = coarse * fine
    moved = (nodes[None, :] * fine - fine_rows[:, None] * coarse) % period
    moved = jnp.where(moved * 2 >= period, moved - period, moved)
    distance = moved.astype(jnp.float32) / fine
    return jnp.maximum(0.0, 1.0 - jnp.abs(distance))


def interpolate(mat_x, mat_y, mat_z, cube):
    highest = lax.Precision.HIGHEST
    first = jnp.einsum('ax,xyz->ayz', mat_x, cube, precision=highest)
    second = jnp.einsum('by,ayz->abz', mat_y, first, precision=highest)
    return jnp.einsum('cz,abz->abc', mat_z, second, precision=highest)


def reference(cell_x, cell_y, cell_z, offsets, charge, block_count, level_amplitude, density):
    live = (jnp.arange(BQ, dtype=jnp.int32)[None, :] < block_count[:, None]).astype(jnp.float32)
    weighted = charge.reshape(NBLOCKS, BQ) * live
    inputs = (weighted, cell_x.reshape(NBLOCKS, BQ), cell_y.reshape(NBLOCKS, BQ), cell_z.reshape(NBLOCKS, BQ), jnp.transpose(offsets.reshape(3, NBLOCKS, BQ), (1, 0, 2)))
    start = [jnp.zeros((dim_x * dim_y, dim_z), jnp.float32) for dim_x, dim_y, dim_z in level_dims()]

    def advance(totals, item):
        parts = spread_block(*item)
        return [total + part for total, part in zip(totals, parts)], None

    coarse, _ = lax.scan(advance, start, inputs)
    field = jnp.zeros((FINE_X, FINE_Y, FINE_Z), jnp.float32)
    for factor, (dim_x, dim_y, dim_z) in enumerate(level_dims()):
        cube = coarse[factor].reshape(dim_x, dim_y, dim_z)
        mat_x = hat_matrix(FINE_X, dim_x, 0, FINE_X)
        mat_y = hat_matrix(FINE_Y, dim_y, 0, FINE_Y)
        mat_z = hat_matrix(FINE_Z, dim_z, 0, FINE_Z)
        field = field + level_amplitude[factor] * interpolate(mat_x, mat_y, mat_z, cube)
    energy = (jnp.sum(density * field) / (FINE_X * FINE_Y * FINE_Z)).reshape(1)
    return field, energy
```

```python
import functools

import jax
import jax.numpy as jnp
import numpy as np
from jax import lax
from jax.experimental import pallas as pl
from jax.experimental.pallas import tpu as pltpu
from jax.sharding import PartitionSpec as P

G0X = 64
G0Y = 128
G0Z = 128
FINE_X = 256
FINE_Y = 256
FINE_Z = 256
BQ = 256
LEVELS = 4
LANES = 128
HALO = 16
spread_width = 1.25
MESH = pl.DeviceIdType.MESH


def coarse_cells(base, level):
    return base * (4 - level) // 4


class Plan:
    def __init__(self, slabs, cols, rows_x, rows_y, rows_z):
        self.slabs, self.cols = slabs, cols
        self.rows = (rows_x, rows_y, rows_z)
        self.gx = [coarse_cells(G0X, l) for l in range(LEVELS)]
        self.gy = [coarse_cells(G0Y, l) for l in range(LEVELS)]
        self.gz = [coarse_cells(G0Z, l) for l in range(LEVELS)]
        self.nx = [g // slabs + 1 for g in self.gx]
        self.ny = [g // cols for g in self.gy]
        self.main = [a * b for a, b in zip(self.nx, self.ny)]
        self.block = [m + HALO for m in self.main]
        self.start = [sum(self.block[:l]) for l in range(LEVELS)]
        self.total = sum(self.block)
        self.xrow = [sum(self.nx[:l]) for l in range(LEVELS)]
        self.yrow = [sum(self.ny[:l]) for l in range(LEVELS)]
        self.zrow = [sum(self.gz[:l]) for l in range(LEVELS)]

    def node_table(self):
        def frac(node, cells):
            return (2 * node * 2**32 + cells) // (2 * cells)

        xs = [frac(r, g) for g, n in zip(self.gx, self.nx) for r in range(n)]
        hs = [frac(c, g) for g, n, c in zip(self.gy, self.nx, self.ny) for r in range(n)]
        pad = [0] * (HALO - len(xs))
        ys = [frac(r, g) for g, n in zip(self.gy, self.ny) for r in range(n)]
        zs = [frac(r, g) for g in self.gz for r in range(g)]
        flat = np.array(xs + pad + hs + pad + ys + zs, np.int64) + 2**31
        flat = ((flat + 2**31) % 2**32 - 2**31).astype(np.int32)
        return np.repeat(flat[:, None], LANES, axis=1)

    def factor_table(self):
        k = [exponent(g) for g, n in zip(self.gx, self.nx) for _ in range(n)]
        h = [exponent(g) for g, n in zip(self.gy, self.nx) for _ in range(n)]
        pad = [0.0] * (HALO - len(k))
        return np.repeat(np.array(k + pad + h + pad, np.float32)[:, None], LANES, axis=1)

    def y_matrix(self, l):
        fine = self.rows[1]
        nx, ny, main = self.nx[l], self.ny[l], self.main[l]
        b = np.arange(fine)[:, None]
        y = np.arange(ny + 1)[None, :]
        hat = np.maximum(0.0, 1.0 - np.abs(y - b * self.gy[l] / FINE_Y))
        out = np.zeros((nx * fine, self.block[l]), np.float32)
        for x in range(nx):
            out[x * fine : (x + 1) * fine, x * ny : (x + 1) * ny] = hat[:, :ny]
            out[x * fine : (x + 1) * fine, main + self.xrow[l] + x] = hat[:, ny]
        return np.concatenate([out, out], axis=1)

    def x_matrix(self, l):
        a = np.arange(self.rows[0])[:, None]
        x = np.arange(self.nx[l])[None, :]
        return np.maximum(0.0, 1.0 - np.abs(x - a * self.gx[l] / FINE_X))


def exponent(cells):
    return -0.5 * np.log2(np.e) / spread_width**2 * (cells / 2.0**32) ** 2


def split(value):
    high = value.astype(jnp.bfloat16)
    low = (value - high.astype(jnp.float32)).astype(jnp.bfloat16)
    return high, low


def kernel(
    plan, cx, cy, cz, off, charge, count, amp, dens, nodes, factors, my0, my1, my2, my3,
    field, energy,
    buf, planes, wz, wy, wx, acc, other, pz, t2, dens_v, field_v, ez, ex,
    zs_sem, zr_sem, xs_sem, xr_sem, ps_sem, pr_sem, es_sem, er_sem, fs_sem, fr_sem, d_sem, o_sem,
):
    slabs, cols = plan.slabs, plan.cols
    half = slabs // 2
    me = lax.axis_index("slab")
    col = lax.axis_index("blk")
    core = lax.axis_index("sub")
    mats = (my0, my1, my2, my3)
    wide = 2 * BQ

    def at(ds, dc, dk):
        return {
            "slab": lax.rem(me + slabs + ds, slabs),
            "blk": lax.rem(col + cols + dc, cols),
            "sub": lax.rem(core + dk, 2),
        }

    order = [0]
    for d in range(1, half):
        order += [d, -d]
    order.append(half)
    others = [(dc, dk) for dc in range(cols) for dk in range(2)][1:]

    barrier = pltpu.get_barrier_semaphore()
    for ds in order[1:]:
        pl.semaphore_signal(barrier, inc=1, device_id=at(ds, 0, 0), device_id_type=MESH)
    for dc, dk in others:
        pl.semaphore_signal(barrier, inc=1, device_id=at(0, dc, dk), device_id_type=MESH)

    load = pltpu.make_async_copy(dens, dens_v, d_sem)
    load.start()

    lane = lax.broadcasted_iota(jnp.int32, (1, BQ), 1)
    live = jnp.where(lane < count[0], 1.0, 0.0).astype(jnp.float32)
    buf[0, 0, 0:1, 0:BQ] = charge[...] * live
    buf[0, 0, 1:2, 0:BQ] = cx[...].astype(jnp.float32) + off[0:1, :]
    buf[0, 0, 2:3, 0:BQ] = cy[...].astype(jnp.float32) + off[1:2, :]
    buf[0, 0, 3:4, 0:BQ] = cz[...].astype(jnp.float32) + off[2:3, :]
    acc[...] = jnp.zeros_like(acc)

    node = lax.broadcasted_iota(jnp.int32, (LANES, LANES), 0)
    fine = lax.broadcasted_iota(jnp.int32, (LANES, LANES), 1) + core * LANES
    for l in range(LEVELS):
        g = plan.gz[l]
        moved = node * FINE_Z - fine * g
        moved = jnp.where(moved < 0, moved + g * FINE_Z, moved)
        moved = jnp.where(moved * 2 >= g * FINE_Z, moved - g * FINE_Z, moved)
        hat = jnp.maximum(0.0, 1.0 - jnp.abs(moved.astype(jnp.float32)) * (1.0 / FINE_Z))
        hat = jnp.where(node < g, hat, 0.0).astype(jnp.bfloat16)
        pz[l, 0:LANES, :] = hat
        pz[l, LANES:, :] = hat

    pl.semaphore_wait(barrier, len(order) - 1 + len(others))

    def z_copy(k):
        row, part = k // 2, k % 2
        slot = buf.at[0, row, :, part * BQ : (part + 1) * BQ]
        return pltpu.make_async_remote_copy(
            src_ref=buf.at[0, 0, :, 0:BQ], dst_ref=slot, send_sem=zs_sem.at[k], recv_sem=zr_sem.at[k],
            device_id=at(-order[k], 0, 0), device_id_type=MESH,
        )

    for k in range(slabs - 1, 0, -1):
        z_copy(k).start()

    def z_wait(j, part):
        pltpu.make_async_remote_copy(
            src_ref=buf.at[0, 0, :, 0:BQ], dst_ref=buf.at[0, j, :, part * BQ : (part + 1) * BQ],
            send_sem=zs_sem.at[2 * j + part], recv_sem=zr_sem.at[2 * j + part],
            device_id=at(1, 0, 0), device_id_type=MESH,
        ).wait_recv()

    def x_copy(p, j):
        return pltpu.make_async_remote_copy(
            src_ref=buf.at[0, j], dst_ref=buf.at[p, j], send_sem=xs_sem.at[p, j], recv_sem=xr_sem.at[p, j],
            device_id=at(0, -p, 0), device_id_type=MESH,
        )

    scale = 2.0**32
    top = 2.0**31 - 128.0

    def fixed(row, cells):
        moved = jnp.minimum((row - 0.5 * cells) * (scale / cells), top)
        return moved.astype(jnp.int32)

    def gauss(first, rows, at_row, factor):
        table = nodes[first : first + rows, :]
        wrapped = (jnp.concatenate([table] * (wide // LANES), axis=1) - at_row).astype(jnp.float32)
        return jnp.exp2(wrapped * wrapped * factor)

    def spread(p, j):
        chunk = buf[p, j]
        ux = fixed(chunk[1:2, :], G0X) - me * (2**32 // slabs)
        uy = fixed(chunk[2:3, :], G0Y) - col * (2**32 // cols)
        uz = fixed(chunk[3:4, :], G0Z)
        fx = jnp.concatenate([factors[0:HALO, :]] * (wide // LANES), axis=1)
        fh = jnp.concatenate([factors[HALO : 2 * HALO, :]] * (wide // LANES), axis=1)
        weighted = chunk[0:1, :] * gauss(0, HALO, ux, fx)
        wx[...] = weighted
        edge = (weighted * gauss(HALO, HALO, uy, fh)).astype(jnp.bfloat16)
        for l in range(LEVELS):
            start, main = plan.start[l], plan.main[l]
            planes[start + main : start + main + HALO, :] = edge
            z0 = 2 * HALO + plan.yrow[-1] + plan.ny[-1] + plan.zrow[l]
            for r in range(0, plan.gz[l], 16):
                part = gauss(z0 + r, 16, uz, exponent(plan.gz[l])).astype(jnp.bfloat16)
                wz[plan.zrow[l] + r : plan.zrow[l] + r + 16, :] = part
            ny = plan.ny[l]
            along_y = gauss(2 * HALO + plan.yrow[l], ny, uy, exponent(plan.gy[l]))
            step = 1 if ny % 16 == 0 else 2
            for x in range(0, plan.nx[l], step):
                both = [wx[plan.xrow[l] + x + i : plan.xrow[l] + x + i + 1, :] * along_y for i in range(step)]
                value = both[0] if step == 1 else jnp.concatenate(both, axis=0)
                planes[start + x * ny : start + (x + step) * ny, :] = value.astype(jnp.bfloat16)
            rows = plan.block[l]
            acc[start : start + rows, 0 : plan.gz[l]] += lax.dot_general(
                planes[start : start + rows, :], wz[plan.zrow[l] : plan.zrow[l] + plan.gz[l], :],
                (((1,), (1,)), ((), ())), preferred_element_type=jnp.float32,
            )

    @pl.loop(0, half + 1)
    def _(j):
        @pl.when(j < half)
        def _():
            @pl.when(j > 0)
            def _():
                z_wait(j, 0)

            z_wait(j, 1)
            for p in range(1, cols):
                x_copy(p, j).start()

        @pl.loop(0, cols)
        def _(p):
            held = jnp.where(p == 0, j, j - 1)

            @pl.when((held >= 0) & (held < half))
            def _():
                @pl.when(p > 0)
                def _():
                    x_copy(p, held).wait_recv()

                spread(p, held)

    swap = pltpu.make_async_remote_copy(
        src_ref=acc, dst_ref=other, send_sem=ps_sem, recv_sem=pr_sem, device_id=at(0, 0, 1), device_id_type=MESH
    )
    swap.start()
    load.wait()
    swap.wait_recv()

    fine_y = plan.rows[1]
    for l in range(LEVELS):
        start, rows = plan.start[l], plan.block[l]
        cube = acc[start : start + rows, :] + other[start : start + rows, :]
        along_z = jnp.dot(jnp.concatenate(split(cube), axis=1), pz[l], preferred_element_type=jnp.float32)
        t2[plan.xrow[l] * fine_y : (plan.xrow[l] + plan.nx[l]) * fine_y, :] = amp[l] * jnp.dot(
            mats[l][...], jnp.concatenate(split(along_z), axis=0), preferred_element_type=jnp.float32
        )

    sums = jnp.zeros((fine_y, LANES), jnp.float32)
    for a in range(plan.rows[0]):
        value = None
        for l in range(LEVELS):
            hat = plan.x_matrix(l)[a]
            for x in range(plan.nx[l]):
                if hat[x] > 0.0:
                    at_x = (plan.xrow[l] + x) * fine_y
                    term = float(hat[x]) * t2[at_x : at_x + fine_y, :]
                    value = term if value is None else value + term
        field_v[a] = value
        sums = sums + value * dens_v[a]
    store = pltpu.make_async_copy(field_v, field, o_sem)
    store.start()

    ez[0] = jnp.sum(sums, axis=0, keepdims=True)

    def e_copy(k):
        return pltpu.make_async_remote_copy(
            src_ref=ez.at[0], dst_ref=ez.at[k], send_sem=es_sem.at[k], recv_sem=er_sem.at[k],
            device_id=at(-order[k], 0, 0), device_id_type=MESH,
        )

    for k in range(slabs - 1, 0, -1):
        e_copy(k).start()
    for k in range(1, slabs):
        e_copy(k).wait_recv()
    ex[0] = jnp.sum(ez[...], axis=0)

    def f_copy(k):
        dc, dk = others[k - 1]
        return pltpu.make_async_remote_copy(
            src_ref=ex.at[0], dst_ref=ex.at[k], send_sem=fs_sem.at[k], recv_sem=fr_sem.at[k],
            device_id=at(0, -dc, dk), device_id_type=MESH,
        )

    for k in range(len(others), 0, -1):
        f_copy(k).start()
    for k in range(1, len(others) + 1):
        f_copy(k).wait_recv()
    energy[0, 0] = jnp.sum(jnp.sum(ex[...], axis=0)) * (1.0 / (FINE_X * FINE_Y * FINE_Z))

    for k in range(1, slabs):
        z_copy(k).wait_send()
        e_copy(k).wait_send()

    @pl.loop(0, half)
    def _(j):
        for p in range(1, cols):
            x_copy(p, j).wait_send()

    for k in range(1, len(others) + 1):
        f_copy(k).wait_send()
    swap.wait_send()
    store.wait()


def on_device(cell_x, cell_y, cell_z, offsets, charge, block_count, level_amplitude, density):
    slabs, cols = lax.axis_size("slab"), lax.axis_size("blk")
    plan = Plan(slabs, cols, *density.shape)
    slots = cell_x.shape[0]
    mats = [jnp.asarray(plan.y_matrix(l), jnp.bfloat16) for l in range(LEVELS)]
    vmem = pl.BlockSpec(memory_space=pltpu.VMEM)
    smem = pl.BlockSpec(memory_space=pltpu.SMEM)
    anywhere = pl.BlockSpec(memory_space=pl.ANY)
    dma = pltpu.SemaphoreType.DMA
    field, energy = pl.pallas_call(
        functools.partial(kernel, plan),
        out_shape=(jax.ShapeDtypeStruct(density.shape, jnp.float32), jax.ShapeDtypeStruct((1, 1), jnp.float32)),
        in_specs=[vmem] * 5 + [smem] * 2 + [anywhere] + [vmem] * 6,
        out_specs=(anywhere, smem),
        scratch_shapes=[
            pltpu.VMEM((cols, slabs // 2, 4, 2 * BQ), jnp.float32),
            pltpu.VMEM((plan.total, 2 * BQ), jnp.bfloat16),
            pltpu.VMEM((sum(plan.gz), 2 * BQ), jnp.bfloat16),
            pltpu.VMEM((sum(plan.ny), 2 * BQ), jnp.float32),
            pltpu.VMEM((HALO, 2 * BQ), jnp.float32),
            pltpu.VMEM((plan.total, LANES), jnp.float32),
            pltpu.VMEM((plan.total, LANES), jnp.float32),
            pltpu.VMEM((LEVELS, 2 * LANES, LANES), jnp.bfloat16),
            pltpu.VMEM((sum(plan.nx) * density.shape[1], LANES), jnp.float32),
            pltpu.VMEM(density.shape, jnp.float32),
            pltpu.VMEM(density.shape, jnp.float32),
            pltpu.VMEM((slabs, 1, LANES), jnp.float32),
            pltpu.VMEM((2 * cols, 1, LANES), jnp.float32),
            dma((slabs,)), dma((slabs,)),
            dma((cols, slabs // 2)), dma((cols, slabs // 2)),
            dma, dma,
            dma((slabs,)), dma((slabs,)),
            dma((2 * cols,)), dma((2 * cols,)),
            dma, dma,
        ],
        compiler_params=pltpu.CompilerParams(collective_id=0, has_side_effects=True),
    )(
        cell_x.reshape(1, slots), cell_y.reshape(1, slots), cell_z.reshape(1, slots), offsets,
        charge.reshape(1, slots), block_count, level_amplitude, density,
        jnp.asarray(plan.node_table()), jnp.asarray(plan.factor_table()), *mats,
    )
    return field, energy.reshape(1)


def solution(mesh):
    split_all = ("grp", "slab", "blk", "sub")
    in_specs = (
        P(split_all), P(split_all), P(split_all), P(None, split_all), P(split_all), P(split_all), P(),
        P(("grp", "slab"), "blk", "sub"),
    )
    out_specs = (P(("grp", "slab"), "blk", "sub"), P("grp"))
    return jax.shard_map(on_device, mesh=mesh, in_specs=in_specs, out_specs=out_specs, check_vma=False)
```

```python
import functools

import jax
import jax.numpy as jnp
import numpy as np
from jax import lax
from jax.experimental import pallas as pl
from jax.experimental.pallas import tpu as pltpu
from jax.sharding import PartitionSpec as P

G0X = 64
G0Y = 128
G0Z = 128
FINE_X = 256
FINE_Y = 256
FINE_Z = 256
BQ = 256
LEVELS = 4
LANES = 128
SPAN = 256
ROWS = 8
HALO = 16
spread_width = 1.25
MESH = pl.DeviceIdType.MESH

ORDER = ((0, 2, 1, 3), (0, 1, 2), (0, 1), (0,))
SETS = (
    ((3, 0), ((3, 0, 1.0), (2, 0, 4.0), (1, 0, 9.0), (0, 0, 16.0))),
    ((2, 1), ((2, 1, 1.0), (0, 1, 4.0))),
    ((1, 1), ((1, 1, 1.0),)),
    ((1, 2), ((1, 2, 1.0),)),
    ((0, 1), ((0, 2, 1.0),)),
    ((0, 3), ((0, 3, 1.0),)),
)


def coarse_cells(base, level):
    return base * (4 - level) // 4


def exponent(cells):
    return -0.5 * np.log2(np.e) / spread_width**2 * (cells / 2.0**32) ** 2


class Plan:
    def __init__(self, slabs, cols, rows_x, rows_y, rows_z):
        self.slabs, self.cols = slabs, cols
        self.rows = (rows_x, rows_y, rows_z)
        self.gx = [coarse_cells(G0X, l) for l in range(LEVELS)]
        self.gy = [coarse_cells(G0Y, l) for l in range(LEVELS)]
        self.gz = [coarse_cells(G0Z, l) for l in range(LEVELS)]
        self.nx = [g // slabs + 1 for g in self.gx]
        self.ny = [g // cols for g in self.gy]
        self.main = [a * b for a, b in zip(self.nx, self.ny)]
        self.block = [m + HALO for m in self.main]
        self.start = [sum(self.block[:l]) for l in range(LEVELS)]
        self.total = sum(self.block)
        self.xrow = [sum(self.nx[:l]) for l in range(LEVELS)]
        self.yrow = [sum(self.ny[:l]) for l in range(LEVELS)]
        self.zrow = [sum(self.gz[:l]) for l in range(LEVELS)]
        self.yset, self.zset = self.ny[-1], self.gz[-1]
        self.ytable = 2 * HALO
        self.ztable = self.ytable + len(SETS) * self.yset

    def y_nodes(self, l):
        m = LEVELS - l
        return [m * k + s for s in ORDER[l] for k in range(self.yset)]

    def node_table(self):
        def frac(node, cells):
            return (2 * node * 2**32 + cells) // (2 * cells)

        flat = [frac(r, g) for g, n in zip(self.gx, self.nx) for r in range(n)]
        flat += [0] * (HALO - len(flat))
        flat += [frac(c, g) for g, n, c in zip(self.gy, self.nx, self.ny) for _ in range(n)]
        flat += [0] * (2 * HALO - len(flat))
        for cells, count in ((self.gy, self.yset), (self.gz, self.zset)):
            for (l, s), _ in SETS:
                flat += [frac((LEVELS - l) * k + s, cells[l]) for k in range(count)]
        flat = np.array(flat, np.int64) + 2**31
        flat = ((flat + 2**31) % 2**32 - 2**31).astype(np.int32)
        return np.repeat(flat[:, None], LANES, axis=1)

    def factor_table(self):
        k = [exponent(g) for g, n in zip(self.gx, self.nx) for _ in range(n)]
        h = [exponent(g) for g, n in zip(self.gy, self.nx) for _ in range(n)]
        pad = [0.0] * (HALO - len(k))
        return np.repeat(np.array(k + pad + h + pad, np.float32)[:, None], LANES, axis=1)

    def y_matrix(self, l):
        fine = self.rows[1]
        nx, ny, main = self.nx[l], self.ny[l], self.main[l]
        b = np.arange(fine)[:, None]
        y = np.array(self.y_nodes(l) + [ny])[None, :]
        hat = np.maximum(0.0, 1.0 - np.abs(y - b * self.gy[l] / FINE_Y))
        out = np.zeros((nx * fine, self.block[l]), np.float32)
        for x in range(nx):
            out[x * fine : (x + 1) * fine, x * ny : (x + 1) * ny] = hat[:, :ny]
            out[x * fine : (x + 1) * fine, main + self.xrow[l] + x] = hat[:, ny]
        return out

    def x_matrix(self, l):
        a = np.arange(self.rows[0])[:, None]
        x = np.arange(self.nx[l])[None, :]
        return np.maximum(0.0, 1.0 - np.abs(x - a * self.gx[l] / FINE_X))

    def constants(self):
        twice = lambda m: jnp.asarray(np.concatenate([m, m], axis=1), jnp.bfloat16)
        down = [twice(self.y_matrix(l)) for l in range(LEVELS)]
        up = [twice(self.y_matrix(l).T) for l in range(LEVELS)]
        return [jnp.asarray(self.node_table()), jnp.asarray(self.factor_table())] + down + up


def split(value):
    high = value.astype(jnp.bfloat16)
    low = (value - high.astype(jnp.float32)).astype(jnp.bfloat16)
    return high, low


def kernel(plan, n_in, *refs):
    hbm, refs = refs[:n_in], refs[n_in:]
    field, energy, refs = refs[0], refs[1], refs[2:]
    held_in, refs = refs[:n_in], refs[n_in:]
    (
        buf, planes, wz, acc, other, dual, dual_other, pz, t2, field_v, ez, ex,
        in_sem, zs_sem, zr_sem, xs_sem, xr_sem, ps_sem, pr_sem, es_sem, er_sem, fs_sem, fr_sem, o_sem,
    ) = refs
    cx, cy, cz, off, charge, count, amp, dens_v, nodes, factors = held_in[:10]
    down, up = held_in[10 : 10 + LEVELS], held_in[10 + LEVELS :]
    slabs, cols = plan.slabs, plan.cols
    half = slabs // 2
    reach = half // 2
    me = lax.axis_index("slab")
    col = lax.axis_index("blk")
    core = lax.axis_index("sub")
    wide = 2 * BQ
    fine_y = plan.rows[1]

    def at(ds, dc, dk):
        return {
            "slab": lax.rem(me + slabs + ds, slabs),
            "blk": lax.rem(col + cols + dc, cols),
            "sub": lax.rem(core + dk, 2),
        }

    order = [0]
    for d in range(1, half):
        order += [d, -d]
    order.append(half)
    others = [(dc, dk) for dc in range(cols) for dk in range(2)][1:]

    barrier = pltpu.get_barrier_semaphore()
    near = order[1 : 2 * reach] + [reach, -reach]
    near = [d for i, d in enumerate(near) if d not in near[:i]]
    for ds in near:
        pl.semaphore_signal(barrier, inc=1, device_id=at(ds, 0, 0), device_id_type=MESH)
    for dc, dk in others:
        pl.semaphore_signal(barrier, inc=1, device_id=at(0, dc, dk), device_id_type=MESH)

    loads = [pltpu.make_async_copy(hbm[i], held_in[i], in_sem.at[i]) for i in range(n_in)]
    for load in loads:
        load.start()
    for i in range(6):
        loads[i].wait()

    lane = lax.broadcasted_iota(jnp.int32, (1, BQ), 1)
    live = jnp.where(lane < count[0], 1.0, 0.0).astype(jnp.float32)
    buf[0, 0, 0:1, 0:BQ] = charge[...] * live
    buf[0, 0, 1:2, 0:BQ] = cx[...].astype(jnp.float32) + off[0:1, :]
    buf[0, 0, 2:3, 0:BQ] = cy[...].astype(jnp.float32) + off[1:2, :]
    buf[0, 0, 3:4, 0:BQ] = cz[...].astype(jnp.float32) + off[2:3, :]

    pl.semaphore_wait(barrier, len(near) + len(others))

    def slot(j, part):
        return buf.at[0, j, :, pl.ds(part * BQ, BQ)]

    def z_copy(src, j, part, ds):
        return pltpu.make_async_remote_copy(
            src_ref=src, dst_ref=slot(j, part), send_sem=zs_sem.at[j, part], recv_sem=zr_sem.at[j, part],
            device_id=at(ds, 0, 0), device_id_type=MESH,
        )

    for k in range(2 * reach, 0, -1):
        z_copy(slot(0, 0), k // 2, k % 2, -order[k]).start()

    def x_copy(p, j):
        return pltpu.make_async_remote_copy(
            src_ref=buf.at[0, j], dst_ref=buf.at[p, j], send_sem=xs_sem.at[p, j], recv_sem=xr_sem.at[p, j],
            device_id=at(0, -p, 0), device_id_type=MESH,
        )

    acc[...] = jnp.zeros_like(acc)
    planes[1] = jnp.zeros(planes.shape[1:], planes.dtype)
    wz[1] = jnp.zeros(wz.shape[1:], wz.dtype)

    row = lax.broadcasted_iota(jnp.int32, (LANES, LANES), 0)
    fine = lax.broadcasted_iota(jnp.int32, (LANES, LANES), 1) + core * LANES
    for l in range(LEVELS):
        g = plan.gz[l]
        place = row // plan.zset
        part = (place % 2) * 2 + place // 2 if l == 0 else place
        node = (row % plan.zset) * (LEVELS - l) + part
        moved = node * FINE_Z - fine * g
        moved = jnp.where(moved < 0, moved + g * FINE_Z, moved)
        moved = jnp.where(moved * 2 >= g * FINE_Z, moved - g * FINE_Z, moved)
        hat = jnp.maximum(0.0, 1.0 - jnp.abs(moved.astype(jnp.float32)) * (1.0 / FINE_Z))
        hat = jnp.where(row < g, hat, 0.0).astype(jnp.bfloat16)
        pz[l, 0:LANES, :] = hat
        pz[l, LANES:, :] = hat

    for i in range(6, n_in):
        loads[i].wait()
    for l in range(LEVELS):
        hats = plan.x_matrix(l)
        for x in range(plan.nx[l]):
            value = None
            for a in range(plan.rows[0]):
                if hats[a, x] > 0.0:
                    term = float(hats[a, x]) * dens_v[a]
                    value = term if value is None else value + term
            at_x = (plan.xrow[l] + x) * fine_y
            t2[at_x : at_x + fine_y, :] = value * amp[l]
        start, rows = plan.start[l], plan.block[l]
        along = t2[plan.xrow[l] * fine_y : (plan.xrow[l] + plan.nx[l]) * fine_y, :]
        on_y = jnp.dot(up[l][...], jnp.concatenate(split(along), axis=0), preferred_element_type=jnp.float32)
        both = lax.dot_general(
            jnp.concatenate(split(on_y), axis=0), pz[l, 0:LANES, :], (((1,), (1,)), ((), ())),
            preferred_element_type=jnp.float32,
        )
        dual[start : start + rows, :] = both[:rows] + both[rows:]

    def swap(k, src, dst):
        return pltpu.make_async_remote_copy(
            src_ref=src, dst_ref=dst, send_sem=ps_sem.at[k], recv_sem=pr_sem.at[k],
            device_id=at(0, 0, 1), device_id_type=MESH,
        )

    swap(0, dual, dual_other).start()

    scale = 2.0**32
    top = 2.0**31 - 128.0

    def fixed(line, cells):
        moved = jnp.minimum((line - 0.5 * cells) * (scale / cells), top)
        return moved.astype(jnp.int32)

    def broad(table):
        return jnp.concatenate([table] * (SPAN // LANES), axis=1)

    def weigh(p, j, s):
        for c in range(0, wide, SPAN):
            lanes = slice(c, c + SPAN)
            chunk = buf[p, j, :, lanes]
            ux = fixed(chunk[1:2, :], G0X) - me * (2**32 // slabs)
            uy = fixed(chunk[2:3, :], G0Y) - col * (2**32 // cols)
            uz = fixed(chunk[3:4, :], G0Z)

            def squared(first, rows, at_line, factor):
                wrapped = (broad(nodes[first : first + rows, :]) - at_line).astype(jnp.float32)
                return wrapped * wrapped * factor

            for i, ((l0, _), uses) in enumerate(SETS):
                for r in range(0, plan.zset, ROWS):
                    power = squared(plan.ztable + i * plan.zset + r, ROWS, uz, exponent(plan.gz[l0]))
                    for l, place, times in uses:
                        value = jnp.exp2(power if times == 1.0 else power * times).astype(jnp.bfloat16)
                        to = plan.zrow[l] + place * plan.zset + r
                        wz[s, to : to + ROWS, lanes] = value
            along_y = [[None] * len(ORDER[l]) for l in range(LEVELS)]
            for i, ((l0, _), uses) in enumerate(SETS):
                power = squared(plan.ytable + i * plan.yset, plan.yset, uy, exponent(plan.gy[l0]))
                for l, place, times in uses:
                    along_y[l][place] = jnp.exp2(power if times == 1.0 else power * times)
            weighted = chunk[0:1, :] * jnp.exp2(squared(0, HALO, ux, broad(factors[0:HALO, :])))
            last = jnp.exp2(squared(HALO, HALO, uy, broad(factors[HALO : 2 * HALO, :])))
            edge = (weighted * last).astype(jnp.bfloat16)
            for l in range(LEVELS):
                start, main, ny = plan.start[l], plan.main[l], plan.ny[l]
                planes[s, start + main : start + main + HALO, lanes] = edge
                tiles = [
                    weighted[plan.xrow[l] + x : plan.xrow[l] + x + 1, :] * on_y
                    for x in range(plan.nx[l]) for on_y in along_y[l]
                ]
                for t, tile in enumerate(tiles):
                    to = start + t * plan.yset
                    planes[s, to : to + plan.yset, lanes] = tile.astype(jnp.bfloat16)

    def gather_in(s):
        for l in range(LEVELS):
            start, rows = plan.start[l], plan.block[l]
            acc[start : start + rows, 0 : plan.gz[l]] += lax.dot_general(
                planes[s, start : start + rows, :], wz[s, plan.zrow[l] : plan.zrow[l] + plan.gz[l], :],
                (((1,), (1,)), ((), ())), preferred_element_type=jnp.float32,
            )

    def arrive(j):
        pair = half // 2

        @pl.when(j > 0)
        def _():
            z_copy(slot(0, 0), j, 0, 1).wait_recv()

        z_copy(slot(0, 0), j, 1, 1).wait_recv()

        @pl.when((j > 0) & (j < pair))
        def _():
            z_copy(slot(j, 0), j + pair, 0, reach).start()

        @pl.when(j < pair)
        def _():
            z_copy(slot(j, 1), j + pair, 1, -reach).start()

        for p in range(1, cols):
            x_copy(p, j).start()

    steps = half // 2

    @pl.loop(0, steps + 1)
    def _(m):
        @pl.when(m < steps)
        def _():
            arrive(2 * m)
            arrive(2 * m + 1)

        @pl.loop(0, cols)
        def _(p):
            held = jnp.where(p == 0, m, m - 1)

            @pl.when((held >= 0) & (held < steps))
            def _():
                @pl.when(p > 0)
                def _():
                    x_copy(p, 2 * held).wait_recv()
                    x_copy(p, 2 * held + 1).wait_recv()

                gather_in(1)
                weigh(p, 2 * held, 0)
                gather_in(0)
                weigh(p, 2 * held + 1, 1)

    gather_in(1)
    swap(1, acc, other).start()
    swap(0, dual, dual_other).wait_recv()
    ez[0] = jnp.sum(acc[...] * (dual[...] + dual_other[...]), axis=0, keepdims=True)

    def e_copy(k):
        return pltpu.make_async_remote_copy(
            src_ref=ez.at[0], dst_ref=ez.at[k], send_sem=es_sem.at[k], recv_sem=er_sem.at[k],
            device_id=at(-order[k], 0, 0), device_id_type=MESH,
        )

    for k in range(slabs - 1, 0, -1):
        e_copy(k).start()
    swap(1, acc, other).wait_recv()

    for l in range(LEVELS):
        start, rows = plan.start[l], plan.block[l]
        cube = acc[start : start + rows, :] + other[start : start + rows, :]
        along_z = jnp.dot(jnp.concatenate(split(cube), axis=1), pz[l], preferred_element_type=jnp.float32)
        t2[plan.xrow[l] * fine_y : (plan.xrow[l] + plan.nx[l]) * fine_y, :] = amp[l] * jnp.dot(
            down[l][...], jnp.concatenate(split(along_z), axis=0), preferred_element_type=jnp.float32
        )
    for a in range(plan.rows[0]):
        value = None
        for l in range(LEVELS):
            hat = plan.x_matrix(l)[a]
            for x in range(plan.nx[l]):
                if hat[x] > 0.0:
                    at_x = (plan.xrow[l] + x) * fine_y
                    term = float(hat[x]) * t2[at_x : at_x + fine_y, :]
                    value = term if value is None else value + term
        field_v[a] = value
    store = pltpu.make_async_copy(field_v, field, o_sem)
    store.start()

    for k in range(1, slabs):
        e_copy(k).wait_recv()
    ex[0] = jnp.sum(ez[...], axis=0)

    def f_copy(k):
        dc, dk = others[k - 1]
        return pltpu.make_async_remote_copy(
            src_ref=ex.at[0], dst_ref=ex.at[k], send_sem=fs_sem.at[k], recv_sem=fr_sem.at[k],
            device_id=at(0, -dc, dk), device_id_type=MESH,
        )

    for k in range(len(others), 0, -1):
        f_copy(k).start()

    for k in range(1, slabs):
        z_copy(slot(0, 0), k // 2, k % 2, 1).wait_send()
        e_copy(k).wait_send()

    @pl.loop(0, half)
    def _(j):
        for p in range(1, cols):
            x_copy(p, j).wait_send()

    swap(0, dual, dual_other).wait_send()
    swap(1, acc, other).wait_send()
    store.wait()
    for k in range(1, len(others) + 1):
        f_copy(k).wait_recv()
    energy[0, 0] = jnp.sum(jnp.sum(ex[...], axis=0)) * (1.0 / (FINE_X * FINE_Y * FINE_Z))
    for k in range(1, len(others) + 1):
        f_copy(k).wait_send()


def on_device(cell_x, cell_y, cell_z, offsets, charge, block_count, level_amplitude, density):
    slabs, cols = lax.axis_size("slab"), lax.axis_size("blk")
    plan = Plan(slabs, cols, *density.shape)
    slots = cell_x.shape[0]
    operands = [
        cell_x.reshape(1, slots), cell_y.reshape(1, slots), cell_z.reshape(1, slots), offsets,
        charge.reshape(1, slots), block_count, level_amplitude, density, *plan.constants(),
    ]
    n_in = len(operands)
    spaces = [pltpu.VMEM] * 5 + [pltpu.SMEM] * 2 + [pltpu.VMEM] * (n_in - 7)
    smem = pl.BlockSpec(memory_space=pltpu.SMEM)
    anywhere = pl.BlockSpec(memory_space=pl.ANY)
    dma = pltpu.SemaphoreType.DMA
    field, energy = pl.pallas_call(
        functools.partial(kernel, plan, n_in),
        out_shape=(jax.ShapeDtypeStruct(density.shape, jnp.float32), jax.ShapeDtypeStruct((1, 1), jnp.float32)),
        in_specs=[anywhere] * n_in,
        out_specs=(anywhere, smem),
        scratch_shapes=[space(o.shape, o.dtype) for space, o in zip(spaces, operands)]
        + [
            pltpu.VMEM((cols, slabs // 2, 4, 2 * BQ), jnp.float32),
            pltpu.VMEM((2, plan.total, 2 * BQ), jnp.bfloat16),
            pltpu.VMEM((2, sum(plan.gz), 2 * BQ), jnp.bfloat16),
            pltpu.VMEM((plan.total, LANES), jnp.float32),
            pltpu.VMEM((plan.total, LANES), jnp.float32),
            pltpu.VMEM((plan.total, LANES), jnp.float32),
            pltpu.VMEM((plan.total, LANES), jnp.float32),
            pltpu.VMEM((LEVELS, 2 * LANES, LANES), jnp.bfloat16),
            pltpu.VMEM((sum(plan.nx) * density.shape[1], LANES), jnp.float32),
            pltpu.VMEM(density.shape, jnp.float32),
            pltpu.VMEM((slabs, 1, LANES), jnp.float32),
            pltpu.VMEM((2 * cols, 1, LANES), jnp.float32),
            dma((n_in,)),
            dma((slabs // 2, 2)), dma((slabs // 2, 2)),
            dma((cols, slabs // 2)), dma((cols, slabs // 2)),
            dma((2,)), dma((2,)),
            dma((slabs,)), dma((slabs,)),
            dma((2 * cols,)), dma((2 * cols,)),
            dma,
        ],
        compiler_params=pltpu.CompilerParams(collective_id=0, has_side_effects=True),
    )(*operands)
    return field, energy.reshape(1)


def solution(mesh):
    split_all = ("grp", "slab", "blk", "sub")
    in_specs = (
        P(split_all), P(split_all), P(split_all), P(None, split_all), P(split_all), P(split_all), P(),
        P(("grp", "slab"), "blk", "sub"),
    )
    out_specs = (P(("grp", "slab"), "blk", "sub"), P("grp"))
    return jax.shard_map(on_device, mesh=mesh, in_specs=in_specs, out_specs=out_specs, check_vma=False)
```

```python
import functools

import jax
import jax.numpy as jnp
import numpy as np
from jax import lax
from jax.experimental import pallas as pl
from jax.experimental.pallas import tpu as pltpu
from jax.sharding import PartitionSpec as P

G0X = 64
G0Y = 128
G0Z = 128
FINE_X = 256
FINE_Y = 256
FINE_Z = 256
BQ = 256
LEVELS = 4
LANES = 128
SPAN = 256
ROWS = 8
HALO = 16
spread_width = 1.25
MESH = pl.DeviceIdType.MESH

ORDER = ((0, 2, 1, 3), (0, 1, 2), (0, 1), (0,))
SETS = (
    ((3, 0), ((3, 0, 1.0), (2, 0, 4.0), (1, 0, 9.0), (0, 0, 16.0))),
    ((2, 1), ((2, 1, 1.0), (0, 1, 4.0))),
    ((1, 1), ((1, 1, 1.0),)),
    ((1, 2), ((1, 2, 1.0),)),
    ((0, 1), ((0, 2, 1.0),)),
    ((0, 3), ((0, 3, 1.0),)),
)


def coarse_cells(base, level):
    return base * (4 - level) // 4


def exponent(cells):
    return -0.5 * np.log2(np.e) / spread_width**2 * (cells / 2.0**32) ** 2


class Plan:
    def __init__(self, slabs, cols, rows_x, rows_y, rows_z):
        self.slabs, self.cols = slabs, cols
        self.rows = (rows_x, rows_y, rows_z)
        self.gx = [coarse_cells(G0X, l) for l in range(LEVELS)]
        self.gy = [coarse_cells(G0Y, l) for l in range(LEVELS)]
        self.gz = [coarse_cells(G0Z, l) for l in range(LEVELS)]
        self.nx = [g // slabs + 1 for g in self.gx]
        self.ny = [g // cols for g in self.gy]
        self.main = [a * b for a, b in zip(self.nx, self.ny)]
        self.block = [m + HALO for m in self.main]
        self.start = [sum(self.block[:l]) for l in range(LEVELS)]
        self.total = sum(self.block)
        self.xrow = [sum(self.nx[:l]) for l in range(LEVELS)]
        self.yrow = [sum(self.ny[:l]) for l in range(LEVELS)]
        self.zrow = [sum(self.gz[:l]) for l in range(LEVELS)]
        self.yset, self.zset = self.ny[-1], self.gz[-1]
        self.ytable = 2 * HALO
        self.ztable = self.ytable + len(SETS) * self.yset

    def y_nodes(self, l):
        m = LEVELS - l
        return [m * k + s for s in ORDER[l] for k in range(self.yset)]

    def node_table(self):
        def frac(node, cells):
            return (2 * node * 2**32 + cells) // (2 * cells)

        flat = [frac(r, g) for g, n in zip(self.gx, self.nx) for r in range(n)]
        flat += [0] * (HALO - len(flat))
        flat += [frac(c, g) for g, n, c in zip(self.gy, self.nx, self.ny) for _ in range(n)]
        flat += [0] * (2 * HALO - len(flat))
        for cells, count in ((self.gy, self.yset), (self.gz, self.zset)):
            for (l, s), _ in SETS:
                flat += [frac((LEVELS - l) * k + s, cells[l]) for k in range(count)]
        flat = np.array(flat, np.int64) + 2**31
        flat = ((flat + 2**31) % 2**32 - 2**31).astype(np.int32)
        return np.repeat(flat[:, None], LANES, axis=1)

    def factor_table(self):
        k = [exponent(g) for g, n in zip(self.gx, self.nx) for _ in range(n)]
        h = [exponent(g) for g, n in zip(self.gy, self.nx) for _ in range(n)]
        pad = [0.0] * (HALO - len(k))
        return np.repeat(np.array(k + pad + h + pad, np.float32)[:, None], LANES, axis=1)

    def y_matrix(self, l):
        fine = self.rows[1]
        nx, ny, main = self.nx[l], self.ny[l], self.main[l]
        b = np.arange(fine)[:, None]
        y = np.array(self.y_nodes(l) + [ny])[None, :]
        hat = np.maximum(0.0, 1.0 - np.abs(y - b * self.gy[l] / FINE_Y))
        out = np.zeros((nx * fine, self.block[l]), np.float32)
        for x in range(nx):
            out[x * fine : (x + 1) * fine, x * ny : (x + 1) * ny] = hat[:, :ny]
            out[x * fine : (x + 1) * fine, main + self.xrow[l] + x] = hat[:, ny]
        return out

    def x_matrix(self, l):
        a = np.arange(self.rows[0])[:, None]
        x = np.arange(self.nx[l])[None, :]
        return np.maximum(0.0, 1.0 - np.abs(x - a * self.gx[l] / FINE_X))

    def constants(self):
        twice = lambda m: jnp.asarray(np.concatenate([m, m], axis=1), jnp.bfloat16)
        down = [twice(self.y_matrix(l)) for l in range(LEVELS)]
        up = [twice(self.y_matrix(l).T) for l in range(LEVELS)]
        return [jnp.asarray(self.node_table()), jnp.asarray(self.factor_table())] + down + up


def split(value):
    high = value.astype(jnp.bfloat16)
    low = (value - high.astype(jnp.float32)).astype(jnp.bfloat16)
    return high, low


def kernel(plan, n_in, *refs):
    hbm, refs = refs[:n_in], refs[n_in:]
    field, energy, refs = refs[0], refs[1], refs[2:]
    held_in, refs = refs[:n_in], refs[n_in:]
    (
        buf, planes, wz, wx, acc, other, dual, dual_other, pz, t2, field_v, ez, ex,
        in_sem, zs_sem, zr_sem, xs_sem, xr_sem, ps_sem, pr_sem, es_sem, er_sem, fs_sem, fr_sem, o_sem,
    ) = refs
    cx, cy, cz, off, charge, count, amp, dens_v, nodes, factors = held_in[:10]
    down, up = held_in[10 : 10 + LEVELS], held_in[10 + LEVELS :]
    slabs, cols = plan.slabs, plan.cols
    half = slabs // 2
    reach = half // 2
    me = lax.axis_index("slab")
    col = lax.axis_index("blk")
    core = lax.axis_index("sub")
    wide = 2 * BQ
    fine_y = plan.rows[1]

    def at(ds, dc, dk):
        return {
            "slab": lax.rem(me + slabs + ds, slabs),
            "blk": lax.rem(col + cols + dc, cols),
            "sub": lax.rem(core + dk, 2),
        }

    order = [0]
    for d in range(1, half):
        order += [d, -d]
    order.append(half)
    others = [(dc, dk) for dc in range(cols) for dk in range(2)][1:]

    barrier = pltpu.get_barrier_semaphore()
    near = order[1 : 2 * reach] + [reach, -reach]
    near = [d for i, d in enumerate(near) if d not in near[:i]]
    for ds in near:
        pl.semaphore_signal(barrier, inc=1, device_id=at(ds, 0, 0), device_id_type=MESH)
    for dc, dk in others:
        pl.semaphore_signal(barrier, inc=1, device_id=at(0, dc, dk), device_id_type=MESH)

    loads = [pltpu.make_async_copy(hbm[i], held_in[i], in_sem.at[i]) for i in range(n_in)]
    for load in loads:
        load.start()
    for i in range(6):
        loads[i].wait()

    lane = lax.broadcasted_iota(jnp.int32, (1, BQ), 1)
    live = jnp.where(lane < count[...], 1.0, 0.0).astype(jnp.float32)
    buf[0, 0, 0:1, 0:BQ] = charge[...] * live
    buf[0, 0, 1:2, 0:BQ] = cx[...].astype(jnp.float32) + off[0:1, :]
    buf[0, 0, 2:3, 0:BQ] = cy[...].astype(jnp.float32) + off[1:2, :]
    buf[0, 0, 3:4, 0:BQ] = cz[...].astype(jnp.float32) + off[2:3, :]

    pl.semaphore_wait(barrier, len(near) + len(others))

    def slot(j, part):
        return buf.at[0, j, :, pl.ds(part * BQ, BQ)]

    def z_copy(src, j, part, ds):
        return pltpu.make_async_remote_copy(
            src_ref=src, dst_ref=slot(j, part), send_sem=zs_sem.at[j, part], recv_sem=zr_sem.at[j, part],
            device_id=at(ds, 0, 0), device_id_type=MESH,
        )

    for k in range(2 * reach, 0, -1):
        z_copy(slot(0, 0), k // 2, k % 2, -order[k]).start()

    def x_copy(p, j):
        return pltpu.make_async_remote_copy(
            src_ref=buf.at[0, j], dst_ref=buf.at[p, j], send_sem=xs_sem.at[p, j], recv_sem=xr_sem.at[p, j],
            device_id=at(0, -p, 0), device_id_type=MESH,
        )

    acc[...] = jnp.zeros_like(acc)
    planes[1] = jnp.zeros(planes.shape[1:], planes.dtype)
    wz[1] = jnp.zeros(wz.shape[1:], wz.dtype)

    row = lax.broadcasted_iota(jnp.int32, (LANES, LANES), 0)
    fine = lax.broadcasted_iota(jnp.int32, (LANES, LANES), 1) + core * LANES
    for l in range(LEVELS):
        g = plan.gz[l]
        place = row // plan.zset
        part = (place % 2) * 2 + place // 2 if l == 0 else place
        node = (row % plan.zset) * (LEVELS - l) + part
        moved = node * FINE_Z - fine * g
        moved = jnp.where(moved < 0, moved + g * FINE_Z, moved)
        moved = jnp.where(moved * 2 >= g * FINE_Z, moved - g * FINE_Z, moved)
        hat = jnp.maximum(0.0, 1.0 - jnp.abs(moved.astype(jnp.float32)) * (1.0 / FINE_Z))
        hat = jnp.where(row < g, hat, 0.0).astype(jnp.bfloat16)
        pz[l, 0:LANES, :] = hat
        pz[l, LANES:, :] = hat

    for i in range(6, n_in):
        loads[i].wait()
    for l in range(LEVELS):
        hats = plan.x_matrix(l)
        for x in range(plan.nx[l]):
            value = None
            for a in range(plan.rows[0]):
                if hats[a, x] > 0.0:
                    term = float(hats[a, x]) * dens_v[a]
                    value = term if value is None else value + term
            at_x = (plan.xrow[l] + x) * fine_y
            t2[at_x : at_x + fine_y, :] = value * amp[l]
        start, rows = plan.start[l], plan.block[l]
        along = t2[plan.xrow[l] * fine_y : (plan.xrow[l] + plan.nx[l]) * fine_y, :]
        on_y = jnp.dot(up[l][...], jnp.concatenate(split(along), axis=0), preferred_element_type=jnp.float32)
        both = lax.dot_general(
            jnp.concatenate(split(on_y), axis=0), pz[l, 0:LANES, :], (((1,), (1,)), ((), ())),
            preferred_element_type=jnp.float32,
        )
        dual[start : start + rows, :] = both[:rows] + both[rows:]

    def swap(k, src, dst):
        return pltpu.make_async_remote_copy(
            src_ref=src, dst_ref=dst, send_sem=ps_sem.at[k], recv_sem=pr_sem.at[k],
            device_id=at(0, 0, 1), device_id_type=MESH,
        )

    swap(0, dual, dual_other).start()

    scale = 2.0**32
    top = 2.0**31 - 128.0

    def fixed(line, cells):
        moved = jnp.minimum((line - 0.5 * cells) * (scale / cells), top)
        return moved.astype(jnp.int32)

    def broad(table):
        return jnp.concatenate([table] * (SPAN // LANES), axis=1)

    def weigh(p, j, s):
        for c in range(0, wide, SPAN):
            lanes = slice(c, c + SPAN)
            chunk = buf[p, j, :, lanes]
            ux = fixed(chunk[1:2, :], G0X) - me * (2**32 // slabs)
            uy = fixed(chunk[2:3, :], G0Y) - col * (2**32 // cols)
            uz = fixed(chunk[3:4, :], G0Z)

            def squared(first, rows, at_line, factor):
                wrapped = (broad(nodes[first : first + rows, :]) - at_line).astype(jnp.float32)
                return wrapped * wrapped * factor

            for i, ((l0, _), uses) in enumerate(SETS):
                for r in range(0, plan.zset, ROWS):
                    power = squared(plan.ztable + i * plan.zset + r, ROWS, uz, exponent(plan.gz[l0]))
                    for l, place, times in uses:
                        value = jnp.exp2(power if times == 1.0 else power * times).astype(jnp.bfloat16)
                        to = plan.zrow[l] + place * plan.zset + r
                        wz[s, to : to + ROWS, lanes] = value
            along_y = [[None] * len(ORDER[l]) for l in range(LEVELS)]
            for i, ((l0, _), uses) in enumerate(SETS):
                power = squared(plan.ytable + i * plan.yset, plan.yset, uy, exponent(plan.gy[l0]))
                for l, place, times in uses:
                    along_y[l][place] = jnp.exp2(power if times == 1.0 else power * times)
            weighted = chunk[0:1, :] * jnp.exp2(squared(0, HALO, ux, broad(factors[0:HALO, :])))
            last = jnp.exp2(squared(HALO, HALO, uy, broad(factors[HALO : 2 * HALO, :])))
            wx[s, :, lanes] = weighted
            edge = (weighted * last).astype(jnp.bfloat16)
            for l in range(LEVELS):
                start, main, ny = plan.start[l], plan.main[l], plan.ny[l]
                planes[s, start + main : start + main + HALO, lanes] = edge
                tiles = [
                    wx[s, plan.xrow[l] + x : plan.xrow[l] + x + 1, lanes] * on_y
                    for x in range(plan.nx[l]) for on_y in along_y[l]
                ]
                for t, tile in enumerate(tiles):
                    to = start + t * plan.yset
                    planes[s, to : to + plan.yset, lanes] = tile.astype(jnp.bfloat16)

    def gather_in(s):
        for l in range(LEVELS):
            start, rows = plan.start[l], plan.block[l]
            acc[start : start + rows, 0 : plan.gz[l]] += lax.dot_general(
                planes[s, start : start + rows, :], wz[s, plan.zrow[l] : plan.zrow[l] + plan.gz[l], :],
                (((1,), (1,)), ((), ())), preferred_element_type=jnp.float32,
            )

    def arrive(j):
        pair = half // 2

        @pl.when(j > 0)
        def _():
            z_copy(slot(0, 0), j, 0, 1).wait_recv()

        z_copy(slot(0, 0), j, 1, 1).wait_recv()

        @pl.when((j > 0) & (j < pair))
        def _():
            z_copy(slot(j, 0), j + pair, 0, reach).start()

        @pl.when(j < pair)
        def _():
            z_copy(slot(j, 1), j + pair, 1, -reach).start()

        for p in range(1, cols):
            x_copy(p, j).start()

    steps = half // 2
    far = steps // 2
    turn = far + cols - 1
    rest = turn + steps - far

    @pl.loop(0, steps * cols)
    def _(t):
        early, late = t < far, t >= rest
        own = early | ((t >= turn) & (t < rest))
        p = jnp.where(own, 0, jnp.where(late, lax.rem(t + (cols - 1) * rest - rest, cols - 1) + 1, t - far + 1))
        m = jnp.where(early, t, jnp.where(late, lax.div(t + (cols - 1) - rest, cols - 1), jnp.where(own, t - turn + far, 0)))

        @pl.when((t == 0) | (t == turn))
        def _():
            first = jnp.where(t == 0, 0, 2 * far)

            @pl.loop(0, 2 * far)
            def _(j):
                arrive(first + j)

        @pl.when(p > 0)
        def _():
            x_copy(p, 2 * m).wait_recv()
            x_copy(p, 2 * m + 1).wait_recv()

        gather_in(1)
        weigh(p, 2 * m, 0)
        gather_in(0)
        weigh(p, 2 * m + 1, 1)

    gather_in(1)
    swap(1, acc, other).start()
    swap(0, dual, dual_other).wait_recv()
    ez[0] = jnp.sum(acc[...] * (dual[...] + dual_other[...]), axis=0, keepdims=True)

    def e_copy(k):
        return pltpu.make_async_remote_copy(
            src_ref=ez.at[0], dst_ref=ez.at[k], send_sem=es_sem.at[k], recv_sem=er_sem.at[k],
            device_id=at(-order[k], 0, 0), device_id_type=MESH,
        )

    for k in range(slabs - 1, 0, -1):
        e_copy(k).start()
    swap(1, acc, other).wait_recv()

    for l in range(LEVELS):
        start, rows = plan.start[l], plan.block[l]
        cube = acc[start : start + rows, :] + other[start : start + rows, :]
        along_z = jnp.dot(jnp.concatenate(split(cube), axis=1), pz[l], preferred_element_type=jnp.float32)
        t2[plan.xrow[l] * fine_y : (plan.xrow[l] + plan.nx[l]) * fine_y, :] = amp[l] * jnp.dot(
            down[l][...], jnp.concatenate(split(along_z), axis=0), preferred_element_type=jnp.float32
        )
    for a in range(plan.rows[0]):
        value = None
        for l in range(LEVELS):
            hat = plan.x_matrix(l)[a]
            for x in range(plan.nx[l]):
                if hat[x] > 0.0:
                    at_x = (plan.xrow[l] + x) * fine_y
                    term = float(hat[x]) * t2[at_x : at_x + fine_y, :]
                    value = term if value is None else value + term
        field_v[a] = value
    store = pltpu.make_async_copy(field_v, field, o_sem)
    store.start()

    for k in range(1, slabs):
        e_copy(k).wait_recv()
    ex[0] = jnp.sum(ez[...], axis=0)

    def f_copy(k):
        dc, dk = others[k - 1]
        return pltpu.make_async_remote_copy(
            src_ref=ex.at[0], dst_ref=ex.at[k], send_sem=fs_sem.at[k], recv_sem=fr_sem.at[k],
            device_id=at(0, -dc, dk), device_id_type=MESH,
        )

    for k in range(len(others), 0, -1):
        f_copy(k).start()

    for k in range(1, slabs):
        z_copy(slot(0, 0), k // 2, k % 2, 1).wait_send()
        e_copy(k).wait_send()

    @pl.loop(0, half)
    def _(j):
        for p in range(1, cols):
            x_copy(p, j).wait_send()

    swap(0, dual, dual_other).wait_send()
    swap(1, acc, other).wait_send()
    store.wait()
    for k in range(1, len(others) + 1):
        f_copy(k).wait_recv()
    energy[0, 0] = jnp.sum(jnp.sum(ex[...], axis=0)) * (1.0 / (FINE_X * FINE_Y * FINE_Z))
    for k in range(1, len(others) + 1):
        f_copy(k).wait_send()


def on_device(cell_x, cell_y, cell_z, offsets, charge, block_count, level_amplitude, density):
    slabs, cols = lax.axis_size("slab"), lax.axis_size("blk")
    plan = Plan(slabs, cols, *density.shape)
    slots = cell_x.shape[0]
    operands = [
        cell_x.reshape(1, slots), cell_y.reshape(1, slots), cell_z.reshape(1, slots), offsets,
        charge.reshape(1, slots), block_count.reshape(1, 1), level_amplitude, density, *plan.constants(),
    ]
    n_in = len(operands)
    spaces = [pltpu.VMEM] * 6 + [pltpu.SMEM] + [pltpu.VMEM] * (n_in - 7)
    smem = pl.BlockSpec(memory_space=pltpu.SMEM)
    anywhere = pl.BlockSpec(memory_space=pl.ANY)
    dma = pltpu.SemaphoreType.DMA
    field, energy = pl.pallas_call(
        functools.partial(kernel, plan, n_in),
        out_shape=(jax.ShapeDtypeStruct(density.shape, jnp.float32), jax.ShapeDtypeStruct((1, 1), jnp.float32)),
        in_specs=[anywhere] * n_in,
        out_specs=(anywhere, smem),
        scratch_shapes=[space(o.shape, o.dtype) for space, o in zip(spaces, operands)]
        + [
            pltpu.VMEM((cols, slabs // 2, 4, 2 * BQ), jnp.float32),
            pltpu.VMEM((2, plan.total, 2 * BQ), jnp.bfloat16),
            pltpu.VMEM((2, sum(plan.gz), 2 * BQ), jnp.bfloat16),
            pltpu.VMEM((2, HALO, 2 * BQ), jnp.float32),
            pltpu.VMEM((plan.total, LANES), jnp.float32),
            pltpu.VMEM((plan.total, LANES), jnp.float32),
            pltpu.VMEM((plan.total, LANES), jnp.float32),
            pltpu.VMEM((plan.total, LANES), jnp.float32),
            pltpu.VMEM((LEVELS, 2 * LANES, LANES), jnp.bfloat16),
            pltpu.VMEM((sum(plan.nx) * density.shape[1], LANES), jnp.float32),
            pltpu.VMEM(density.shape, jnp.float32),
            pltpu.VMEM((slabs, 1, LANES), jnp.float32),
            pltpu.VMEM((2 * cols, 1, LANES), jnp.float32),
            dma((n_in,)),
            dma((slabs // 2, 2)), dma((slabs // 2, 2)),
            dma((cols, slabs // 2)), dma((cols, slabs // 2)),
            dma((2,)), dma((2,)),
            dma((slabs,)), dma((slabs,)),
            dma((2 * cols,)), dma((2 * cols,)),
            dma,
        ],
        compiler_params=pltpu.CompilerParams(collective_id=0, has_side_effects=True),
    )(*operands)
    return field, energy.reshape(1)


def solution(mesh):
    split_all = ("grp", "slab", "blk", "sub")
    in_specs = (
        P(split_all), P(split_all), P(split_all), P(None, split_all), P(split_all), P(split_all), P(),
        P(("grp", "slab"), "blk", "sub"),
    )
    out_specs = (P(("grp", "slab"), "blk", "sub"), P("grp"))
    return jax.shard_map(on_device, mesh=mesh, in_specs=in_specs, out_specs=out_specs, check_vma=False)
```

```python
import functools

import jax
import jax.numpy as jnp
import numpy as np
from jax import lax
from jax.experimental import pallas as pl
from jax.experimental.pallas import tpu as pltpu
from jax.sharding import PartitionSpec as P

G0X = 64
G0Y = 128
G0Z = 128
FINE_X = 256
FINE_Y = 256
FINE_Z = 256
BQ = 256
LEVELS = 4
LANES = 128
SPAN = 256
ROWS = 8
HALO = 16
spread_width = 1.25
MESH = pl.DeviceIdType.MESH

ORDER = ((0, 2, 1, 3), (0, 1, 2), (0, 1), (0,))
SETS = (
    ((3, 0), ((3, 0, 1.0), (2, 0, 4.0), (1, 0, 9.0), (0, 0, 16.0))),
    ((2, 1), ((2, 1, 1.0), (0, 1, 4.0))),
    ((1, 1), ((1, 1, 1.0),)),
    ((1, 2), ((1, 2, 1.0),)),
    ((0, 1), ((0, 2, 1.0),)),
    ((0, 3), ((0, 3, 1.0),)),
)


def coarse_cells(base, level):
    return base * (4 - level) // 4


def exponent(cells):
    return -0.5 * np.log2(np.e) / spread_width**2 * (cells / 2.0**32) ** 2


class Plan:
    def __init__(self, slabs, cols, rows_x, rows_y, rows_z):
        self.slabs, self.cols = slabs, cols
        self.rows = (rows_x, rows_y, rows_z)
        self.gx = [coarse_cells(G0X, l) for l in range(LEVELS)]
        self.gy = [coarse_cells(G0Y, l) for l in range(LEVELS)]
        self.gz = [coarse_cells(G0Z, l) for l in range(LEVELS)]
        self.nx = [g // slabs + 1 for g in self.gx]
        self.ny = [g // cols for g in self.gy]
        self.main = [a * b for a, b in zip(self.nx, self.ny)]
        self.block = [m + HALO for m in self.main]
        self.start = [sum(self.block[:l]) for l in range(LEVELS)]
        self.total = sum(self.block)
        self.xrow = [sum(self.nx[:l]) for l in range(LEVELS)]
        self.yrow = [sum(self.ny[:l]) for l in range(LEVELS)]
        self.zrow = [sum(self.gz[:l]) for l in range(LEVELS)]
        self.yset, self.zset = self.ny[-1], self.gz[-1]
        self.ytable = 2 * HALO
        self.ztable = self.ytable + len(SETS) * self.yset

    def y_nodes(self, l):
        m = LEVELS - l
        return [m * k + s for s in ORDER[l] for k in range(self.yset)]

    def node_table(self):
        def frac(node, cells):
            return (2 * node * 2**32 + cells) // (2 * cells)

        flat = [frac(r, g) for g, n in zip(self.gx, self.nx) for r in range(n)]
        flat += [0] * (HALO - len(flat))
        flat += [frac(c, g) for g, n, c in zip(self.gy, self.nx, self.ny) for _ in range(n)]
        flat += [0] * (2 * HALO - len(flat))
        for cells, count in ((self.gy, self.yset), (self.gz, self.zset)):
            for (l, s), _ in SETS:
                flat += [frac((LEVELS - l) * k + s, cells[l]) for k in range(count)]
        flat = np.array(flat, np.int64) + 2**31
        flat = ((flat + 2**31) % 2**32 - 2**31).astype(np.int32)
        return np.repeat(flat[:, None], LANES, axis=1)

    def factor_table(self):
        k = [exponent(g) for g, n in zip(self.gx, self.nx) for _ in range(n)]
        h = [exponent(g) for g, n in zip(self.gy, self.nx) for _ in range(n)]
        pad = [0.0] * (HALO - len(k))
        return np.repeat(np.array(k + pad + h + pad, np.float32)[:, None], LANES, axis=1)

    def y_matrix(self, l):
        fine = self.rows[1]
        nx, ny, main = self.nx[l], self.ny[l], self.main[l]
        b = np.arange(fine)[:, None]
        y = np.array(self.y_nodes(l) + [ny])[None, :]
        hat = np.maximum(0.0, 1.0 - np.abs(y - b * self.gy[l] / FINE_Y))
        out = np.zeros((nx * fine, self.block[l]), np.float32)
        for x in range(nx):
            out[x * fine : (x + 1) * fine, x * ny : (x + 1) * ny] = hat[:, :ny]
            out[x * fine : (x + 1) * fine, main + self.xrow[l] + x] = hat[:, ny]
        return out

    def x_matrix(self, l):
        a = np.arange(self.rows[0])[:, None]
        x = np.arange(self.nx[l])[None, :]
        return np.maximum(0.0, 1.0 - np.abs(x - a * self.gx[l] / FINE_X))

    def constants(self):
        twice = lambda m: jnp.asarray(np.concatenate([m, m], axis=1), jnp.bfloat16)
        down = [twice(self.y_matrix(l)) for l in range(LEVELS)]
        up = [twice(self.y_matrix(l).T) for l in range(LEVELS)]
        return [jnp.asarray(self.node_table()), jnp.asarray(self.factor_table())] + down + up


def split(value):
    high = value.astype(jnp.bfloat16)
    low = (value - high.astype(jnp.float32)).astype(jnp.bfloat16)
    return high, low


def kernel(plan, n_in, *refs):
    hbm, refs = refs[:n_in], refs[n_in:]
    field, energy, refs = refs[0], refs[1], refs[2:]
    held_in, refs = refs[:n_in], refs[n_in:]
    (
        buf, planes, wz, wx, acc, other, dual, dual_other, pz, t2, field_v, ez, ex,
        in_sem, zs_sem, zr_sem, xs_sem, xr_sem, ps_sem, pr_sem, es_sem, er_sem, fs_sem, fr_sem, o_sem,
    ) = refs
    cx, cy, cz, off, charge, count, amp, dens_v, nodes, factors = held_in[:10]
    down, up = held_in[10 : 10 + LEVELS], held_in[10 + LEVELS :]
    slabs, cols = plan.slabs, plan.cols
    half = slabs // 2
    reach = half // 2
    me = lax.axis_index("slab")
    col = lax.axis_index("blk")
    core = lax.axis_index("sub")
    wide = 2 * BQ
    fine_y = plan.rows[1]

    def at(ds, dc, dk):
        return {
            "slab": lax.rem(me + slabs + ds, slabs),
            "blk": lax.rem(col + cols + dc, cols),
            "sub": lax.rem(core + dk, 2),
        }

    order = [0]
    for d in range(1, half):
        order += [d, -d]
    order.append(half)
    others = [(dc, dk) for dc in range(cols) for dk in range(2)][1:]

    barrier = pltpu.get_barrier_semaphore()
    near = order[1 : 2 * reach] + [reach, -reach]
    near = [d for i, d in enumerate(near) if d not in near[:i]]
    for ds in near:
        pl.semaphore_signal(barrier, inc=1, device_id=at(ds, 0, 0), device_id_type=MESH)
    for dc, dk in others:
        pl.semaphore_signal(barrier, inc=1, device_id=at(0, dc, dk), device_id_type=MESH)

    loads = [pltpu.make_async_copy(hbm[i], held_in[i], in_sem.at[i]) for i in range(n_in)]
    for load in loads:
        load.start()
    for i in range(6):
        loads[i].wait()

    lane = lax.broadcasted_iota(jnp.int32, (1, BQ), 1)
    live = jnp.where(lane < count[...], 1.0, 0.0).astype(jnp.float32)
    buf[0, 0, 0:1, 0:BQ] = charge[...] * live
    buf[0, 0, 1:2, 0:BQ] = cx[...].astype(jnp.float32) + off[0:1, :]
    buf[0, 0, 2:3, 0:BQ] = cy[...].astype(jnp.float32) + off[1:2, :]
    buf[0, 0, 3:4, 0:BQ] = cz[...].astype(jnp.float32) + off[2:3, :]

    pl.semaphore_wait(barrier, len(near) + len(others))

    def slot(j, part):
        return buf.at[0, j, :, pl.ds(part * BQ, BQ)]

    def z_copy(src, j, part, ds):
        return pltpu.make_async_remote_copy(
            src_ref=src, dst_ref=slot(j, part), send_sem=zs_sem.at[j, part], recv_sem=zr_sem.at[j, part],
            device_id=at(ds, 0, 0), device_id_type=MESH,
        )

    for k in range(2 * reach, 0, -1):
        z_copy(slot(0, 0), k // 2, k % 2, -order[k]).start()

    def x_copy(p, j):
        return pltpu.make_async_remote_copy(
            src_ref=buf.at[0, j], dst_ref=buf.at[p, j], send_sem=xs_sem.at[p, j], recv_sem=xr_sem.at[p, j],
            device_id=at(0, -p, 0), device_id_type=MESH,
        )

    acc[...] = jnp.zeros_like(acc)
    planes[1] = jnp.zeros(planes.shape[1:], planes.dtype)
    wz[1] = jnp.zeros(wz.shape[1:], wz.dtype)

    row = lax.broadcasted_iota(jnp.int32, (LANES, LANES), 0)
    fine = lax.broadcasted_iota(jnp.int32, (LANES, LANES), 1) + core * LANES
    for l in range(LEVELS):
        g = plan.gz[l]
        place = row // plan.zset
        part = (place % 2) * 2 + place // 2 if l == 0 else place
        node = (row % plan.zset) * (LEVELS - l) + part
        moved = node * FINE_Z - fine * g
        moved = jnp.where(moved < 0, moved + g * FINE_Z, moved)
        moved = jnp.where(moved * 2 >= g * FINE_Z, moved - g * FINE_Z, moved)
        hat = jnp.maximum(0.0, 1.0 - jnp.abs(moved.astype(jnp.float32)) * (1.0 / FINE_Z))
        hat = jnp.where(row < g, hat, 0.0).astype(jnp.bfloat16)
        pz[l, 0:LANES, :] = hat
        pz[l, LANES:, :] = hat

    for i in range(6, n_in):
        loads[i].wait()
    for l in range(LEVELS):
        hats = plan.x_matrix(l)
        for x in range(plan.nx[l]):
            value = None
            for a in range(plan.rows[0]):
                if hats[a, x] > 0.0:
                    term = float(hats[a, x]) * dens_v[a]
                    value = term if value is None else value + term
            at_x = (plan.xrow[l] + x) * fine_y
            t2[at_x : at_x + fine_y, :] = value * amp[l]
        start, rows = plan.start[l], plan.block[l]
        along = t2[plan.xrow[l] * fine_y : (plan.xrow[l] + plan.nx[l]) * fine_y, :]
        on_y = jnp.dot(up[l][...], jnp.concatenate(split(along), axis=0), preferred_element_type=jnp.float32)
        both = lax.dot_general(
            jnp.concatenate(split(on_y), axis=0), pz[l, 0:LANES, :], (((1,), (1,)), ((), ())),
            preferred_element_type=jnp.float32,
        )
        dual[start : start + rows, :] = both[:rows] + both[rows:]

    def swap(k, src, dst):
        return pltpu.make_async_remote_copy(
            src_ref=src, dst_ref=dst, send_sem=ps_sem.at[k], recv_sem=pr_sem.at[k],
            device_id=at(0, 0, 1), device_id_type=MESH,
        )

    swap(0, dual, dual_other).start()

    scale = 2.0**32
    top = 2.0**31 - 128.0

    def fixed(line, cells):
        moved = jnp.minimum((line - 0.5 * cells) * (scale / cells), top)
        return moved.astype(jnp.int32)

    def broad(table):
        return jnp.concatenate([table] * (SPAN // LANES), axis=1)

    def weigh(p, j, s, beside):
        for turn_of, c in enumerate(range(0, wide, SPAN)):
            lanes = slice(c, c + SPAN)
            chunk = buf[p, j, :, lanes]
            ux = fixed(chunk[1:2, :], G0X) - me * (2**32 // slabs)
            uy = fixed(chunk[2:3, :], G0Y) - col * (2**32 // cols)
            uz = fixed(chunk[3:4, :], G0Z)

            def squared(first, rows, at_line, factor):
                wrapped = (broad(nodes[first : first + rows, :]) - at_line).astype(jnp.float32)
                return wrapped * wrapped * factor

            for i, ((l0, _), uses) in enumerate(SETS):
                for r in range(0, plan.zset, ROWS):
                    power = squared(plan.ztable + i * plan.zset + r, ROWS, uz, exponent(plan.gz[l0]))
                    for l, place, times in uses:
                        value = jnp.exp2(power if times == 1.0 else power * times).astype(jnp.bfloat16)
                        to = plan.zrow[l] + place * plan.zset + r
                        wz[s, to : to + ROWS, lanes] = value
            beside(2 * turn_of)
            along_y = [[None] * len(ORDER[l]) for l in range(LEVELS)]
            for i, ((l0, _), uses) in enumerate(SETS):
                power = squared(plan.ytable + i * plan.yset, plan.yset, uy, exponent(plan.gy[l0]))
                for l, place, times in uses:
                    along_y[l][place] = jnp.exp2(power if times == 1.0 else power * times)
            beside(2 * turn_of + 1)
            weighted = chunk[0:1, :] * jnp.exp2(squared(0, HALO, ux, broad(factors[0:HALO, :])))
            last = jnp.exp2(squared(HALO, HALO, uy, broad(factors[HALO : 2 * HALO, :])))
            wx[s, :, lanes] = weighted
            edge = (weighted * last).astype(jnp.bfloat16)
            for l in range(LEVELS):
                start, main, ny = plan.start[l], plan.main[l], plan.ny[l]
                planes[s, start + main : start + main + HALO, lanes] = edge
                tiles = [
                    wx[s, plan.xrow[l] + x : plan.xrow[l] + x + 1, lanes] * on_y
                    for x in range(plan.nx[l]) for on_y in along_y[l]
                ]
                for t, tile in enumerate(tiles):
                    to = start + t * plan.yset
                    planes[s, to : to + plan.yset, lanes] = tile.astype(jnp.bfloat16)

    def gather_in(s, *levels):
        for l in levels or range(LEVELS):
            start, rows = plan.start[l], plan.block[l]
            acc[start : start + rows, 0 : plan.gz[l]] += lax.dot_general(
                planes[s, start : start + rows, :], wz[s, plan.zrow[l] : plan.zrow[l] + plan.gz[l], :],
                (((1,), (1,)), ((), ())), preferred_element_type=jnp.float32,
            )

    def arrive(j):
        pair = half // 2

        @pl.when(j > 0)
        def _():
            z_copy(slot(0, 0), j, 0, 1).wait_recv()

        z_copy(slot(0, 0), j, 1, 1).wait_recv()

        @pl.when((j > 0) & (j < pair))
        def _():
            z_copy(slot(j, 0), j + pair, 0, reach).start()

        @pl.when(j < pair)
        def _():
            z_copy(slot(j, 1), j + pair, 1, -reach).start()

        for p in range(1, cols):
            x_copy(p, j).start()

    steps = half // 2
    far = steps // 2
    turn = far + cols - 1
    rest = turn + steps - far

    @pl.loop(0, 2 * steps * cols)
    def _(group):
        t, half_of = lax.div(group, 2), lax.rem(group, 2)
        early, late = t < far, t >= rest
        own = early | ((t >= turn) & (t < rest))
        p = jnp.where(own, 0, jnp.where(late, lax.rem(t + (cols - 1) * rest - rest, cols - 1) + 1, t - far + 1))
        m = jnp.where(early, t, jnp.where(late, lax.div(t + (cols - 1) - rest, cols - 1), jnp.where(own, t - turn + far, 0)))
        j = 2 * m + half_of

        @pl.when(early | (group == 2 * turn))
        def _():
            @pl.loop(0, jnp.where(early, 1, 2 * (steps - far)))
            def _(k):
                arrive(j + k)

        @pl.when(p > 0)
        def _():
            x_copy(p, j).wait_recv()

        for s in range(2):

            @pl.when(half_of == s)
            def _():
                weigh(p, j, s, lambda l: gather_in(1 - s, l))

    gather_in(1)
    swap(1, acc, other).start()
    swap(0, dual, dual_other).wait_recv()
    ez[0] = jnp.sum(acc[...] * (dual[...] + dual_other[...]), axis=0, keepdims=True)

    def e_copy(k):
        return pltpu.make_async_remote_copy(
            src_ref=ez.at[0], dst_ref=ez.at[k], send_sem=es_sem.at[k], recv_sem=er_sem.at[k],
            device_id=at(-order[k], 0, 0), device_id_type=MESH,
        )

    for k in range(slabs - 1, 0, -1):
        e_copy(k).start()
    swap(1, acc, other).wait_recv()

    for l in range(LEVELS):
        start, rows = plan.start[l], plan.block[l]
        cube = acc[start : start + rows, :] + other[start : start + rows, :]
        along_z = jnp.dot(jnp.concatenate(split(cube), axis=1), pz[l], preferred_element_type=jnp.float32)
        t2[plan.xrow[l] * fine_y : (plan.xrow[l] + plan.nx[l]) * fine_y, :] = amp[l] * jnp.dot(
            down[l][...], jnp.concatenate(split(along_z), axis=0), preferred_element_type=jnp.float32
        )
    for a in range(plan.rows[0]):
        value = None
        for l in range(LEVELS):
            hat = plan.x_matrix(l)[a]
            for x in range(plan.nx[l]):
                if hat[x] > 0.0:
                    at_x = (plan.xrow[l] + x) * fine_y
                    term = float(hat[x]) * t2[at_x : at_x + fine_y, :]
                    value = term if value is None else value + term
        field_v[a] = value
    store = pltpu.make_async_copy(field_v, field, o_sem)
    store.start()

    for k in range(1, slabs):
        e_copy(k).wait_recv()
    ex[0] = jnp.sum(ez[...], axis=0)

    def f_copy(k):
        dc, dk = others[k - 1]
        return pltpu.make_async_remote_copy(
            src_ref=ex.at[0], dst_ref=ex.at[k], send_sem=fs_sem.at[k], recv_sem=fr_sem.at[k],
            device_id=at(0, -dc, dk), device_id_type=MESH,
        )

    for k in range(len(others), 0, -1):
        f_copy(k).start()

    for k in range(1, slabs):
        z_copy(slot(0, 0), k // 2, k % 2, 1).wait_send()
        e_copy(k).wait_send()

    @pl.loop(0, half)
    def _(j):
        for p in range(1, cols):
            x_copy(p, j).wait_send()

    swap(0, dual, dual_other).wait_send()
    swap(1, acc, other).wait_send()
    store.wait()
    for k in range(1, len(others) + 1):
        f_copy(k).wait_recv()
    energy[0, 0] = jnp.sum(jnp.sum(ex[...], axis=0)) * (1.0 / (FINE_X * FINE_Y * FINE_Z))
    for k in range(1, len(others) + 1):
        f_copy(k).wait_send()


def on_device(cell_x, cell_y, cell_z, offsets, charge, block_count, level_amplitude, density):
    slabs, cols = lax.axis_size("slab"), lax.axis_size("blk")
    plan = Plan(slabs, cols, *density.shape)
    slots = cell_x.shape[0]
    operands = [
        cell_x.reshape(1, slots), cell_y.reshape(1, slots), cell_z.reshape(1, slots), offsets,
        charge.reshape(1, slots), block_count.reshape(1, 1), level_amplitude, density, *plan.constants(),
    ]
    n_in = len(operands)
    spaces = [pltpu.VMEM] * 6 + [pltpu.SMEM] + [pltpu.VMEM] * (n_in - 7)
    smem = pl.BlockSpec(memory_space=pltpu.SMEM)
    anywhere = pl.BlockSpec(memory_space=pl.ANY)
    dma = pltpu.SemaphoreType.DMA
    field, energy = pl.pallas_call(
        functools.partial(kernel, plan, n_in),
        out_shape=(jax.ShapeDtypeStruct(density.shape, jnp.float32), jax.ShapeDtypeStruct((1, 1), jnp.float32)),
        in_specs=[anywhere] * n_in,
        out_specs=(anywhere, smem),
        scratch_shapes=[space(o.shape, o.dtype) for space, o in zip(spaces, operands)]
        + [
            pltpu.VMEM((cols, slabs // 2, 4, 2 * BQ), jnp.float32),
            pltpu.VMEM((2, plan.total, 2 * BQ), jnp.bfloat16),
            pltpu.VMEM((2, sum(plan.gz), 2 * BQ), jnp.bfloat16),
            pltpu.VMEM((2, HALO, 2 * BQ), jnp.float32),
            pltpu.VMEM((plan.total, LANES), jnp.float32),
            pltpu.VMEM((plan.total, LANES), jnp.float32),
            pltpu.VMEM((plan.total, LANES), jnp.float32),
            pltpu.VMEM((plan.total, LANES), jnp.float32),
            pltpu.VMEM((LEVELS, 2 * LANES, LANES), jnp.bfloat16),
            pltpu.VMEM((sum(plan.nx) * density.shape[1], LANES), jnp.float32),
            pltpu.VMEM(density.shape, jnp.float32),
            pltpu.VMEM((slabs, 1, LANES), jnp.float32),
            pltpu.VMEM((2 * cols, 1, LANES), jnp.float32),
            dma((n_in,)),
            dma((slabs // 2, 2)), dma((slabs // 2, 2)),
            dma((cols, slabs // 2)), dma((cols, slabs // 2)),
            dma((2,)), dma((2,)),
            dma((slabs,)), dma((slabs,)),
            dma((2 * cols,)), dma((2 * cols,)),
            dma,
        ],
        compiler_params=pltpu.CompilerParams(collective_id=0, has_side_effects=True),
    )(*operands)
    return field, energy.reshape(1)


def solution(mesh):
    split_all = ("grp", "slab", "blk", "sub")
    in_specs = (
        P(split_all), P(split_all), P(split_all), P(None, split_all), P(split_all), P(split_all), P(),
        P(("grp", "slab"), "blk", "sub"),
    )
    out_specs = (P(("grp", "slab"), "blk", "sub"), P("grp"))
    return jax.shard_map(on_device, mesh=mesh, in_specs=in_specs, out_specs=out_specs, check_vma=False)
```

```python
import functools

import jax
import jax.numpy as jnp
import numpy as np
from jax import lax
from jax.experimental import pallas as pl
from jax.experimental.pallas import tpu as pltpu
from jax.sharding import PartitionSpec as P

G0X = 64
G0Y = 128
G0Z = 128
FINE_X = 256
FINE_Y = 256
FINE_Z = 256
BQ = 256
LEVELS = 4
LANES = 128
SPAN = 256
ROWS = 8
FAN = 2
HALO = 16
spread_width = 1.25
MESH = pl.DeviceIdType.MESH

ORDER = ((0, 2, 1, 3), (0, 1, 2), (0, 1), (0,))
SETS = (
    ((3, 0), ((3, 0, 1.0), (2, 0, 4.0), (1, 0, 9.0), (0, 0, 16.0))),
    ((2, 1), ((2, 1, 1.0), (0, 1, 4.0))),
    ((1, 1), ((1, 1, 1.0),)),
    ((1, 2), ((1, 2, 1.0),)),
    ((0, 1), ((0, 2, 1.0),)),
    ((0, 3), ((0, 3, 1.0),)),
)


def coarse_cells(base, level):
    return base * (4 - level) // 4


def exponent(cells):
    return -0.5 * np.log2(np.e) / spread_width**2 * (cells / 2.0**32) ** 2


class Plan:
    def __init__(self, slabs, cols, rows_x, rows_y, rows_z):
        self.slabs, self.cols = slabs, cols
        self.rows = (rows_x, rows_y, rows_z)
        self.gx = [coarse_cells(G0X, l) for l in range(LEVELS)]
        self.gy = [coarse_cells(G0Y, l) for l in range(LEVELS)]
        self.gz = [coarse_cells(G0Z, l) for l in range(LEVELS)]
        self.nx = [g // slabs + 1 for g in self.gx]
        self.ny = [g // cols for g in self.gy]
        self.main = [a * b for a, b in zip(self.nx, self.ny)]
        self.block = [m + HALO for m in self.main]
        self.start = [sum(self.block[:l]) for l in range(LEVELS)]
        self.total = sum(self.block)
        self.xrow = [sum(self.nx[:l]) for l in range(LEVELS)]
        self.yrow = [sum(self.ny[:l]) for l in range(LEVELS)]
        self.zrow = [sum(self.gz[:l]) for l in range(LEVELS)]
        self.yset, self.zset = self.ny[-1], self.gz[-1]
        self.ytable = 2 * HALO
        self.ztable = self.ytable + len(SETS) * self.yset

    def y_nodes(self, l):
        m = LEVELS - l
        return [m * k + s for s in ORDER[l] for k in range(self.yset)]

    def node_table(self):
        def frac(node, cells):
            return (2 * node * 2**32 + cells) // (2 * cells)

        flat = [frac(r, g) for g, n in zip(self.gx, self.nx) for r in range(n)]
        flat += [0] * (HALO - len(flat))
        flat += [frac(c, g) for g, n, c in zip(self.gy, self.nx, self.ny) for _ in range(n)]
        flat += [0] * (2 * HALO - len(flat))
        for cells, count in ((self.gy, self.yset), (self.gz, self.zset)):
            for (l, s), _ in SETS:
                flat += [frac((LEVELS - l) * k + s, cells[l]) for k in range(count)]
        flat = np.array(flat, np.int64) + 2**31
        flat = ((flat + 2**31) % 2**32 - 2**31).astype(np.int32)
        return np.repeat(flat[:, None], LANES, axis=1)

    def factor_table(self):
        k = [exponent(g) for g, n in zip(self.gx, self.nx) for _ in range(n)]
        h = [exponent(g) for g, n in zip(self.gy, self.nx) for _ in range(n)]
        pad = [0.0] * (HALO - len(k))
        return np.repeat(np.array(k + pad + h + pad, np.float32)[:, None], LANES, axis=1)

    def y_matrix(self, l):
        fine = self.rows[1]
        nx, ny, main = self.nx[l], self.ny[l], self.main[l]
        b = np.arange(fine)[:, None]
        y = np.array(self.y_nodes(l) + [ny])[None, :]
        hat = np.maximum(0.0, 1.0 - np.abs(y - b * self.gy[l] / FINE_Y))
        out = np.zeros((nx * fine, self.block[l]), np.float32)
        for x in range(nx):
            out[x * fine : (x + 1) * fine, x * ny : (x + 1) * ny] = hat[:, :ny]
            out[x * fine : (x + 1) * fine, main + self.xrow[l] + x] = hat[:, ny]
        return out

    def x_matrix(self, l):
        a = np.arange(self.rows[0])[:, None]
        x = np.arange(self.nx[l])[None, :]
        return np.maximum(0.0, 1.0 - np.abs(x - a * self.gx[l] / FINE_X))

    def constants(self):
        twice = lambda m: jnp.asarray(np.concatenate([m, m], axis=1), jnp.bfloat16)
        down = [twice(self.y_matrix(l)) for l in range(LEVELS)]
        up = [twice(self.y_matrix(l).T) for l in range(LEVELS)]
        return [jnp.asarray(self.node_table()), jnp.asarray(self.factor_table())] + down + up


def split(value):
    high = value.astype(jnp.bfloat16)
    low = (value - high.astype(jnp.float32)).astype(jnp.bfloat16)
    return high, low


def kernel(plan, n_in, *refs):
    hbm, refs = refs[:n_in], refs[n_in:]
    field, energy, refs = refs[0], refs[1], refs[2:]
    held_in, refs = refs[:n_in], refs[n_in:]
    (
        buf, planes, wz, wx, acc, from_x, other, dual, dual_other, pz, t2, field_v, ez, ex,
        in_sem, zs_sem, zr_sem, xs_sem, xr_sem, ps_sem, pr_sem, ns_sem, nr_sem, es_sem, er_sem, fs_sem, fr_sem, o_sem,
    ) = refs
    cx, cy, cz, off, charge, count, amp, dens_v, nodes, factors = held_in[:10]
    down, up = held_in[10 : 10 + LEVELS], held_in[10 + LEVELS :]
    slabs, cols = plan.slabs, plan.cols
    half = slabs // 2
    reach = half // 2
    me = lax.axis_index("slab")
    col = lax.axis_index("blk")
    core = lax.axis_index("sub")
    beside = 1 - 2 * lax.rem(col, 2)
    wide = 2 * BQ
    fine_y = plan.rows[1]

    def at(ds, dc, dk):
        return {
            "slab": lax.rem(me + slabs + ds, slabs),
            "blk": lax.rem(col + cols + dc, cols),
            "sub": lax.rem(core + dk, 2),
        }

    order = [0]
    for d in range(1, half):
        order += [d, -d]
    order.append(half)
    others = [(dc, dk) for dc in range(cols) for dk in range(2)][1:]

    barrier = pltpu.get_barrier_semaphore()
    near = order[1 : 2 * reach] + [reach, -reach]
    near = [d for i, d in enumerate(near) if d not in near[:i]]
    for ds in near:
        pl.semaphore_signal(barrier, inc=1, device_id=at(ds, 0, 0), device_id_type=MESH)
    for dc, dk in others:
        pl.semaphore_signal(barrier, inc=1, device_id=at(0, dc, dk), device_id_type=MESH)

    loads = [pltpu.make_async_copy(hbm[i], held_in[i], in_sem.at[i]) for i in range(n_in)]
    for load in loads:
        load.start()
    for i in range(6):
        loads[i].wait()

    lane = lax.broadcasted_iota(jnp.int32, (1, BQ), 1)
    live = jnp.where(lane < count[...], 1.0, 0.0).astype(jnp.float32)
    buf[0, 0, 0:1, 0:BQ] = charge[...] * live
    buf[0, 0, 1:2, 0:BQ] = cx[...].astype(jnp.float32) + off[0:1, :]
    buf[0, 0, 2:3, 0:BQ] = cy[...].astype(jnp.float32) + off[1:2, :]
    buf[0, 0, 3:4, 0:BQ] = cz[...].astype(jnp.float32) + off[2:3, :]

    pl.semaphore_wait(barrier, len(near) + len(others))

    def slot(j, part):
        return buf.at[0, j, :, pl.ds(part * BQ, BQ)]

    def z_copy(src, j, part, ds):
        return pltpu.make_async_remote_copy(
            src_ref=src, dst_ref=slot(j, part), send_sem=zs_sem.at[j, part], recv_sem=zr_sem.at[j, part],
            device_id=at(ds, 0, 0), device_id_type=MESH,
        )

    for k in range(2 * reach, 0, -1):
        z_copy(slot(0, 0), k // 2, k % 2, -order[k]).start()

    def x_copy(p, j):
        return pltpu.make_async_remote_copy(
            src_ref=buf.at[0, j], dst_ref=buf.at[p, j], send_sem=xs_sem.at[p, j], recv_sem=xr_sem.at[p, j],
            device_id=at(0, -(cols // FAN), 0), device_id_type=MESH,
        )

    acc[...] = jnp.zeros_like(acc)
    planes[1] = jnp.zeros(planes.shape[1:], planes.dtype)
    wz[1] = jnp.zeros(wz.shape[1:], wz.dtype)

    row = lax.broadcasted_iota(jnp.int32, (LANES, LANES), 0)
    fine = lax.broadcasted_iota(jnp.int32, (LANES, LANES), 1) + core * LANES
    for l in range(LEVELS):
        g = plan.gz[l]
        place = row // plan.zset
        part = (place % 2) * 2 + place // 2 if l == 0 else place
        node = (row % plan.zset) * (LEVELS - l) + part
        moved = node * FINE_Z - fine * g
        moved = jnp.where(moved < 0, moved + g * FINE_Z, moved)
        moved = jnp.where(moved * 2 >= g * FINE_Z, moved - g * FINE_Z, moved)
        hat = jnp.maximum(0.0, 1.0 - jnp.abs(moved.astype(jnp.float32)) * (1.0 / FINE_Z))
        hat = jnp.where(row < g, hat, 0.0).astype(jnp.bfloat16)
        pz[l, 0:LANES, :] = hat
        pz[l, LANES:, :] = hat

    for i in range(6, n_in):
        loads[i].wait()
    for l in range(LEVELS):
        hats = plan.x_matrix(l)
        for x in range(plan.nx[l]):
            value = None
            for a in range(plan.rows[0]):
                if hats[a, x] > 0.0:
                    term = float(hats[a, x]) * dens_v[a]
                    value = term if value is None else value + term
            at_x = (plan.xrow[l] + x) * fine_y
            t2[at_x : at_x + fine_y, :] = value * amp[l]
        start, rows = plan.start[l], plan.block[l]
        along = t2[plan.xrow[l] * fine_y : (plan.xrow[l] + plan.nx[l]) * fine_y, :]
        on_y = jnp.dot(up[l][...], jnp.concatenate(split(along), axis=0), preferred_element_type=jnp.float32)
        both = lax.dot_general(
            jnp.concatenate(split(on_y), axis=0), pz[l, 0:LANES, :], (((1,), (1,)), ((), ())),
            preferred_element_type=jnp.float32,
        )
        dual[0, start : start + rows, :] = both[:rows] + both[rows:]

    def swap(k, src, dst):
        return pltpu.make_async_remote_copy(
            src_ref=src, dst_ref=dst, send_sem=ps_sem.at[k], recv_sem=pr_sem.at[k],
            device_id=at(0, 0, 1), device_id_type=MESH,
        )

    def pass_beside(k, src, dst):
        return pltpu.make_async_remote_copy(
            src_ref=src, dst_ref=dst, send_sem=ns_sem.at[k], recv_sem=nr_sem.at[k],
            device_id=at(0, beside, 0), device_id_type=MESH,
        )

    swap(0, dual.at[0], dual_other).start()
    swap(0, dual.at[0], dual_other).wait()
    dual[0] = dual[0] + dual_other[...]
    pass_beside(0, dual.at[0], dual.at[1]).start()

    scale = 2.0**32
    top = 2.0**31 - 128.0

    def fixed(line, cells):
        moved = jnp.minimum((line - 0.5 * cells) * (scale / cells), top)
        return moved.astype(jnp.int32)

    def broad(table):
        return jnp.concatenate([table] * (SPAN // LANES), axis=1)

    def weigh(p, j, s):
        for c in range(0, wide, SPAN):
            lanes = slice(c, c + SPAN)
            chunk = buf[p, j, :, lanes]
            ux = fixed(chunk[1:2, :], G0X) - me * (2**32 // slabs)
            uy = fixed(chunk[2:3, :], G0Y)
            uz = fixed(chunk[3:4, :], G0Z)

            def squared(first, rows, at_line, factor):
                wrapped = (broad(nodes[first : first + rows, :]) - at_line).astype(jnp.float32)
                return wrapped * wrapped * factor

            for i, ((l0, _), uses) in enumerate(SETS):
                for r in range(0, plan.zset, ROWS):
                    power = squared(plan.ztable + i * plan.zset + r, ROWS, uz, exponent(plan.gz[l0]))
                    for l, place, times in uses:
                        value = jnp.exp2(power if times == 1.0 else power * times).astype(jnp.bfloat16)
                        to = plan.zrow[l] + place * plan.zset + r
                        wz[s, to : to + ROWS, lanes] = value
            weighted = chunk[0:1, :] * jnp.exp2(squared(0, HALO, ux, broad(factors[0:HALO, :])))
            wx[s, :, lanes] = weighted
            for r in range(FAN):
                uy_r = uy - (col + r * beside) * (2**32 // cols)
                along_y = [[None] * len(ORDER[l]) for l in range(LEVELS)]
                for i, ((l0, _), uses) in enumerate(SETS):
                    power = squared(plan.ytable + i * plan.yset, plan.yset, uy_r, exponent(plan.gy[l0]))
                    for l, place, times in uses:
                        along_y[l][place] = jnp.exp2(power if times == 1.0 else power * times)
                last = jnp.exp2(squared(HALO, HALO, uy_r, broad(factors[HALO : 2 * HALO, :])))
                edge = (weighted * last).astype(jnp.bfloat16)
                for l in range(LEVELS):
                    start, main = FAN * plan.start[l] + r * plan.block[l], plan.main[l]
                    planes[s, start + main : start + main + HALO, lanes] = edge
                    tiles = [
                        wx[s, plan.xrow[l] + x : plan.xrow[l] + x + 1, lanes] * on_y
                        for x in range(plan.nx[l]) for on_y in along_y[l]
                    ]
                    for t, tile in enumerate(tiles):
                        to = start + t * plan.yset
                        planes[s, to : to + plan.yset, lanes] = tile.astype(jnp.bfloat16)

    def gather_in(s):
        for l in range(LEVELS):
            start, rows = plan.start[l], plan.block[l]
            terms = lax.dot_general(
                planes[s, FAN * start : FAN * (start + rows), :], wz[s, plan.zrow[l] : plan.zrow[l] + plan.gz[l], :],
                (((1,), (1,)), ((), ())), preferred_element_type=jnp.float32,
            )
            for r in range(FAN):
                acc[r, start : start + rows, 0 : plan.gz[l]] += terms[r * rows : (r + 1) * rows]

    def arrive(j):
        pair = half // 2

        @pl.when(j > 0)
        def _():
            z_copy(slot(0, 0), j, 0, 1).wait_recv()

        z_copy(slot(0, 0), j, 1, 1).wait_recv()

        @pl.when((j > 0) & (j < pair))
        def _():
            z_copy(slot(j, 0), j + pair, 0, reach).start()

        @pl.when(j < pair)
        def _():
            z_copy(slot(j, 1), j + pair, 1, -reach).start()

        x_copy(1, j).start()

    steps = half // 2
    far = steps // 2

    @pl.loop(0, steps * FAN)
    def _(t):
        side, place = lax.div(t, far), lax.rem(t, far)
        p, m = lax.rem(side, FAN), lax.div(side, FAN) * far + place

        @pl.when((p == 0) & (place == 0))
        def _():
            @pl.loop(0, 2 * far)
            def _(j):
                arrive(2 * m + j)

        @pl.when(p > 0)
        def _():
            x_copy(1, 2 * m).wait_recv()
            x_copy(1, 2 * m + 1).wait_recv()

        gather_in(1)
        weigh(p, 2 * m, 0)
        gather_in(0)
        weigh(p, 2 * m + 1, 1)

    gather_in(1)
    pass_beside(1, acc.at[1], from_x).start()
    pass_beside(0, dual.at[0], dual.at[1]).wait_recv()
    ez[0] = jnp.sum(acc[0] * dual[0] + acc[1] * dual[1], axis=0, keepdims=True)

    def e_copy(k):
        return pltpu.make_async_remote_copy(
            src_ref=ez.at[0], dst_ref=ez.at[k], send_sem=es_sem.at[k], recv_sem=er_sem.at[k],
            device_id=at(-order[k], 0, 0), device_id_type=MESH,
        )

    for k in range(slabs - 1, 0, -1):
        e_copy(k).start()
    pass_beside(1, acc.at[1], from_x).wait_recv()
    acc[0] = acc[0] + from_x[...]
    swap(1, acc.at[0], other).start()
    swap(1, acc.at[0], other).wait_recv()

    for l in range(LEVELS):
        start, rows = plan.start[l], plan.block[l]
        cube = acc[0, start : start + rows, :] + other[start : start + rows, :]
        along_z = jnp.dot(jnp.concatenate(split(cube), axis=1), pz[l], preferred_element_type=jnp.float32)
        t2[plan.xrow[l] * fine_y : (plan.xrow[l] + plan.nx[l]) * fine_y, :] = amp[l] * jnp.dot(
            down[l][...], jnp.concatenate(split(along_z), axis=0), preferred_element_type=jnp.float32
        )
    for a in range(plan.rows[0]):
        value = None
        for l in range(LEVELS):
            hat = plan.x_matrix(l)[a]
            for x in range(plan.nx[l]):
                if hat[x] > 0.0:
                    at_x = (plan.xrow[l] + x) * fine_y
                    term = float(hat[x]) * t2[at_x : at_x + fine_y, :]
                    value = term if value is None else value + term
        field_v[a] = value
    store = pltpu.make_async_copy(field_v, field, o_sem)
    store.start()

    for k in range(1, slabs):
        e_copy(k).wait_recv()
    ex[0] = jnp.sum(ez[...], axis=0)

    def f_copy(k):
        dc, dk = others[k - 1]
        return pltpu.make_async_remote_copy(
            src_ref=ex.at[0], dst_ref=ex.at[k], send_sem=fs_sem.at[k], recv_sem=fr_sem.at[k],
            device_id=at(0, -dc, dk), device_id_type=MESH,
        )

    for k in range(len(others), 0, -1):
        f_copy(k).start()

    for k in range(1, slabs):
        z_copy(slot(0, 0), k // 2, k % 2, 1).wait_send()
        e_copy(k).wait_send()

    @pl.loop(0, half)
    def _(j):
        x_copy(1, j).wait_send()

    pass_beside(0, dual.at[0], dual.at[1]).wait_send()
    pass_beside(1, acc.at[1], from_x).wait_send()
    swap(1, acc.at[0], other).wait_send()
    store.wait()
    for k in range(1, len(others) + 1):
        f_copy(k).wait_recv()
    energy[0, 0] = jnp.sum(jnp.sum(ex[...], axis=0)) * (1.0 / (FINE_X * FINE_Y * FINE_Z))
    for k in range(1, len(others) + 1):
        f_copy(k).wait_send()


def on_device(cell_x, cell_y, cell_z, offsets, charge, block_count, level_amplitude, density):
    slabs, cols = lax.axis_size("slab"), lax.axis_size("blk")
    plan = Plan(slabs, cols, *density.shape)
    slots = cell_x.shape[0]
    operands = [
        cell_x.reshape(1, slots), cell_y.reshape(1, slots), cell_z.reshape(1, slots), offsets,
        charge.reshape(1, slots), block_count.reshape(1, 1), level_amplitude, density, *plan.constants(),
    ]
    n_in = len(operands)
    spaces = [pltpu.VMEM] * 6 + [pltpu.SMEM] + [pltpu.VMEM] * (n_in - 7)
    smem = pl.BlockSpec(memory_space=pltpu.SMEM)
    anywhere = pl.BlockSpec(memory_space=pl.ANY)
    dma = pltpu.SemaphoreType.DMA
    field, energy = pl.pallas_call(
        functools.partial(kernel, plan, n_in),
        out_shape=(jax.ShapeDtypeStruct(density.shape, jnp.float32), jax.ShapeDtypeStruct((1, 1), jnp.float32)),
        in_specs=[anywhere] * n_in,
        out_specs=(anywhere, smem),
        scratch_shapes=[space(o.shape, o.dtype) for space, o in zip(spaces, operands)]
        + [
            pltpu.VMEM((FAN, slabs // 2, 4, 2 * BQ), jnp.float32),
            pltpu.VMEM((2, FAN * plan.total, 2 * BQ), jnp.bfloat16),
            pltpu.VMEM((2, sum(plan.gz), 2 * BQ), jnp.bfloat16),
            pltpu.VMEM((2, HALO, 2 * BQ), jnp.float32),
            pltpu.VMEM((FAN, plan.total, LANES), jnp.float32),
            pltpu.VMEM((plan.total, LANES), jnp.float32),
            pltpu.VMEM((plan.total, LANES), jnp.float32),
            pltpu.VMEM((FAN, plan.total, LANES), jnp.float32),
            pltpu.VMEM((plan.total, LANES), jnp.float32),
            pltpu.VMEM((LEVELS, 2 * LANES, LANES), jnp.bfloat16),
            pltpu.VMEM((sum(plan.nx) * density.shape[1], LANES), jnp.float32),
            pltpu.VMEM(density.shape, jnp.float32),
            pltpu.VMEM((slabs, 1, LANES), jnp.float32),
            pltpu.VMEM((2 * cols, 1, LANES), jnp.float32),
            dma((n_in,)),
            dma((slabs // 2, 2)), dma((slabs // 2, 2)),
            dma((FAN, slabs // 2)), dma((FAN, slabs // 2)),
            dma((2,)), dma((2,)),
            dma((2,)), dma((2,)),
            dma((slabs,)), dma((slabs,)),
            dma((2 * cols,)), dma((2 * cols,)),
            dma,
        ],
        compiler_params=pltpu.CompilerParams(collective_id=0, has_side_effects=True),
    )(*operands)
    return field, energy.reshape(1)


def solution(mesh):
    split_all = ("grp", "slab", "blk", "sub")
    in_specs = (
        P(split_all), P(split_all), P(split_all), P(None, split_all), P(split_all), P(split_all), P(),
        P(("grp", "slab"), "blk", "sub"),
    )
    out_specs = (P(("grp", "slab"), "blk", "sub"), P("grp"))
    return jax.shard_map(on_device, mesh=mesh, in_specs=in_specs, out_specs=out_specs, check_vma=False)
```

```python
import functools

import jax
import jax.numpy as jnp
import numpy as np
from jax import lax
from jax.experimental import pallas as pl
from jax.experimental.pallas import tpu as pltpu
from jax.sharding import PartitionSpec as P

G0X = 64
G0Y = 128
G0Z = 128
FINE_X = 256
FINE_Y = 256
FINE_Z = 256
BQ = 256
LEVELS = 4
LANES = 128
SPAN = 256
ROWS = 8
FAN = 2
HALO = 16
spread_width = 1.25
MESH = pl.DeviceIdType.MESH

ORDER = ((0, 2, 1, 3), (0, 1, 2), (0, 1), (0,))
SETS = (
    ((3, 0), ((3, 0, 1.0), (2, 0, 4.0), (1, 0, 9.0), (0, 0, 16.0))),
    ((2, 1), ((2, 1, 1.0), (0, 1, 4.0))),
    ((1, 1), ((1, 1, 1.0),)),
    ((1, 2), ((1, 2, 1.0),)),
    ((0, 1), ((0, 2, 1.0),)),
    ((0, 3), ((0, 3, 1.0),)),
)


def coarse_cells(base, level):
    return base * (4 - level) // 4


def exponent(cells):
    return -0.5 * np.log2(np.e) / spread_width**2 * (cells / 2.0**32) ** 2


class Plan:
    def __init__(self, slabs, cols, rows_x, rows_y, rows_z):
        self.slabs, self.cols = slabs, cols
        self.rows = (rows_x, rows_y, rows_z)
        self.gx = [coarse_cells(G0X, l) for l in range(LEVELS)]
        self.gy = [coarse_cells(G0Y, l) for l in range(LEVELS)]
        self.gz = [coarse_cells(G0Z, l) for l in range(LEVELS)]
        self.nx = [g // slabs + 1 for g in self.gx]
        self.ny = [g // cols for g in self.gy]
        self.main = [a * b for a, b in zip(self.nx, self.ny)]
        self.block = [m + HALO for m in self.main]
        self.start = [sum(self.block[:l]) for l in range(LEVELS)]
        self.total = sum(self.block)
        self.xrow = [sum(self.nx[:l]) for l in range(LEVELS)]
        self.yrow = [sum(self.ny[:l]) for l in range(LEVELS)]
        self.zrow = [sum(self.gz[:l]) for l in range(LEVELS)]
        self.yset, self.zset = self.ny[-1], self.gz[-1]
        self.ytable = 2 * HALO
        self.ztable = self.ytable + len(SETS) * self.yset

    def y_nodes(self, l):
        m = LEVELS - l
        return [m * k + s for s in ORDER[l] for k in range(self.yset)]

    def node_table(self):
        def frac(node, cells):
            return (2 * node * 2**32 + cells) // (2 * cells)

        flat = [frac(r, g) for g, n in zip(self.gx, self.nx) for r in range(n)]
        flat += [0] * (HALO - len(flat))
        flat += [frac(c, g) for g, n, c in zip(self.gy, self.nx, self.ny) for _ in range(n)]
        flat += [0] * (2 * HALO - len(flat))
        for cells, count in ((self.gy, self.yset), (self.gz, self.zset)):
            for (l, s), _ in SETS:
                flat += [frac((LEVELS - l) * k + s, cells[l]) for k in range(count)]
        flat = np.array(flat, np.int64) + 2**31
        flat = ((flat + 2**31) % 2**32 - 2**31).astype(np.int32)
        return np.repeat(flat[:, None], LANES, axis=1)

    def factor_table(self):
        k = [exponent(g) for g, n in zip(self.gx, self.nx) for _ in range(n)]
        h = [exponent(g) for g, n in zip(self.gy, self.nx) for _ in range(n)]
        pad = [0.0] * (HALO - len(k))
        return np.repeat(np.array(k + pad + h + pad, np.float32)[:, None], LANES, axis=1)

    def y_matrix(self, l):
        fine = self.rows[1]
        nx, ny, main = self.nx[l], self.ny[l], self.main[l]
        b = np.arange(fine)[:, None]
        y = np.array(self.y_nodes(l) + [ny])[None, :]
        hat = np.maximum(0.0, 1.0 - np.abs(y - b * self.gy[l] / FINE_Y))
        out = np.zeros((nx * fine, self.block[l]), np.float32)
        for x in range(nx):
            out[x * fine : (x + 1) * fine, x * ny : (x + 1) * ny] = hat[:, :ny]
            out[x * fine : (x + 1) * fine, main + self.xrow[l] + x] = hat[:, ny]
        return out

    def x_matrix(self, l):
        a = np.arange(self.rows[0])[:, None]
        x = np.arange(self.nx[l])[None, :]
        return np.maximum(0.0, 1.0 - np.abs(x - a * self.gx[l] / FINE_X))

    def constants(self):
        twice = lambda m: jnp.asarray(np.concatenate([m, m], axis=1), jnp.bfloat16)
        down = [twice(self.y_matrix(l)) for l in range(LEVELS)]
        up = [twice(self.y_matrix(l).T) for l in range(LEVELS)]
        return [jnp.asarray(self.node_table()), jnp.asarray(self.factor_table())] + down + up


def split(value):
    high = value.astype(jnp.bfloat16)
    low = (value - high.astype(jnp.float32)).astype(jnp.bfloat16)
    return high, low


def kernel(plan, n_in, *refs):
    hbm, refs = refs[:n_in], refs[n_in:]
    field, energy, refs = refs[0], refs[1], refs[2:]
    held_in, refs = refs[:n_in], refs[n_in:]
    (
        buf, planes, wz, wx, acc, from_x, other, dual, dual_other, pz, t2, field_v, ez, ex,
        in_sem, zs_sem, zr_sem, xs_sem, xr_sem, ps_sem, pr_sem, ns_sem, nr_sem, es_sem, er_sem, fs_sem, fr_sem, o_sem,
    ) = refs
    cx, cy, cz, off, charge, count, amp, dens_v, nodes, factors = held_in[:10]
    down, up = held_in[10 : 10 + LEVELS], held_in[10 + LEVELS :]
    slabs, cols = plan.slabs, plan.cols
    half = slabs // 2
    reach = half // 2
    me = lax.axis_index("slab")
    col = lax.axis_index("blk")
    core = lax.axis_index("sub")
    beside = 1 - 2 * lax.rem(col, 2)
    wide = 2 * BQ
    fine_y = plan.rows[1]

    def at(ds, dc, dk):
        return {
            "slab": lax.rem(me + slabs + ds, slabs),
            "blk": lax.rem(col + cols + dc, cols),
            "sub": lax.rem(core + dk, 2),
        }

    order = [0]
    for d in range(1, half):
        order += [d, -d]
    order.append(half)
    others = [(dc, dk) for dc in range(cols) for dk in range(2)][1:]

    barrier = pltpu.get_barrier_semaphore()
    near = order[1 : 2 * reach] + [reach, -reach]
    near = [d for i, d in enumerate(near) if d not in near[:i]]
    for ds in near:
        pl.semaphore_signal(barrier, inc=1, device_id=at(ds, 0, 0), device_id_type=MESH)
    for dc, dk in others:
        pl.semaphore_signal(barrier, inc=1, device_id=at(0, dc, dk), device_id_type=MESH)

    loads = [pltpu.make_async_copy(hbm[i], held_in[i], in_sem.at[i]) for i in range(n_in)]
    for load in loads:
        load.start()
    for i in range(6):
        loads[i].wait()

    lane = lax.broadcasted_iota(jnp.int32, (1, BQ), 1)
    live = jnp.where(lane < count[...], 1.0, 0.0).astype(jnp.float32)
    buf[0, 0, 0:1, 0:BQ] = charge[...] * live
    buf[0, 0, 1:2, 0:BQ] = cx[...].astype(jnp.float32) + off[0:1, :]
    buf[0, 0, 2:3, 0:BQ] = cy[...].astype(jnp.float32) + off[1:2, :]
    buf[0, 0, 3:4, 0:BQ] = cz[...].astype(jnp.float32) + off[2:3, :]

    pl.semaphore_wait(barrier, len(near) + len(others))

    def slot(j, part):
        return buf.at[0, j, :, pl.ds(part * BQ, BQ)]

    def z_copy(src, j, part, ds):
        return pltpu.make_async_remote_copy(
            src_ref=src, dst_ref=slot(j, part), send_sem=zs_sem.at[j, part], recv_sem=zr_sem.at[j, part],
            device_id=at(ds, 0, 0), device_id_type=MESH,
        )

    for k in range(2 * reach, 0, -1):
        z_copy(slot(0, 0), k // 2, k % 2, -order[k]).start()

    def x_copy(p, j):
        return pltpu.make_async_remote_copy(
            src_ref=buf.at[0, j], dst_ref=buf.at[p, j], send_sem=xs_sem.at[p, j], recv_sem=xr_sem.at[p, j],
            device_id=at(0, -(cols // FAN), 0), device_id_type=MESH,
        )

    acc[...] = jnp.zeros_like(acc)
    planes[1] = jnp.zeros(planes.shape[1:], planes.dtype)
    wz[1] = jnp.zeros(wz.shape[1:], wz.dtype)

    row = lax.broadcasted_iota(jnp.int32, (LANES, LANES), 0)
    fine = lax.broadcasted_iota(jnp.int32, (LANES, LANES), 1) + core * LANES
    for l in range(LEVELS):
        g = plan.gz[l]
        place = row // plan.zset
        part = (place % 2) * 2 + place // 2 if l == 0 else place
        node = (row % plan.zset) * (LEVELS - l) + part
        moved = node * FINE_Z - fine * g
        moved = jnp.where(moved < 0, moved + g * FINE_Z, moved)
        moved = jnp.where(moved * 2 >= g * FINE_Z, moved - g * FINE_Z, moved)
        hat = jnp.maximum(0.0, 1.0 - jnp.abs(moved.astype(jnp.float32)) * (1.0 / FINE_Z))
        hat = jnp.where(row < g, hat, 0.0).astype(jnp.bfloat16)
        pz[l, 0:LANES, :] = hat
        pz[l, LANES:, :] = hat

    for i in range(6, n_in):
        loads[i].wait()
    for l in range(LEVELS):
        hats = plan.x_matrix(l)
        for x in range(plan.nx[l]):
            value = None
            for a in range(plan.rows[0]):
                if hats[a, x] > 0.0:
                    term = float(hats[a, x]) * dens_v[a]
                    value = term if value is None else value + term
            at_x = (plan.xrow[l] + x) * fine_y
            t2[at_x : at_x + fine_y, :] = value * amp[l]
        start, rows = plan.start[l], plan.block[l]
        along = t2[plan.xrow[l] * fine_y : (plan.xrow[l] + plan.nx[l]) * fine_y, :]
        on_y = jnp.dot(up[l][...], jnp.concatenate(split(along), axis=0), preferred_element_type=jnp.float32)
        both = lax.dot_general(
            jnp.concatenate(split(on_y), axis=0), pz[l, 0:LANES, :], (((1,), (1,)), ((), ())),
            preferred_element_type=jnp.float32,
        )
        dual[0, start : start + rows, :] = both[:rows] + both[rows:]

    def swap(k, src, dst):
        return pltpu.make_async_remote_copy(
            src_ref=src, dst_ref=dst, send_sem=ps_sem.at[k], recv_sem=pr_sem.at[k],
            device_id=at(0, 0, 1), device_id_type=MESH,
        )

    def pass_beside(k, src, dst):
        return pltpu.make_async_remote_copy(
            src_ref=src, dst_ref=dst, send_sem=ns_sem.at[k], recv_sem=nr_sem.at[k],
            device_id=at(0, beside, 0), device_id_type=MESH,
        )

    swap(0, dual.at[0], dual_other).start()

    scale = 2.0**32
    top = 2.0**31 - 128.0

    def fixed(line, cells):
        moved = jnp.minimum((line - 0.5 * cells) * (scale / cells), top)
        return moved.astype(jnp.int32)

    def broad(table):
        return jnp.concatenate([table] * (SPAN // LANES), axis=1)

    def weigh(p, j, s):
        for c in range(0, wide, SPAN):
            lanes = slice(c, c + SPAN)
            chunk = buf[p, j, :, lanes]
            ux = fixed(chunk[1:2, :], G0X) - me * (2**32 // slabs)
            uy = fixed(chunk[2:3, :], G0Y)
            uz = fixed(chunk[3:4, :], G0Z)

            def squared(first, rows, at_line, factor):
                wrapped = (broad(nodes[first : first + rows, :]) - at_line).astype(jnp.float32)
                return wrapped * wrapped * factor

            for i, ((l0, _), uses) in enumerate(SETS):
                for r in range(0, plan.zset, ROWS):
                    power = squared(plan.ztable + i * plan.zset + r, ROWS, uz, exponent(plan.gz[l0]))
                    for l, place, times in uses:
                        value = jnp.exp2(power if times == 1.0 else power * times).astype(jnp.bfloat16)
                        to = plan.zrow[l] + place * plan.zset + r
                        wz[s, to : to + ROWS, lanes] = value
            weighted = chunk[0:1, :] * jnp.exp2(squared(0, HALO, ux, broad(factors[0:HALO, :])))
            wx[s, :, lanes] = weighted
            for r in range(FAN):
                uy_r = uy - (col + r * beside) * (2**32 // cols)
                along_y = [[None] * len(ORDER[l]) for l in range(LEVELS)]
                for i, ((l0, _), uses) in enumerate(SETS):
                    power = squared(plan.ytable + i * plan.yset, plan.yset, uy_r, exponent(plan.gy[l0]))
                    for l, place, times in uses:
                        along_y[l][place] = jnp.exp2(power if times == 1.0 else power * times)
                last = jnp.exp2(squared(HALO, HALO, uy_r, broad(factors[HALO : 2 * HALO, :])))
                edge = (weighted * last).astype(jnp.bfloat16)
                for l in range(LEVELS):
                    start, main = FAN * plan.start[l] + r * plan.block[l], plan.main[l]
                    planes[s, start + main : start + main + HALO, lanes] = edge
                    tiles = [
                        wx[s, plan.xrow[l] + x : plan.xrow[l] + x + 1, lanes] * on_y
                        for x in range(plan.nx[l]) for on_y in along_y[l]
                    ]
                    for t, tile in enumerate(tiles):
                        to = start + t * plan.yset
                        planes[s, to : to + plan.yset, lanes] = tile.astype(jnp.bfloat16)

    def gather_in(s):
        for l in range(LEVELS):
            start, rows = plan.start[l], plan.block[l]
            terms = lax.dot_general(
                planes[s, FAN * start : FAN * (start + rows), :], wz[s, plan.zrow[l] : plan.zrow[l] + plan.gz[l], :],
                (((1,), (1,)), ((), ())), preferred_element_type=jnp.float32,
            )
            for r in range(FAN):
                acc[r, start : start + rows, 0 : plan.gz[l]] += terms[r * rows : (r + 1) * rows]

    def arrive(j):
        pair = half // 2

        @pl.when(j > 0)
        def _():
            z_copy(slot(0, 0), j, 0, 1).wait_recv()

        z_copy(slot(0, 0), j, 1, 1).wait_recv()

        @pl.when((j > 0) & (j < pair))
        def _():
            z_copy(slot(j, 0), j + pair, 0, reach).start()

        @pl.when(j < pair)
        def _():
            z_copy(slot(j, 1), j + pair, 1, -reach).start()

        x_copy(1, j).start()

        @pl.when(j == 1)
        def _():
            swap(0, dual.at[0], dual_other).wait()
            dual[0] = dual[0] + dual_other[...]

        near_piece = plan.total // pair
        far_piece = near_piece * (pair - 2) // half

        def piece(first, rows):
            rows = pl.ds(pl.multiple_of(first, 8), rows)
            pass_beside(0, dual.at[0, rows, :], dual.at[1, rows, :]).start()

        @pl.when((j > 1) & (j < pair))
        def _():
            piece((j - 2) * near_piece, near_piece)

        @pl.when(j >= pair)
        def _():
            piece((pair - 2) * near_piece + (j - pair) * 2 * far_piece, 2 * far_piece)

    steps = half // 2
    far = steps // 2

    @pl.loop(0, steps * FAN)
    def _(t):
        side, place = lax.div(t, far), lax.rem(t, far)
        p, m = lax.rem(side, FAN), lax.div(side, FAN) * far + place

        @pl.when((p == 0) & (place == 0))
        def _():
            @pl.loop(0, 2 * far)
            def _(j):
                arrive(2 * m + j)

        @pl.when(p > 0)
        def _():
            x_copy(1, 2 * m).wait_recv()
            x_copy(1, 2 * m + 1).wait_recv()

        gather_in(1)
        weigh(p, 2 * m, 0)
        gather_in(0)
        weigh(p, 2 * m + 1, 1)

    gather_in(1)
    pass_beside(1, acc.at[1], from_x).start()
    pass_beside(0, dual.at[0], dual.at[1]).wait_recv()
    ez[0] = jnp.sum(acc[0] * dual[0] + acc[1] * dual[1], axis=0, keepdims=True)

    def e_copy(k):
        return pltpu.make_async_remote_copy(
            src_ref=ez.at[0], dst_ref=ez.at[k], send_sem=es_sem.at[k], recv_sem=er_sem.at[k],
            device_id=at(-order[k], 0, 0), device_id_type=MESH,
        )

    for k in range(slabs - 1, 0, -1):
        e_copy(k).start()
    pass_beside(1, acc.at[1], from_x).wait_recv()
    acc[0] = acc[0] + from_x[...]
    swap(1, acc.at[0], other).start()
    swap(1, acc.at[0], other).wait_recv()

    for l in range(LEVELS):
        start, rows = plan.start[l], plan.block[l]
        cube = acc[0, start : start + rows, :] + other[start : start + rows, :]
        along_z = jnp.dot(jnp.concatenate(split(cube), axis=1), pz[l], preferred_element_type=jnp.float32)
        t2[plan.xrow[l] * fine_y : (plan.xrow[l] + plan.nx[l]) * fine_y, :] = amp[l] * jnp.dot(
            down[l][...], jnp.concatenate(split(along_z), axis=0), preferred_element_type=jnp.float32
        )
    for a in range(plan.rows[0]):
        value = None
        for l in range(LEVELS):
            hat = plan.x_matrix(l)[a]
            for x in range(plan.nx[l]):
                if hat[x] > 0.0:
                    at_x = (plan.xrow[l] + x) * fine_y
                    term = float(hat[x]) * t2[at_x : at_x + fine_y, :]
                    value = term if value is None else value + term
        field_v[a] = value
    store = pltpu.make_async_copy(field_v, field, o_sem)
    store.start()

    for k in range(1, slabs):
        e_copy(k).wait_recv()
    ex[0] = jnp.sum(ez[...], axis=0)

    def f_copy(k):
        dc, dk = others[k - 1]
        return pltpu.make_async_remote_copy(
            src_ref=ex.at[0], dst_ref=ex.at[k], send_sem=fs_sem.at[k], recv_sem=fr_sem.at[k],
            device_id=at(0, -dc, dk), device_id_type=MESH,
        )

    for k in range(len(others), 0, -1):
        f_copy(k).start()

    for k in range(1, slabs):
        z_copy(slot(0, 0), k // 2, k % 2, 1).wait_send()
        e_copy(k).wait_send()

    @pl.loop(0, half)
    def _(j):
        x_copy(1, j).wait_send()

    pass_beside(0, dual.at[0], dual.at[1]).wait_send()
    pass_beside(1, acc.at[1], from_x).wait_send()
    swap(1, acc.at[0], other).wait_send()
    store.wait()
    for k in range(1, len(others) + 1):
        f_copy(k).wait_recv()
    energy[0, 0] = jnp.sum(jnp.sum(ex[...], axis=0)) * (1.0 / (FINE_X * FINE_Y * FINE_Z))
    for k in range(1, len(others) + 1):
        f_copy(k).wait_send()


def on_device(cell_x, cell_y, cell_z, offsets, charge, block_count, level_amplitude, density):
    slabs, cols = lax.axis_size("slab"), lax.axis_size("blk")
    plan = Plan(slabs, cols, *density.shape)
    slots = cell_x.shape[0]
    operands = [
        cell_x.reshape(1, slots), cell_y.reshape(1, slots), cell_z.reshape(1, slots), offsets,
        charge.reshape(1, slots), block_count.reshape(1, 1), level_amplitude, density, *plan.constants(),
    ]
    n_in = len(operands)
    spaces = [pltpu.VMEM] * 6 + [pltpu.SMEM] + [pltpu.VMEM] * (n_in - 7)
    smem = pl.BlockSpec(memory_space=pltpu.SMEM)
    anywhere = pl.BlockSpec(memory_space=pl.ANY)
    dma = pltpu.SemaphoreType.DMA
    field, energy = pl.pallas_call(
        functools.partial(kernel, plan, n_in),
        out_shape=(jax.ShapeDtypeStruct(density.shape, jnp.float32), jax.ShapeDtypeStruct((1, 1), jnp.float32)),
        in_specs=[anywhere] * n_in,
        out_specs=(anywhere, smem),
        scratch_shapes=[space(o.shape, o.dtype) for space, o in zip(spaces, operands)]
        + [
            pltpu.VMEM((FAN, slabs // 2, 4, 2 * BQ), jnp.float32),
            pltpu.VMEM((2, FAN * plan.total, 2 * BQ), jnp.bfloat16),
            pltpu.VMEM((2, sum(plan.gz), 2 * BQ), jnp.bfloat16),
            pltpu.VMEM((2, HALO, 2 * BQ), jnp.float32),
            pltpu.VMEM((FAN, plan.total, LANES), jnp.float32),
            pltpu.VMEM((plan.total, LANES), jnp.float32),
            pltpu.VMEM((plan.total, LANES), jnp.float32),
            pltpu.VMEM((FAN, plan.total, LANES), jnp.float32),
            pltpu.VMEM((plan.total, LANES), jnp.float32),
            pltpu.VMEM((LEVELS, 2 * LANES, LANES), jnp.bfloat16),
            pltpu.VMEM((sum(plan.nx) * density.shape[1], LANES), jnp.float32),
            pltpu.VMEM(density.shape, jnp.float32),
            pltpu.VMEM((slabs, 1, LANES), jnp.float32),
            pltpu.VMEM((2 * cols, 1, LANES), jnp.float32),
            dma((n_in,)),
            dma((slabs // 2, 2)), dma((slabs // 2, 2)),
            dma((FAN, slabs // 2)), dma((FAN, slabs // 2)),
            dma((2,)), dma((2,)),
            dma((2,)), dma((2,)),
            dma((slabs,)), dma((slabs,)),
            dma((2 * cols,)), dma((2 * cols,)),
            dma,
        ],
        compiler_params=pltpu.CompilerParams(collective_id=0, has_side_effects=True),
    )(*operands)
    return field, energy.reshape(1)


def solution(mesh):
    split_all = ("grp", "slab", "blk", "sub")
    in_specs = (
        P(split_all), P(split_all), P(split_all), P(None, split_all), P(split_all), P(split_all), P(),
        P(("grp", "slab"), "blk", "sub"),
    )
    out_specs = (P(("grp", "slab"), "blk", "sub"), P("grp"))
    return jax.shard_map(on_device, mesh=mesh, in_specs=in_specs, out_specs=out_specs, check_vma=False)
```

```python
import functools

import jax
import jax.numpy as jnp
import numpy as np
from jax import lax
from jax.experimental import pallas as pl
from jax.experimental.pallas import tpu as pltpu
from jax.sharding import PartitionSpec as P

G0X = 64
G0Y = 128
G0Z = 128
FINE_X = 256
FINE_Y = 256
FINE_Z = 256
BQ = 256
LEVELS = 4
LANES = 128
SPAN = 256
ROWS = 8
FAN = 2
HALO = 16
spread_width = 1.25
MESH = pl.DeviceIdType.MESH

ORDER = ((0, 2, 1, 3), (0, 1, 2), (0, 1), (0,))
SETS = (
    ((3, 0), ((3, 0, 1.0), (2, 0, 4.0), (1, 0, 9.0), (0, 0, 16.0))),
    ((2, 1), ((2, 1, 1.0), (0, 1, 4.0))),
    ((1, 1), ((1, 1, 1.0),)),
    ((1, 2), ((1, 2, 1.0),)),
    ((0, 1), ((0, 2, 1.0),)),
    ((0, 3), ((0, 3, 1.0),)),
)


def coarse_cells(base, level):
    return base * (4 - level) // 4


def exponent(cells):
    return -0.5 * np.log2(np.e) / spread_width**2 * (cells / 2.0**32) ** 2


class Plan:
    def __init__(self, slabs, cols, rows_x, rows_y, rows_z):
        self.slabs, self.cols = slabs, cols
        self.rows = (rows_x, rows_y, rows_z)
        self.gx = [coarse_cells(G0X, l) for l in range(LEVELS)]
        self.gy = [coarse_cells(G0Y, l) for l in range(LEVELS)]
        self.gz = [coarse_cells(G0Z, l) for l in range(LEVELS)]
        self.nx = [g // slabs + 1 for g in self.gx]
        self.ny = [g // cols for g in self.gy]
        self.main = [a * b for a, b in zip(self.nx, self.ny)]
        self.block = [m + HALO for m in self.main]
        self.start = [sum(self.block[:l]) for l in range(LEVELS)]
        self.total = sum(self.block)
        self.xrow = [sum(self.nx[:l]) for l in range(LEVELS)]
        self.yrow = [sum(self.ny[:l]) for l in range(LEVELS)]
        self.zrow = [sum(self.gz[:l]) for l in range(LEVELS)]
        self.yset, self.zset = self.ny[-1], self.gz[-1]
        self.ytable = 2 * HALO
        self.ztable = self.ytable + len(SETS) * self.yset

    def y_nodes(self, l):
        m = LEVELS - l
        return [m * k + s for s in ORDER[l] for k in range(self.yset)]

    def node_table(self):
        def frac(node, cells):
            return (2 * node * 2**32 + cells) // (2 * cells)

        flat = [frac(r, g) for g, n in zip(self.gx, self.nx) for r in range(n)]
        flat += [0] * (HALO - len(flat))
        flat += [frac(c, g) for g, n, c in zip(self.gy, self.nx, self.ny) for _ in range(n)]
        flat += [0] * (2 * HALO - len(flat))
        for cells, count in ((self.gy, self.yset), (self.gz, self.zset)):
            for (l, s), _ in SETS:
                flat += [frac((LEVELS - l) * k + s, cells[l]) for k in range(count)]
        flat = np.array(flat, np.int64) + 2**31
        flat = ((flat + 2**31) % 2**32 - 2**31).astype(np.int32)
        return np.repeat(flat[:, None], LANES, axis=1)

    def factor_table(self):
        k = [exponent(g) for g, n in zip(self.gx, self.nx) for _ in range(n)]
        h = [exponent(g) for g, n in zip(self.gy, self.nx) for _ in range(n)]
        pad = [0.0] * (HALO - len(k))
        return np.repeat(np.array(k + pad + h + pad, np.float32)[:, None], LANES, axis=1)

    def y_matrix(self, l):
        fine = self.rows[1]
        nx, ny, main = self.nx[l], self.ny[l], self.main[l]
        b = np.arange(fine)[:, None]
        y = np.array(self.y_nodes(l) + [ny])[None, :]
        hat = np.maximum(0.0, 1.0 - np.abs(y - b * self.gy[l] / FINE_Y))
        out = np.zeros((nx * fine, self.block[l]), np.float32)
        for x in range(nx):
            out[x * fine : (x + 1) * fine, x * ny : (x + 1) * ny] = hat[:, :ny]
            out[x * fine : (x + 1) * fine, main + self.xrow[l] + x] = hat[:, ny]
        return out

    def x_matrix(self, l):
        a = np.arange(self.rows[0])[:, None]
        x = np.arange(self.nx[l])[None, :]
        return np.maximum(0.0, 1.0 - np.abs(x - a * self.gx[l] / FINE_X))

    def constants(self):
        twice = lambda m: jnp.asarray(np.concatenate([m, m], axis=1), jnp.bfloat16)
        down = [twice(self.y_matrix(l)) for l in range(LEVELS)]
        up = [twice(self.y_matrix(l).T) for l in range(LEVELS)]
        return [jnp.asarray(self.node_table()), jnp.asarray(self.factor_table())] + down + up


def split(value):
    high = value.astype(jnp.bfloat16)
    low = (value - high.astype(jnp.float32)).astype(jnp.bfloat16)
    return high, low


def kernel(plan, n_in, *refs):
    hbm, refs = refs[:n_in], refs[n_in:]
    field, energy, refs = refs[0], refs[1], refs[2:]
    held_in, refs = refs[:n_in], refs[n_in:]
    (
        buf, planes, wz, wx, acc, from_x, other, dual, dual_other, pz, t2, field_v, ez, ex,
        in_sem, zs_sem, zr_sem, xs_sem, xr_sem, ps_sem, pr_sem, ns_sem, nr_sem, es_sem, er_sem, fs_sem, fr_sem, o_sem,
    ) = refs
    cx, cy, cz, off, charge, count, amp, dens_v, nodes, factors = held_in[:10]
    down, up = held_in[10 : 10 + LEVELS], held_in[10 + LEVELS :]
    slabs, cols = plan.slabs, plan.cols
    half = slabs // 2
    reach = half // 2
    me = lax.axis_index("slab")
    col = lax.axis_index("blk")
    core = lax.axis_index("sub")
    beside = 1 - 2 * lax.rem(col, 2)
    wide = 2 * BQ
    fine_y = plan.rows[1]

    def at(ds, dc, dk):
        return {
            "slab": lax.rem(me + slabs + ds, slabs),
            "blk": lax.rem(col + cols + dc, cols),
            "sub": lax.rem(core + dk, 2),
        }

    order = [0]
    for d in range(1, half):
        order += [d, -d]
    order.append(half)
    others = [(dc, dk) for dc in range(cols) for dk in range(2)][1:]

    barrier = pltpu.get_barrier_semaphore()
    near = order[1 : 2 * reach] + [reach, -reach]
    near = [d for i, d in enumerate(near) if d not in near[:i]]
    for ds in near:
        pl.semaphore_signal(barrier, inc=1, device_id=at(ds, 0, 0), device_id_type=MESH)
    for dc, dk in others:
        pl.semaphore_signal(barrier, inc=1, device_id=at(0, dc, dk), device_id_type=MESH)

    loads = [pltpu.make_async_copy(hbm[i], held_in[i], in_sem.at[i]) for i in range(n_in)]
    for load in loads:
        load.start()
    for i in range(6):
        loads[i].wait()

    lane = lax.broadcasted_iota(jnp.int32, (1, BQ), 1)
    live = jnp.where(lane < count[...], 1.0, 0.0).astype(jnp.float32)
    buf[0, 0, 0:1, 0:BQ] = charge[...] * live
    buf[0, 0, 1:2, 0:BQ] = cx[...].astype(jnp.float32) + off[0:1, :]
    buf[0, 0, 2:3, 0:BQ] = cy[...].astype(jnp.float32) + off[1:2, :]
    buf[0, 0, 3:4, 0:BQ] = cz[...].astype(jnp.float32) + off[2:3, :]

    pl.semaphore_wait(barrier, len(near) + len(others))

    def slot(j, part):
        return buf.at[0, j, :, pl.ds(part * BQ, BQ)]

    def z_copy(src, j, part, ds):
        return pltpu.make_async_remote_copy(
            src_ref=src, dst_ref=slot(j, part), send_sem=zs_sem.at[j, part], recv_sem=zr_sem.at[j, part],
            device_id=at(ds, 0, 0), device_id_type=MESH,
        )

    for k in range(2 * reach, 0, -1):
        z_copy(slot(0, 0), k // 2, k % 2, -order[k]).start()

    def x_copy(p, j):
        return pltpu.make_async_remote_copy(
            src_ref=buf.at[0, j], dst_ref=buf.at[p, j], send_sem=xs_sem.at[p, j], recv_sem=xr_sem.at[p, j],
            device_id=at(0, -(cols // FAN), 0), device_id_type=MESH,
        )

    acc[...] = jnp.zeros_like(acc)
    planes[1] = jnp.zeros(planes.shape[1:], planes.dtype)
    wz[1] = jnp.zeros(wz.shape[1:], wz.dtype)

    row = lax.broadcasted_iota(jnp.int32, (LANES, LANES), 0)
    fine = lax.broadcasted_iota(jnp.int32, (LANES, LANES), 1) + core * LANES
    for l in range(LEVELS):
        g = plan.gz[l]
        place = row // plan.zset
        part = (place % 2) * 2 + place // 2 if l == 0 else place
        node = (row % plan.zset) * (LEVELS - l) + part
        moved = node * FINE_Z - fine * g
        moved = jnp.where(moved < 0, moved + g * FINE_Z, moved)
        moved = jnp.where(moved * 2 >= g * FINE_Z, moved - g * FINE_Z, moved)
        hat = jnp.maximum(0.0, 1.0 - jnp.abs(moved.astype(jnp.float32)) * (1.0 / FINE_Z))
        hat = jnp.where(row < g, hat, 0.0).astype(jnp.bfloat16)
        pz[l, 0:LANES, :] = hat
        pz[l, LANES:, :] = hat

    for i in range(6, n_in):
        loads[i].wait()
    for l in range(LEVELS):
        hats = plan.x_matrix(l)
        for x in range(plan.nx[l]):
            value = None
            for a in range(plan.rows[0]):
                if hats[a, x] > 0.0:
                    term = float(hats[a, x]) * dens_v[a]
                    value = term if value is None else value + term
            at_x = (plan.xrow[l] + x) * fine_y
            t2[at_x : at_x + fine_y, :] = value * amp[l]
        start, rows = plan.start[l], plan.block[l]
        along = t2[plan.xrow[l] * fine_y : (plan.xrow[l] + plan.nx[l]) * fine_y, :]
        on_y = jnp.dot(up[l][...], jnp.concatenate(split(along), axis=0), preferred_element_type=jnp.float32)
        both = lax.dot_general(
            jnp.concatenate(split(on_y), axis=0), pz[l, 0:LANES, :], (((1,), (1,)), ((), ())),
            preferred_element_type=jnp.float32,
        )
        dual[0, start : start + rows, :] = both[:rows] + both[rows:]

    def swap(k, src, dst):
        return pltpu.make_async_remote_copy(
            src_ref=src, dst_ref=dst, send_sem=ps_sem.at[k], recv_sem=pr_sem.at[k],
            device_id=at(0, 0, 1), device_id_type=MESH,
        )

    def pass_beside(k, src, dst):
        return pltpu.make_async_remote_copy(
            src_ref=src, dst_ref=dst, send_sem=ns_sem.at[k], recv_sem=nr_sem.at[k],
            device_id=at(0, beside, 0), device_id_type=MESH,
        )

    swap(0, dual.at[0], dual_other).start()

    scale = 2.0**32
    top = 2.0**31 - 128.0

    def fixed(line, cells):
        moved = jnp.minimum((line - 0.5 * cells) * (scale / cells), top)
        return moved.astype(jnp.int32)

    def broad(table):
        return jnp.concatenate([table] * (SPAN // LANES), axis=1)

    def weigh(p, j, s):
        for c in range(0, wide, SPAN):
            lanes = slice(c, c + SPAN)
            chunk = buf[p, j, :, lanes]
            ux = fixed(chunk[1:2, :], G0X) - me * (2**32 // slabs)
            uy = fixed(chunk[2:3, :], G0Y)
            uz = fixed(chunk[3:4, :], G0Z)

            def squared(first, rows, at_line, factor):
                wrapped = (broad(nodes[first : first + rows, :]) - at_line).astype(jnp.float32)
                return wrapped * wrapped * factor

            for i, ((l0, _), uses) in enumerate(SETS):
                for r in range(0, plan.zset, ROWS):
                    power = squared(plan.ztable + i * plan.zset + r, ROWS, uz, exponent(plan.gz[l0]))
                    for l, place, times in uses:
                        value = jnp.exp2(power if times == 1.0 else power * times).astype(jnp.bfloat16)
                        to = plan.zrow[l] + place * plan.zset + r
                        wz[s, to : to + ROWS, lanes] = value
            weighted = chunk[0:1, :] * jnp.exp2(squared(0, HALO, ux, broad(factors[0:HALO, :])))
            wx[s, :, lanes] = weighted
            for r in range(FAN):
                uy_r = uy - (col + r * beside) * (2**32 // cols)
                along_y = [[None] * len(ORDER[l]) for l in range(LEVELS)]
                for i, ((l0, _), uses) in enumerate(SETS):
                    power = squared(plan.ytable + i * plan.yset, plan.yset, uy_r, exponent(plan.gy[l0]))
                    for l, place, times in uses:
                        along_y[l][place] = jnp.exp2(power if times == 1.0 else power * times)
                last = jnp.exp2(squared(HALO, HALO, uy_r, broad(factors[HALO : 2 * HALO, :])))
                edge = (weighted * last).astype(jnp.bfloat16)
                for l in range(LEVELS):
                    start, main = FAN * plan.start[l] + r * plan.block[l], plan.main[l]
                    planes[s, start + main : start + main + HALO, lanes] = edge
                    tiles = [
                        wx[s, plan.xrow[l] + x : plan.xrow[l] + x + 1, lanes] * on_y
                        for x in range(plan.nx[l]) for on_y in along_y[l]
                    ]
                    for t, tile in enumerate(tiles):
                        to = start + t * plan.yset
                        planes[s, to : to + plan.yset, lanes] = tile.astype(jnp.bfloat16)

    def gather_in(s):
        for l in range(LEVELS):
            start, rows = plan.start[l], plan.block[l]
            terms = lax.dot_general(
                planes[s, FAN * start : FAN * (start + rows), :], wz[s, plan.zrow[l] : plan.zrow[l] + plan.gz[l], :],
                (((1,), (1,)), ((), ())), preferred_element_type=jnp.float32,
            )
            for r in range(FAN):
                acc[r, start : start + rows, 0 : plan.gz[l]] += terms[r * rows : (r + 1) * rows]

    def arrive(j):
        pair = half // 2

        @pl.when(j > 0)
        def _():
            z_copy(slot(0, 0), j, 0, 1).wait_recv()

        z_copy(slot(0, 0), j, 1, 1).wait_recv()

        @pl.when((j > 0) & (j < pair))
        def _():
            z_copy(slot(j, 0), j + pair, 0, reach).start()

        @pl.when(j < pair)
        def _():
            z_copy(slot(j, 1), j + pair, 1, -reach).start()

        x_copy(1, j).start()

        @pl.when(j == 1)
        def _():
            swap(0, dual.at[0], dual_other).wait()
            dual[0] = dual[0] + dual_other[...]

        near_piece = plan.total // pair
        far_piece = near_piece * (pair - 2) // half

        def piece(first, rows):
            rows = pl.ds(pl.multiple_of(first, 8), rows)
            pass_beside(0, dual.at[0, rows, :], dual.at[1, rows, :]).start()

        @pl.when((j > 1) & (j < pair))
        def _():
            piece((j - 2) * near_piece, near_piece)

        @pl.when(j >= pair)
        def _():
            piece((pair - 2) * near_piece + (j - pair) * 2 * far_piece, 2 * far_piece)

    steps = half // 2
    far = steps // 2

    @pl.loop(0, steps * FAN)
    def _(t):
        side, place = lax.div(t, far), lax.rem(t, far)
        p, m = lax.rem(side, FAN), lax.div(side, FAN) * far + place

        @pl.when((t == 0) | (t == FAN * far - 1))
        def _():
            first = jnp.where(t == 0, 0, 2 * far)

            @pl.loop(0, 2 * far)
            def _(j):
                arrive(first + j)

        @pl.when(p > 0)
        def _():
            x_copy(1, 2 * m).wait_recv()
            x_copy(1, 2 * m + 1).wait_recv()

        gather_in(1)
        weigh(p, 2 * m, 0)
        gather_in(0)
        weigh(p, 2 * m + 1, 1)

    gather_in(1)
    pass_beside(1, acc.at[1], from_x).start()
    pass_beside(0, dual.at[0], dual.at[1]).wait_recv()
    ez[0] = jnp.sum(acc[0] * dual[0] + acc[1] * dual[1], axis=0, keepdims=True)

    def e_copy(k):
        return pltpu.make_async_remote_copy(
            src_ref=ez.at[0], dst_ref=ez.at[k], send_sem=es_sem.at[k], recv_sem=er_sem.at[k],
            device_id=at(-order[k], 0, 0), device_id_type=MESH,
        )

    for k in range(slabs - 1, 0, -1):
        e_copy(k).start()
    pass_beside(1, acc.at[1], from_x).wait_recv()
    acc[0] = acc[0] + from_x[...]
    swap(1, acc.at[0], other).start()
    for k in range(1, slabs):
        e_copy(k).wait_recv()
    ex[0] = jnp.sum(ez[...], axis=0)

    def f_copy(k):
        dc, dk = others[k - 1]
        return pltpu.make_async_remote_copy(
            src_ref=ex.at[0], dst_ref=ex.at[k], send_sem=fs_sem.at[k], recv_sem=fr_sem.at[k],
            device_id=at(0, -dc, dk), device_id_type=MESH,
        )

    for k in range(len(others), 0, -1):
        f_copy(k).start()

    swap(1, acc.at[0], other).wait_recv()

    for l in range(LEVELS):
        start, rows = plan.start[l], plan.block[l]
        cube = acc[0, start : start + rows, :] + other[start : start + rows, :]
        along_z = jnp.dot(jnp.concatenate(split(cube), axis=1), pz[l], preferred_element_type=jnp.float32)
        t2[plan.xrow[l] * fine_y : (plan.xrow[l] + plan.nx[l]) * fine_y, :] = amp[l] * jnp.dot(
            down[l][...], jnp.concatenate(split(along_z), axis=0), preferred_element_type=jnp.float32
        )
    for a in range(plan.rows[0]):
        value = None
        for l in range(LEVELS):
            hat = plan.x_matrix(l)[a]
            for x in range(plan.nx[l]):
                if hat[x] > 0.0:
                    at_x = (plan.xrow[l] + x) * fine_y
                    term = float(hat[x]) * t2[at_x : at_x + fine_y, :]
                    value = term if value is None else value + term
        field_v[a] = value
    store = pltpu.make_async_copy(field_v, field, o_sem)
    store.start()

    for k in range(1, slabs):
        z_copy(slot(0, 0), k // 2, k % 2, 1).wait_send()
        e_copy(k).wait_send()

    @pl.loop(0, half)
    def _(j):
        x_copy(1, j).wait_send()

    pass_beside(0, dual.at[0], dual.at[1]).wait_send()
    pass_beside(1, acc.at[1], from_x).wait_send()
    swap(1, acc.at[0], other).wait_send()
    store.wait()
    for k in range(1, len(others) + 1):
        f_copy(k).wait_recv()
    energy[0, 0] = jnp.sum(jnp.sum(ex[...], axis=0)) * (1.0 / (FINE_X * FINE_Y * FINE_Z))
    for k in range(1, len(others) + 1):
        f_copy(k).wait_send()


def on_device(cell_x, cell_y, cell_z, offsets, charge, block_count, level_amplitude, density):
    slabs, cols = lax.axis_size("slab"), lax.axis_size("blk")
    plan = Plan(slabs, cols, *density.shape)
    slots = cell_x.shape[0]
    operands = [
        cell_x.reshape(1, slots), cell_y.reshape(1, slots), cell_z.reshape(1, slots), offsets,
        charge.reshape(1, slots), block_count.reshape(1, 1), level_amplitude, density, *plan.constants(),
    ]
    n_in = len(operands)
    spaces = [pltpu.VMEM] * 6 + [pltpu.SMEM] + [pltpu.VMEM] * (n_in - 7)
    smem = pl.BlockSpec(memory_space=pltpu.SMEM)
    anywhere = pl.BlockSpec(memory_space=pl.ANY)
    dma = pltpu.SemaphoreType.DMA
    field, energy = pl.pallas_call(
        functools.partial(kernel, plan, n_in),
        out_shape=(jax.ShapeDtypeStruct(density.shape, jnp.float32), jax.ShapeDtypeStruct((1, 1), jnp.float32)),
        in_specs=[anywhere] * n_in,
        out_specs=(anywhere, smem),
        scratch_shapes=[space(o.shape, o.dtype) for space, o in zip(spaces, operands)]
        + [
            pltpu.VMEM((FAN, slabs // 2, 4, 2 * BQ), jnp.float32),
            pltpu.VMEM((2, FAN * plan.total, 2 * BQ), jnp.bfloat16),
            pltpu.VMEM((2, sum(plan.gz), 2 * BQ), jnp.bfloat16),
            pltpu.VMEM((2, HALO, 2 * BQ), jnp.float32),
            pltpu.VMEM((FAN, plan.total, LANES), jnp.float32),
            pltpu.VMEM((plan.total, LANES), jnp.float32),
            pltpu.VMEM((plan.total, LANES), jnp.float32),
            pltpu.VMEM((FAN, plan.total, LANES), jnp.float32),
            pltpu.VMEM((plan.total, LANES), jnp.float32),
            pltpu.VMEM((LEVELS, 2 * LANES, LANES), jnp.bfloat16),
            pltpu.VMEM((sum(plan.nx) * density.shape[1], LANES), jnp.float32),
            pltpu.VMEM(density.shape, jnp.float32),
            pltpu.VMEM((slabs, 1, LANES), jnp.float32),
            pltpu.VMEM((2 * cols, 1, LANES), jnp.float32),
            dma((n_in,)),
            dma((slabs // 2, 2)), dma((slabs // 2, 2)),
            dma((FAN, slabs // 2)), dma((FAN, slabs // 2)),
            dma((2,)), dma((2,)),
            dma((2,)), dma((2,)),
            dma((slabs,)), dma((slabs,)),
            dma((2 * cols,)), dma((2 * cols,)),
            dma,
        ],
        compiler_params=pltpu.CompilerParams(collective_id=0, has_side_effects=True),
    )(*operands)
    return field, energy.reshape(1)


def solution(mesh):
    split_all = ("grp", "slab", "blk", "sub")
    in_specs = (
        P(split_all), P(split_all), P(split_all), P(None, split_all), P(split_all), P(split_all), P(),
        P(("grp", "slab"), "blk", "sub"),
    )
    out_specs = (P(("grp", "slab"), "blk", "sub"), P("grp"))
    return jax.shard_map(on_device, mesh=mesh, in_specs=in_specs, out_specs=out_specs, check_vma=False)
```

```python
import functools

import jax
import jax.numpy as jnp
import numpy as np
from jax import lax
from jax.experimental import pallas as pl
from jax.experimental.pallas import tpu as pltpu
from jax.sharding import PartitionSpec as P

G0X = 64
G0Y = 128
G0Z = 128
FINE_X = 256
FINE_Y = 256
FINE_Z = 256
BQ = 256
LEVELS = 4
LANES = 128
SPAN = 256
ROWS = 8
FAN = 2
HALO = 16
spread_width = 1.25
MESH = pl.DeviceIdType.MESH

ORDER = ((0, 2, 1, 3), (0, 1, 2), (0, 1), (0,))
SETS = (
    ((3, 0), ((3, 0, 1.0), (2, 0, 4.0), (1, 0, 9.0), (0, 0, 16.0))),
    ((2, 1), ((2, 1, 1.0), (0, 1, 4.0))),
    ((1, 1), ((1, 1, 1.0),)),
    ((1, 2), ((1, 2, 1.0),)),
    ((0, 1), ((0, 2, 1.0),)),
    ((0, 3), ((0, 3, 1.0),)),
)


def coarse_cells(base, level):
    return base * (4 - level) // 4


def exponent(cells):
    return -0.5 * np.log2(np.e) / spread_width**2 * (cells / 2.0**32) ** 2


class Plan:
    def __init__(self, slabs, cols, rows_x, rows_y, rows_z):
        self.slabs, self.cols = slabs, cols
        self.rows = (rows_x, rows_y, rows_z)
        self.gx = [coarse_cells(G0X, l) for l in range(LEVELS)]
        self.gy = [coarse_cells(G0Y, l) for l in range(LEVELS)]
        self.gz = [coarse_cells(G0Z, l) for l in range(LEVELS)]
        self.nx = [g // slabs + 1 for g in self.gx]
        self.ny = [g // cols for g in self.gy]
        self.main = [a * b for a, b in zip(self.nx, self.ny)]
        self.block = [m + HALO for m in self.main]
        self.start = [sum(self.block[:l]) for l in range(LEVELS)]
        self.total = sum(self.block)
        self.xrow = [sum(self.nx[:l]) for l in range(LEVELS)]
        self.yrow = [sum(self.ny[:l]) for l in range(LEVELS)]
        self.zrow = [sum(self.gz[:l]) for l in range(LEVELS)]
        self.yset, self.zset = self.ny[-1], self.gz[-1]
        self.ytable = 2 * HALO
        self.ztable = self.ytable + len(SETS) * self.yset

    def y_nodes(self, l):
        m = LEVELS - l
        return [m * k + s for s in ORDER[l] for k in range(self.yset)]

    def node_table(self):
        def frac(node, cells):
            return (2 * node * 2**32 + cells) // (2 * cells)

        flat = [frac(r, g) for g, n in zip(self.gx, self.nx) for r in range(n)]
        flat += [0] * (HALO - len(flat))
        flat += [frac(c, g) for g, n, c in zip(self.gy, self.nx, self.ny) for _ in range(n)]
        flat += [0] * (2 * HALO - len(flat))
        for cells, count in ((self.gy, self.yset), (self.gz, self.zset)):
            for (l, s), _ in SETS:
                flat += [frac((LEVELS - l) * k + s, cells[l]) for k in range(count)]
        flat = np.array(flat, np.int64) + 2**31
        flat = ((flat + 2**31) % 2**32 - 2**31).astype(np.int32)
        return np.repeat(flat[:, None], LANES, axis=1)

    def factor_table(self):
        k = [exponent(g) for g, n in zip(self.gx, self.nx) for _ in range(n)]
        h = [exponent(g) for g, n in zip(self.gy, self.nx) for _ in range(n)]
        pad = [0.0] * (HALO - len(k))
        return np.repeat(np.array(k + pad + h + pad, np.float32)[:, None], LANES, axis=1)

    def y_matrix(self, l):
        fine = self.rows[1]
        nx, ny, main = self.nx[l], self.ny[l], self.main[l]
        b = np.arange(fine)[:, None]
        y = np.array(self.y_nodes(l) + [ny])[None, :]
        hat = np.maximum(0.0, 1.0 - np.abs(y - b * self.gy[l] / FINE_Y))
        out = np.zeros((nx * fine, self.block[l]), np.float32)
        for x in range(nx):
            out[x * fine : (x + 1) * fine, x * ny : (x + 1) * ny] = hat[:, :ny]
            out[x * fine : (x + 1) * fine, main + self.xrow[l] + x] = hat[:, ny]
        return out

    def x_matrix(self, l):
        a = np.arange(self.rows[0])[:, None]
        x = np.arange(self.nx[l])[None, :]
        return np.maximum(0.0, 1.0 - np.abs(x - a * self.gx[l] / FINE_X))

    def constants(self):
        twice = lambda m: jnp.asarray(np.concatenate([m, m], axis=1), jnp.bfloat16)
        down = [twice(self.y_matrix(l)) for l in range(LEVELS)]
        up = [twice(self.y_matrix(l).T) for l in range(LEVELS)]
        return [jnp.asarray(self.node_table()), jnp.asarray(self.factor_table())] + down + up


def split(value):
    high = value.astype(jnp.bfloat16)
    low = (value - high.astype(jnp.float32)).astype(jnp.bfloat16)
    return high, low


def kernel(plan, n_in, *refs):
    hbm, refs = refs[:n_in], refs[n_in:]
    field, energy, refs = refs[0], refs[1], refs[2:]
    held_in, refs = refs[:n_in], refs[n_in:]
    (
        buf, planes, wz, wx, acc, from_x, other, dual, dual_other, pz, t2, field_v, ez, ex,
        in_sem, zs_sem, zr_sem, ws_sem, wr_sem, xs_sem, xr_sem, ps_sem, pr_sem, ns_sem, nr_sem, es_sem, er_sem, fs_sem, fr_sem, o_sem,
    ) = refs
    cx, cy, cz, off, charge, count, amp, dens_v, nodes, factors = held_in[:10]
    down, up = held_in[10 : 10 + LEVELS], held_in[10 + LEVELS :]
    slabs, cols = plan.slabs, plan.cols
    half = slabs // 2
    reach = half // 2
    me = lax.axis_index("slab")
    col = lax.axis_index("blk")
    core = lax.axis_index("sub")
    beside = 1 - 2 * lax.rem(col, 2)
    wide = 2 * BQ
    fine_y = plan.rows[1]

    def at(ds, dc, dk):
        return {
            "slab": lax.rem(me + slabs + ds, slabs),
            "blk": lax.rem(col + cols + dc, cols),
            "sub": lax.rem(core + dk, 2),
        }

    order = [0]
    for d in range(1, half):
        order += [d, -d]
    order.append(half)
    others = [(dc, dk) for dc in range(cols) for dk in range(2)][1:]

    barrier = pltpu.get_barrier_semaphore()
    near = order[1 : 2 * reach] + [reach, -reach]
    near = [d for i, d in enumerate(near) if d not in near[:i]]
    for ds in near:
        pl.semaphore_signal(barrier, inc=1, device_id=at(ds, 0, 0), device_id_type=MESH)
    for dc, dk in others:
        pl.semaphore_signal(barrier, inc=1, device_id=at(0, dc, dk), device_id_type=MESH)
    for ds in (reach, -reach):
        pl.semaphore_signal(barrier, inc=1, device_id=at(ds, cols // FAN, 0), device_id_type=MESH)

    loads = [pltpu.make_async_copy(hbm[i], held_in[i], in_sem.at[i]) for i in range(n_in)]
    for load in loads:
        load.start()
    for i in range(6):
        loads[i].wait()

    lane = lax.broadcasted_iota(jnp.int32, (1, BQ), 1)
    live = jnp.where(lane < count[...], 1.0, 0.0).astype(jnp.float32)
    buf[0, 0, 0:1, 0:BQ] = charge[...] * live
    buf[0, 0, 1:2, 0:BQ] = cx[...].astype(jnp.float32) + off[0:1, :]
    buf[0, 0, 2:3, 0:BQ] = cy[...].astype(jnp.float32) + off[1:2, :]
    buf[0, 0, 3:4, 0:BQ] = cz[...].astype(jnp.float32) + off[2:3, :]

    pl.semaphore_wait(barrier, len(near) + len(others) + 2)

    def slot(j, part):
        return buf.at[0, j, :, pl.ds(part * BQ, BQ)]

    def z_copy(src, j, part, ds):
        return pltpu.make_async_remote_copy(
            src_ref=src, dst_ref=slot(j, part), send_sem=zs_sem.at[j, part], recv_sem=zr_sem.at[j, part],
            device_id=at(ds, 0, 0), device_id_type=MESH,
        )

    def far_copy(src, j, part, ds):
        return pltpu.make_async_remote_copy(
            src_ref=src, dst_ref=buf.at[1, j, :, pl.ds(part * BQ, BQ)],
            send_sem=ws_sem.at[j, part], recv_sem=wr_sem.at[j, part],
            device_id=at(ds, -(cols // FAN), 0), device_id_type=MESH,
        )

    far_copy(slot(0, 0), reach, 0, reach).start()
    for k in range(2 * reach, 0, -1):
        z_copy(slot(0, 0), k // 2, k % 2, -order[k]).start()

    def x_copy(p, j):
        return pltpu.make_async_remote_copy(
            src_ref=buf.at[0, j], dst_ref=buf.at[p, j], send_sem=xs_sem.at[p, j], recv_sem=xr_sem.at[p, j],
            device_id=at(0, -(cols // FAN), 0), device_id_type=MESH,
        )

    acc[...] = jnp.zeros_like(acc)
    planes[1] = jnp.zeros(planes.shape[1:], planes.dtype)
    wz[1] = jnp.zeros(wz.shape[1:], wz.dtype)

    row = lax.broadcasted_iota(jnp.int32, (LANES, LANES), 0)
    fine = lax.broadcasted_iota(jnp.int32, (LANES, LANES), 1) + core * LANES
    for l in range(LEVELS):
        g = plan.gz[l]
        place = row // plan.zset
        part = (place % 2) * 2 + place // 2 if l == 0 else place
        node = (row % plan.zset) * (LEVELS - l) + part
        moved = node * FINE_Z - fine * g
        moved = jnp.where(moved < 0, moved + g * FINE_Z, moved)
        moved = jnp.where(moved * 2 >= g * FINE_Z, moved - g * FINE_Z, moved)
        hat = jnp.maximum(0.0, 1.0 - jnp.abs(moved.astype(jnp.float32)) * (1.0 / FINE_Z))
        hat = jnp.where(row < g, hat, 0.0).astype(jnp.bfloat16)
        pz[l, 0:LANES, :] = hat
        pz[l, LANES:, :] = hat

    for i in range(6, n_in):
        loads[i].wait()
    for l in range(LEVELS):
        hats = plan.x_matrix(l)
        for x in range(plan.nx[l]):
            value = None
            for a in range(plan.rows[0]):
                if hats[a, x] > 0.0:
                    term = float(hats[a, x]) * dens_v[a]
                    value = term if value is None else value + term
            at_x = (plan.xrow[l] + x) * fine_y
            t2[at_x : at_x + fine_y, :] = value * amp[l]
        start, rows = plan.start[l], plan.block[l]
        along = t2[plan.xrow[l] * fine_y : (plan.xrow[l] + plan.nx[l]) * fine_y, :]
        on_y = jnp.dot(up[l][...], jnp.concatenate(split(along), axis=0), preferred_element_type=jnp.float32)
        both = lax.dot_general(
            jnp.concatenate(split(on_y), axis=0), pz[l, 0:LANES, :], (((1,), (1,)), ((), ())),
            preferred_element_type=jnp.float32,
        )
        dual[0, start : start + rows, :] = both[:rows] + both[rows:]

    def swap(k, src, dst):
        return pltpu.make_async_remote_copy(
            src_ref=src, dst_ref=dst, send_sem=ps_sem.at[k], recv_sem=pr_sem.at[k],
            device_id=at(0, 0, 1), device_id_type=MESH,
        )

    def pass_beside(k, src, dst):
        return pltpu.make_async_remote_copy(
            src_ref=src, dst_ref=dst, send_sem=ns_sem.at[k], recv_sem=nr_sem.at[k],
            device_id=at(0, beside, 0), device_id_type=MESH,
        )

    swap(0, dual.at[0], dual_other).start()

    scale = 2.0**32
    top = 2.0**31 - 128.0

    def fixed(line, cells):
        moved = jnp.minimum((line - 0.5 * cells) * (scale / cells), top)
        return moved.astype(jnp.int32)

    def broad(table):
        return jnp.concatenate([table] * (SPAN // LANES), axis=1)

    def weigh(p, j, s):
        for c in range(0, wide, SPAN):
            lanes = slice(c, c + SPAN)
            chunk = buf[p, j, :, lanes]
            ux = fixed(chunk[1:2, :], G0X) - me * (2**32 // slabs)
            uy = fixed(chunk[2:3, :], G0Y)
            uz = fixed(chunk[3:4, :], G0Z)

            def squared(first, rows, at_line, factor):
                wrapped = (broad(nodes[first : first + rows, :]) - at_line).astype(jnp.float32)
                return wrapped * wrapped * factor

            for i, ((l0, _), uses) in enumerate(SETS):
                for r in range(0, plan.zset, ROWS):
                    power = squared(plan.ztable + i * plan.zset + r, ROWS, uz, exponent(plan.gz[l0]))
                    for l, place, times in uses:
                        value = jnp.exp2(power if times == 1.0 else power * times).astype(jnp.bfloat16)
                        to = plan.zrow[l] + place * plan.zset + r
                        wz[s, to : to + ROWS, lanes] = value
            weighted = chunk[0:1, :] * jnp.exp2(squared(0, HALO, ux, broad(factors[0:HALO, :])))
            wx[s, :, lanes] = weighted
            for r in range(FAN):
                uy_r = uy - (col + r * beside) * (2**32 // cols)
                along_y = [[None] * len(ORDER[l]) for l in range(LEVELS)]
                for i, ((l0, _), uses) in enumerate(SETS):
                    power = squared(plan.ytable + i * plan.yset, plan.yset, uy_r, exponent(plan.gy[l0]))
                    for l, place, times in uses:
                        along_y[l][place] = jnp.exp2(power if times == 1.0 else power * times)
                last = jnp.exp2(squared(HALO, HALO, uy_r, broad(factors[HALO : 2 * HALO, :])))
                edge = (weighted * last).astype(jnp.bfloat16)
                for l in range(LEVELS):
                    start, main = FAN * plan.start[l] + r * plan.block[l], plan.main[l]
                    planes[s, start + main : start + main + HALO, lanes] = edge
                    tiles = [
                        wx[s, plan.xrow[l] + x : plan.xrow[l] + x + 1, lanes] * on_y
                        for x in range(plan.nx[l]) for on_y in along_y[l]
                    ]
                    for t, tile in enumerate(tiles):
                        to = start + t * plan.yset
                        planes[s, to : to + plan.yset, lanes] = tile.astype(jnp.bfloat16)

    def gather_in(s):
        for l in range(LEVELS):
            start, rows = plan.start[l], plan.block[l]
            terms = lax.dot_general(
                planes[s, FAN * start : FAN * (start + rows), :], wz[s, plan.zrow[l] : plan.zrow[l] + plan.gz[l], :],
                (((1,), (1,)), ((), ())), preferred_element_type=jnp.float32,
            )
            for r in range(FAN):
                acc[r, start : start + rows, 0 : plan.gz[l]] += terms[r * rows : (r + 1) * rows]

    def arrive(j):
        pair = half // 2

        @pl.when(j > 0)
        def _():
            z_copy(slot(0, 0), j, 0, 1).wait_recv()

        z_copy(slot(0, 0), j, 1, 1).wait_recv()

        @pl.when((j > 0) & (j < pair))
        def _():
            z_copy(slot(j, 0), j + pair, 0, reach).start()
            far_copy(slot(j, 0), j + pair, 0, reach).start()

        @pl.when(j < pair)
        def _():
            z_copy(slot(j, 1), j + pair, 1, -reach).start()
            far_copy(slot(j, 1), j + pair, 1, -reach).start()
            x_copy(1, j).start()

        @pl.when(j == 1)
        def _():
            swap(0, dual.at[0], dual_other).wait()
            dual[0] = dual[0] + dual_other[...]

        def piece(first, rows):
            rows = pl.ds(first, rows)
            pass_beside(0, dual.at[0, rows, :], dual.at[1, rows, :]).start()

        quarter = plan.total // 4

        @pl.when(j == pair - 2)
        def _():
            piece(0, quarter)

        @pl.when(j == pair - 1)
        def _():
            piece(quarter, 3 * quarter)

    steps = half // 2
    far = steps // 2

    @pl.loop(0, steps * FAN)
    def _(t):
        side, place = lax.div(t, far), lax.rem(t, far)
        p, m = lax.rem(side, FAN), lax.div(side, FAN) * far + place

        @pl.when((t == 0) | (t == FAN * far))
        def _():
            first = jnp.where(t == 0, 0, 2 * far)

            @pl.loop(0, 2 * far)
            def _(j):
                arrive(first + j)

        @pl.when((p > 0) & (m < far))
        def _():
            x_copy(1, 2 * m).wait_recv()
            x_copy(1, 2 * m + 1).wait_recv()

        @pl.when((p > 0) & (m >= far))
        def _():
            for i in range(2):
                for part in range(2):
                    far_copy(slot(0, 0), 2 * m + i, part, reach).wait_recv()

        gather_in(1)
        weigh(p, 2 * m, 0)
        gather_in(0)
        weigh(p, 2 * m + 1, 1)

    gather_in(1)
    pass_beside(1, acc.at[1], from_x).start()
    pass_beside(0, dual.at[0], dual.at[1]).wait_recv()
    ez[0] = jnp.sum(acc[0] * dual[0] + acc[1] * dual[1], axis=0, keepdims=True)

    def e_copy(k):
        return pltpu.make_async_remote_copy(
            src_ref=ez.at[0], dst_ref=ez.at[k], send_sem=es_sem.at[k], recv_sem=er_sem.at[k],
            device_id=at(-order[k], 0, 0), device_id_type=MESH,
        )

    for k in range(slabs - 1, 0, -1):
        e_copy(k).start()
    pass_beside(1, acc.at[1], from_x).wait_recv()
    acc[0] = acc[0] + from_x[...]
    swap(1, acc.at[0], other).start()
    for k in range(1, slabs):
        e_copy(k).wait_recv()
    ex[0] = jnp.sum(ez[...], axis=0)

    def f_copy(k):
        dc, dk = others[k - 1]
        return pltpu.make_async_remote_copy(
            src_ref=ex.at[0], dst_ref=ex.at[k], send_sem=fs_sem.at[k], recv_sem=fr_sem.at[k],
            device_id=at(0, -dc, dk), device_id_type=MESH,
        )

    for k in range(len(others), 0, -1):
        f_copy(k).start()

    swap(1, acc.at[0], other).wait_recv()

    for l in range(LEVELS):
        start, rows = plan.start[l], plan.block[l]
        cube = acc[0, start : start + rows, :] + other[start : start + rows, :]
        along_z = jnp.dot(jnp.concatenate(split(cube), axis=1), pz[l], preferred_element_type=jnp.float32)
        t2[plan.xrow[l] * fine_y : (plan.xrow[l] + plan.nx[l]) * fine_y, :] = amp[l] * jnp.dot(
            down[l][...], jnp.concatenate(split(along_z), axis=0), preferred_element_type=jnp.float32
        )
    for a in range(plan.rows[0]):
        value = None
        for l in range(LEVELS):
            hat = plan.x_matrix(l)[a]
            for x in range(plan.nx[l]):
                if hat[x] > 0.0:
                    at_x = (plan.xrow[l] + x) * fine_y
                    term = float(hat[x]) * t2[at_x : at_x + fine_y, :]
                    value = term if value is None else value + term
        field_v[a] = value
    store = pltpu.make_async_copy(field_v, field, o_sem)
    store.start()

    for k in range(1, slabs):
        z_copy(slot(0, 0), k // 2, k % 2, 1).wait_send()
        e_copy(k).wait_send()

    @pl.loop(0, reach)
    def _(j):
        x_copy(1, j).wait_send()
        for part in range(2):
            far_copy(slot(0, 0), j + reach, part, reach).wait_send()

    pass_beside(0, dual.at[0], dual.at[1]).wait_send()
    pass_beside(1, acc.at[1], from_x).wait_send()
    swap(1, acc.at[0], other).wait_send()
    store.wait()
    for k in range(1, len(others) + 1):
        f_copy(k).wait_recv()
    energy[0, 0] = jnp.sum(jnp.sum(ex[...], axis=0)) * (1.0 / (FINE_X * FINE_Y * FINE_Z))
    for k in range(1, len(others) + 1):
        f_copy(k).wait_send()


def on_device(cell_x, cell_y, cell_z, offsets, charge, block_count, level_amplitude, density):
    slabs, cols = lax.axis_size("slab"), lax.axis_size("blk")
    plan = Plan(slabs, cols, *density.shape)
    slots = cell_x.shape[0]
    operands = [
        cell_x.reshape(1, slots), cell_y.reshape(1, slots), cell_z.reshape(1, slots), offsets,
        charge.reshape(1, slots), block_count.reshape(1, 1), level_amplitude, density, *plan.constants(),
    ]
    n_in = len(operands)
    spaces = [pltpu.VMEM] * 6 + [pltpu.SMEM] + [pltpu.VMEM] * (n_in - 7)
    smem = pl.BlockSpec(memory_space=pltpu.SMEM)
    anywhere = pl.BlockSpec(memory_space=pl.ANY)
    dma = pltpu.SemaphoreType.DMA
    field, energy = pl.pallas_call(
        functools.partial(kernel, plan, n_in),
        out_shape=(jax.ShapeDtypeStruct(density.shape, jnp.float32), jax.ShapeDtypeStruct((1, 1), jnp.float32)),
        in_specs=[anywhere] * n_in,
        out_specs=(anywhere, smem),
        scratch_shapes=[space(o.shape, o.dtype) for space, o in zip(spaces, operands)]
        + [
            pltpu.VMEM((FAN, slabs // 2, 4, 2 * BQ), jnp.float32),
            pltpu.VMEM((2, FAN * plan.total, 2 * BQ), jnp.bfloat16),
            pltpu.VMEM((2, sum(plan.gz), 2 * BQ), jnp.bfloat16),
            pltpu.VMEM((2, HALO, 2 * BQ), jnp.float32),
            pltpu.VMEM((FAN, plan.total, LANES), jnp.float32),
            pltpu.VMEM((plan.total, LANES), jnp.float32),
            pltpu.VMEM((plan.total, LANES), jnp.float32),
            pltpu.VMEM((FAN, plan.total, LANES), jnp.float32),
            pltpu.VMEM((plan.total, LANES), jnp.float32),
            pltpu.VMEM((LEVELS, 2 * LANES, LANES), jnp.bfloat16),
            pltpu.VMEM((sum(plan.nx) * density.shape[1], LANES), jnp.float32),
            pltpu.VMEM(density.shape, jnp.float32),
            pltpu.VMEM((slabs, 1, LANES), jnp.float32),
            pltpu.VMEM((2 * cols, 1, LANES), jnp.float32),
            dma((n_in,)),
            dma((slabs // 2, 2)), dma((slabs // 2, 2)),
            dma((slabs // 2, 2)), dma((slabs // 2, 2)),
            dma((FAN, slabs // 2)), dma((FAN, slabs // 2)),
            dma((2,)), dma((2,)),
            dma((2,)), dma((2,)),
            dma((slabs,)), dma((slabs,)),
            dma((2 * cols,)), dma((2 * cols,)),
            dma,
        ],
        compiler_params=pltpu.CompilerParams(collective_id=0, has_side_effects=True),
    )(*operands)
    return field, energy.reshape(1)


def solution(mesh):
    split_all = ("grp", "slab", "blk", "sub")
    in_specs = (
        P(split_all), P(split_all), P(split_all), P(None, split_all), P(split_all), P(split_all), P(),
        P(("grp", "slab"), "blk", "sub"),
    )
    out_specs = (P(("grp", "slab"), "blk", "sub"), P("grp"))
    return jax.shard_map(on_device, mesh=mesh, in_specs=in_specs, out_specs=out_specs, check_vma=False)
```

```python
import functools

import jax
import jax.numpy as jnp
import numpy as np
from jax import lax
from jax.experimental import pallas as pl
from jax.experimental.pallas import tpu as pltpu
from jax.sharding import PartitionSpec as P

G0X = 64
G0Y = 128
G0Z = 128
FINE_X = 256
FINE_Y = 256
FINE_Z = 256
BQ = 256
LEVELS = 4
LANES = 128
SPAN = 256
ROWS = 8
FAN = 2
HALO = 16
spread_width = 1.25
MESH = pl.DeviceIdType.MESH

ORDER = ((0, 2, 1, 3), (0, 1, 2), (0, 1), (0,))
SETS = (
    ((3, 0), ((3, 0, 1.0), (2, 0, 4.0), (1, 0, 9.0), (0, 0, 16.0))),
    ((2, 1), ((2, 1, 1.0), (0, 1, 4.0))),
    ((1, 1), ((1, 1, 1.0),)),
    ((1, 2), ((1, 2, 1.0),)),
    ((0, 1), ((0, 2, 1.0),)),
    ((0, 3), ((0, 3, 1.0),)),
)


def coarse_cells(base, level):
    return base * (4 - level) // 4


def exponent(cells):
    return -0.5 * np.log2(np.e) / spread_width**2 * (cells / 2.0**32) ** 2


class Plan:
    def __init__(self, slabs, cols, rows_x, rows_y, rows_z):
        self.slabs, self.cols = slabs, cols
        self.rows = (rows_x, rows_y, rows_z)
        self.gx = [coarse_cells(G0X, l) for l in range(LEVELS)]
        self.gy = [coarse_cells(G0Y, l) for l in range(LEVELS)]
        self.gz = [coarse_cells(G0Z, l) for l in range(LEVELS)]
        self.nx = [g // slabs + 1 for g in self.gx]
        self.ny = [g // cols for g in self.gy]
        self.main = [a * b for a, b in zip(self.nx, self.ny)]
        self.block = [m + HALO for m in self.main]
        self.start = [sum(self.block[:l]) for l in range(LEVELS)]
        self.total = sum(self.block)
        self.xrow = [sum(self.nx[:l]) for l in range(LEVELS)]
        self.yrow = [sum(self.ny[:l]) for l in range(LEVELS)]
        self.zrow = [sum(self.gz[:l]) for l in range(LEVELS)]
        self.yset, self.zset = self.ny[-1], self.gz[-1]
        self.ytable = 2 * HALO
        self.ztable = self.ytable + len(SETS) * self.yset

    def y_nodes(self, l):
        m = LEVELS - l
        return [m * k + s for s in ORDER[l] for k in range(self.yset)]

    def node_table(self):
        def frac(node, cells):
            return (2 * node * 2**32 + cells) // (2 * cells)

        flat = [frac(r, g) for g, n in zip(self.gx, self.nx) for r in range(n)]
        flat += [0] * (HALO - len(flat))
        flat += [frac(c, g) for g, n, c in zip(self.gy, self.nx, self.ny) for _ in range(n)]
        flat += [0] * (2 * HALO - len(flat))
        for cells, count in ((self.gy, self.yset), (self.gz, self.zset)):
            for (l, s), _ in SETS:
                flat += [frac((LEVELS - l) * k + s, cells[l]) for k in range(count)]
        flat = np.array(flat, np.int64) + 2**31
        flat = ((flat + 2**31) % 2**32 - 2**31).astype(np.int32)
        return np.repeat(flat[:, None], LANES, axis=1)

    def factor_table(self):
        k = [exponent(g) for g, n in zip(self.gx, self.nx) for _ in range(n)]
        h = [exponent(g) for g, n in zip(self.gy, self.nx) for _ in range(n)]
        pad = [0.0] * (HALO - len(k))
        return np.repeat(np.array(k + pad + h + pad, np.float32)[:, None], LANES, axis=1)

    def y_matrix(self, l):
        fine = self.rows[1]
        nx, ny, main = self.nx[l], self.ny[l], self.main[l]
        b = np.arange(fine)[:, None]
        y = np.array(self.y_nodes(l) + [ny])[None, :]
        hat = np.maximum(0.0, 1.0 - np.abs(y - b * self.gy[l] / FINE_Y))
        out = np.zeros((nx * fine, self.block[l]), np.float32)
        for x in range(nx):
            out[x * fine : (x + 1) * fine, x * ny : (x + 1) * ny] = hat[:, :ny]
            out[x * fine : (x + 1) * fine, main + self.xrow[l] + x] = hat[:, ny]
        return out

    def x_matrix(self, l):
        a = np.arange(self.rows[0])[:, None]
        x = np.arange(self.nx[l])[None, :]
        return np.maximum(0.0, 1.0 - np.abs(x - a * self.gx[l] / FINE_X))

    def constants(self):
        twice = lambda m: jnp.asarray(np.concatenate([m, m], axis=1), jnp.bfloat16)
        down = [twice(self.y_matrix(l)) for l in range(LEVELS)]
        up = [twice(self.y_matrix(l).T) for l in range(LEVELS)]
        return [jnp.asarray(self.node_table()), jnp.asarray(self.factor_table())] + down + up


def split(value):
    high = value.astype(jnp.bfloat16)
    low = (value - high.astype(jnp.float32)).astype(jnp.bfloat16)
    return high, low


def kernel(plan, n_in, *refs):
    hbm, refs = refs[:n_in], refs[n_in:]
    field, energy, refs = refs[0], refs[1], refs[2:]
    held_in, refs = refs[:n_in], refs[n_in:]
    (
        buf, planes, wz, wx, acc, from_x, other, dual, dual_other, pz, t2, field_v, ez, ex,
        in_sem, zs_sem, zr_sem, xs_sem, xr_sem, ps_sem, pr_sem, ns_sem, nr_sem, es_sem, er_sem, fs_sem, fr_sem, o_sem,
    ) = refs
    cx, cy, cz, off, charge, count, amp, dens_v, nodes, factors = held_in[:10]
    down, up = held_in[10 : 10 + LEVELS], held_in[10 + LEVELS :]
    slabs, cols = plan.slabs, plan.cols
    half = slabs // 2
    reach = half // 2
    me = lax.axis_index("slab")
    col = lax.axis_index("blk")
    core = lax.axis_index("sub")
    beside = 1 - 2 * lax.rem(col, 2)
    wide = 2 * BQ
    fine_y = plan.rows[1]

    def at(ds, dc, dk):
        return {
            "slab": lax.rem(me + slabs + ds, slabs),
            "blk": lax.rem(col + cols + dc, cols),
            "sub": lax.rem(core + dk, 2),
        }

    order = [0]
    for d in range(1, half):
        order += [d, -d]
    order.append(half)
    others = [(dc, dk) for dc in range(cols) for dk in range(2)][1:]

    barrier = pltpu.get_barrier_semaphore()
    near = order[1 : 2 * reach] + [reach, -reach]
    near = [d for i, d in enumerate(near) if d not in near[:i]]
    for ds in near:
        pl.semaphore_signal(barrier, inc=1, device_id=at(ds, 0, 0), device_id_type=MESH)
    for dc, dk in others:
        pl.semaphore_signal(barrier, inc=1, device_id=at(0, dc, dk), device_id_type=MESH)

    loads = [pltpu.make_async_copy(hbm[i], held_in[i], in_sem.at[i]) for i in range(n_in)]
    for load in loads:
        load.start()
    for i in range(6):
        loads[i].wait()

    lane = lax.broadcasted_iota(jnp.int32, (1, BQ), 1)
    live = jnp.where(lane < count[...], 1.0, 0.0).astype(jnp.float32)
    buf[0, 0, 0:1, 0:BQ] = charge[...] * live
    buf[0, 0, 1:2, 0:BQ] = cx[...].astype(jnp.float32) + off[0:1, :]
    buf[0, 0, 2:3, 0:BQ] = cy[...].astype(jnp.float32) + off[1:2, :]
    buf[0, 0, 3:4, 0:BQ] = cz[...].astype(jnp.float32) + off[2:3, :]

    pl.semaphore_wait(barrier, len(near) + len(others))

    def slot(j, part):
        return buf.at[0, j, :, pl.ds(part * BQ, BQ)]

    def z_copy(src, j, part, ds):
        return pltpu.make_async_remote_copy(
            src_ref=src, dst_ref=slot(j, part), send_sem=zs_sem.at[j, part], recv_sem=zr_sem.at[j, part],
            device_id=at(ds, 0, 0), device_id_type=MESH,
        )

    for k in range(2 * reach, 0, -1):
        z_copy(slot(0, 0), k // 2, k % 2, -order[k]).start()

    def x_copy(p, j):
        return pltpu.make_async_remote_copy(
            src_ref=buf.at[0, j], dst_ref=buf.at[p, j], send_sem=xs_sem.at[p, j], recv_sem=xr_sem.at[p, j],
            device_id=at(0, -(cols // FAN), 0), device_id_type=MESH,
        )

    acc[...] = jnp.zeros_like(acc)
    planes[1] = jnp.zeros(planes.shape[1:], planes.dtype)
    wz[1] = jnp.zeros(wz.shape[1:], wz.dtype)

    row = lax.broadcasted_iota(jnp.int32, (LANES, LANES), 0)
    fine = lax.broadcasted_iota(jnp.int32, (LANES, LANES), 1) + core * LANES
    for l in range(LEVELS):
        g = plan.gz[l]
        place = row // plan.zset
        part = (place % 2) * 2 + place // 2 if l == 0 else place
        node = (row % plan.zset) * (LEVELS - l) + part
        moved = node * FINE_Z - fine * g
        moved = jnp.where(moved < 0, moved + g * FINE_Z, moved)
        moved = jnp.where(moved * 2 >= g * FINE_Z, moved - g * FINE_Z, moved)
        hat = jnp.maximum(0.0, 1.0 - jnp.abs(moved.astype(jnp.float32)) * (1.0 / FINE_Z))
        hat = jnp.where(row < g, hat, 0.0).astype(jnp.bfloat16)
        pz[l, 0:LANES, :] = hat
        pz[l, LANES:, :] = hat

    for i in range(6, n_in):
        loads[i].wait()
    for l in range(LEVELS):
        hats = plan.x_matrix(l)
        for x in range(plan.nx[l]):
            value = None
            for a in range(plan.rows[0]):
                if hats[a, x] > 0.0:
                    term = float(hats[a, x]) * dens_v[a]
                    value = term if value is None else value + term
            at_x = (plan.xrow[l] + x) * fine_y
            t2[at_x : at_x + fine_y, :] = value * amp[l]
        start, rows = plan.start[l], plan.block[l]
        along = t2[plan.xrow[l] * fine_y : (plan.xrow[l] + plan.nx[l]) * fine_y, :]
        on_y = jnp.dot(up[l][...], jnp.concatenate(split(along), axis=0), preferred_element_type=jnp.float32)
        both = lax.dot_general(
            jnp.concatenate(split(on_y), axis=0), pz[l, 0:LANES, :], (((1,), (1,)), ((), ())),
            preferred_element_type=jnp.float32,
        )
        dual[0, start : start + rows, :] = both[:rows] + both[rows:]

    def swap(k, src, dst):
        return pltpu.make_async_remote_copy(
            src_ref=src, dst_ref=dst, send_sem=ps_sem.at[k], recv_sem=pr_sem.at[k],
            device_id=at(0, 0, 1), device_id_type=MESH,
        )

    def pass_beside(k, src, dst):
        return pltpu.make_async_remote_copy(
            src_ref=src, dst_ref=dst, send_sem=ns_sem.at[k], recv_sem=nr_sem.at[k],
            device_id=at(0, beside, 0), device_id_type=MESH,
        )

    swap(0, dual.at[0], dual_other).start()

    scale = 2.0**32
    top = 2.0**31 - 128.0

    def fixed(line, cells):
        moved = jnp.minimum((line - 0.5 * cells) * (scale / cells), top)
        return moved.astype(jnp.int32)

    def broad(table):
        return jnp.concatenate([table] * (SPAN // LANES), axis=1)

    def weigh(p, j, s):
        for c in range(0, wide, SPAN):
            lanes = slice(c, c + SPAN)
            chunk = buf[p, j, :, lanes]
            ux = fixed(chunk[1:2, :], G0X) - me * (2**32 // slabs)
            uy = fixed(chunk[2:3, :], G0Y)
            uz = fixed(chunk[3:4, :], G0Z)

            def squared(first, rows, at_line, factor):
                wrapped = (broad(nodes[first : first + rows, :]) - at_line).astype(jnp.float32)
                return wrapped * wrapped * factor

            for i, ((l0, _), uses) in enumerate(SETS):
                for r in range(0, plan.zset, ROWS):
                    power = squared(plan.ztable + i * plan.zset + r, ROWS, uz, exponent(plan.gz[l0]))
                    for l, place, times in uses:
                        value = jnp.exp2(power if times == 1.0 else power * times).astype(jnp.bfloat16)
                        to = plan.zrow[l] + place * plan.zset + r
                        wz[s, to : to + ROWS, lanes] = value
            weighted = chunk[0:1, :] * jnp.exp2(squared(0, HALO, ux, broad(factors[0:HALO, :])))
            wx[s, :, lanes] = weighted
            for r in range(FAN):
                uy_r = uy - (col + r * beside) * (2**32 // cols)
                along_y = [[None] * len(ORDER[l]) for l in range(LEVELS)]
                for i, ((l0, _), uses) in enumerate(SETS):
                    power = squared(plan.ytable + i * plan.yset, plan.yset, uy_r, exponent(plan.gy[l0]))
                    for l, place, times in uses:
                        along_y[l][place] = jnp.exp2(power if times == 1.0 else power * times)
                last = jnp.exp2(squared(HALO, HALO, uy_r, broad(factors[HALO : 2 * HALO, :])))
                edge = (weighted * last).astype(jnp.bfloat16)
                for l in range(LEVELS):
                    start, main = FAN * plan.start[l] + r * plan.block[l], plan.main[l]
                    planes[s, start + main : start + main + HALO, lanes] = edge
                    tiles = [
                        wx[s, plan.xrow[l] + x : plan.xrow[l] + x + 1, lanes] * on_y
                        for x in range(plan.nx[l]) for on_y in along_y[l]
                    ]
                    for t, tile in enumerate(tiles):
                        to = start + t * plan.yset
                        planes[s, to : to + plan.yset, lanes] = tile.astype(jnp.bfloat16)

    def gather_in(s):
        for l in range(LEVELS):
            start, rows = plan.start[l], plan.block[l]
            terms = lax.dot_general(
                planes[s, FAN * start : FAN * (start + rows), :], wz[s, plan.zrow[l] : plan.zrow[l] + plan.gz[l], :],
                (((1,), (1,)), ((), ())), preferred_element_type=jnp.float32,
            )
            for r in range(FAN):
                acc[r, start : start + rows, 0 : plan.gz[l]] += terms[r * rows : (r + 1) * rows]

    def arrive(j):
        pair = half // 2

        @pl.when(j > 0)
        def _():
            z_copy(slot(0, 0), j, 0, 1).wait_recv()

        z_copy(slot(0, 0), j, 1, 1).wait_recv()

        @pl.when((j > 0) & (j < pair))
        def _():
            z_copy(slot(j, 0), j + pair, 0, reach).start()

        @pl.when(j < pair)
        def _():
            z_copy(slot(j, 1), j + pair, 1, -reach).start()

        x_copy(1, j).start()

        @pl.when(j == 1)
        def _():
            swap(0, dual.at[0], dual_other).wait()
            dual[0] = dual[0] + dual_other[...]

        @pl.when(j == pair - 1)
        def _():
            pass_beside(0, dual.at[0], dual.at[1]).start()

    steps = half // 2
    far = steps // 2

    @pl.loop(0, steps * FAN)
    def _(t):
        side, place = lax.div(t, far), lax.rem(t, far)
        p, m = lax.rem(side, FAN), lax.div(side, FAN) * far + place

        @pl.when((t == 0) | (t == FAN * far - 1))
        def _():
            first = jnp.where(t == 0, 0, 2 * far)

            @pl.loop(0, 2 * far)
            def _(j):
                arrive(first + j)

        @pl.when(p > 0)
        def _():
            x_copy(1, 2 * m).wait_recv()
            x_copy(1, 2 * m + 1).wait_recv()

        gather_in(1)
        weigh(p, 2 * m, 0)
        gather_in(0)
        weigh(p, 2 * m + 1, 1)

    gather_in(1)
    pass_beside(1, acc.at[1], from_x).start()
    pass_beside(0, dual.at[0], dual.at[1]).wait_recv()
    ez[0] = jnp.sum(acc[0] * dual[0] + acc[1] * dual[1], axis=0, keepdims=True)

    def e_copy(k):
        return pltpu.make_async_remote_copy(
            src_ref=ez.at[0], dst_ref=ez.at[k], send_sem=es_sem.at[k], recv_sem=er_sem.at[k],
            device_id=at(-order[k], 0, 0), device_id_type=MESH,
        )

    for k in range(slabs - 1, 0, -1):
        e_copy(k).start()
    pass_beside(1, acc.at[1], from_x).wait_recv()
    acc[0] = acc[0] + from_x[...]
    swap(1, acc.at[0], other).start()
    for k in range(1, slabs):
        e_copy(k).wait_recv()
    ex[0] = jnp.sum(ez[...], axis=0)

    def f_copy(k):
        dc, dk = others[k - 1]
        return pltpu.make_async_remote_copy(
            src_ref=ex.at[0], dst_ref=ex.at[k], send_sem=fs_sem.at[k], recv_sem=fr_sem.at[k],
            device_id=at(0, -dc, dk), device_id_type=MESH,
        )

    for k in range(len(others), 0, -1):
        f_copy(k).start()

    swap(1, acc.at[0], other).wait_recv()

    for l in range(LEVELS):
        start, rows = plan.start[l], plan.block[l]
        cube = acc[0, start : start + rows, :] + other[start : start + rows, :]
        along_z = jnp.dot(jnp.concatenate(split(cube), axis=1), pz[l], preferred_element_type=jnp.float32)
        t2[plan.xrow[l] * fine_y : (plan.xrow[l] + plan.nx[l]) * fine_y, :] = amp[l] * jnp.dot(
            down[l][...], jnp.concatenate(split(along_z), axis=0), preferred_element_type=jnp.float32
        )
    for a in range(plan.rows[0]):
        value = None
        for l in range(LEVELS):
            hat = plan.x_matrix(l)[a]
            for x in range(plan.nx[l]):
                if hat[x] > 0.0:
                    at_x = (plan.xrow[l] + x) * fine_y
                    term = float(hat[x]) * t2[at_x : at_x + fine_y, :]
                    value = term if value is None else value + term
        field_v[a] = value
    store = pltpu.make_async_copy(field_v, field, o_sem)
    store.start()

    for k in range(1, slabs):
        z_copy(slot(0, 0), k // 2, k % 2, 1).wait_send()
        e_copy(k).wait_send()

    @pl.loop(0, half)
    def _(j):
        x_copy(1, j).wait_send()

    pass_beside(0, dual.at[0], dual.at[1]).wait_send()
    pass_beside(1, acc.at[1], from_x).wait_send()
    swap(1, acc.at[0], other).wait_send()
    store.wait()
    for k in range(1, len(others) + 1):
        f_copy(k).wait_recv()
    energy[0, 0] = jnp.sum(jnp.sum(ex[...], axis=0)) * (1.0 / (FINE_X * FINE_Y * FINE_Z))
    for k in range(1, len(others) + 1):
        f_copy(k).wait_send()


def on_device(cell_x, cell_y, cell_z, offsets, charge, block_count, level_amplitude, density):
    slabs, cols = lax.axis_size("slab"), lax.axis_size("blk")
    plan = Plan(slabs, cols, *density.shape)
    slots = cell_x.shape[0]
    operands = [
        cell_x.reshape(1, slots), cell_y.reshape(1, slots), cell_z.reshape(1, slots), offsets,
        charge.reshape(1, slots), block_count.reshape(1, 1), level_amplitude, density, *plan.constants(),
    ]
    n_in = len(operands)
    spaces = [pltpu.VMEM] * 6 + [pltpu.SMEM] + [pltpu.VMEM] * (n_in - 7)
    smem = pl.BlockSpec(memory_space=pltpu.SMEM)
    anywhere = pl.BlockSpec(memory_space=pl.ANY)
    dma = pltpu.SemaphoreType.DMA
    field, energy = pl.pallas_call(
        functools.partial(kernel, plan, n_in),
        out_shape=(jax.ShapeDtypeStruct(density.shape, jnp.float32), jax.ShapeDtypeStruct((1, 1), jnp.float32)),
        in_specs=[anywhere] * n_in,
        out_specs=(anywhere, smem),
        scratch_shapes=[space(o.shape, o.dtype) for space, o in zip(spaces, operands)]
        + [
            pltpu.VMEM((FAN, slabs // 2, 4, 2 * BQ), jnp.float32),
            pltpu.VMEM((2, FAN * plan.total, 2 * BQ), jnp.bfloat16),
            pltpu.VMEM((2, sum(plan.gz), 2 * BQ), jnp.bfloat16),
            pltpu.VMEM((2, HALO, 2 * BQ), jnp.float32),
            pltpu.VMEM((FAN, plan.total, LANES), jnp.float32),
            pltpu.VMEM((plan.total, LANES), jnp.float32),
            pltpu.VMEM((plan.total, LANES), jnp.float32),
            pltpu.VMEM((FAN, plan.total, LANES), jnp.float32),
            pltpu.VMEM((plan.total, LANES), jnp.float32),
            pltpu.VMEM((LEVELS, 2 * LANES, LANES), jnp.bfloat16),
            pltpu.VMEM((sum(plan.nx) * density.shape[1], LANES), jnp.float32),
            pltpu.VMEM(density.shape, jnp.float32),
            pltpu.VMEM((slabs, 1, LANES), jnp.float32),
            pltpu.VMEM((2 * cols, 1, LANES), jnp.float32),
            dma((n_in,)),
            dma((slabs // 2, 2)), dma((slabs // 2, 2)),
            dma((FAN, slabs // 2)), dma((FAN, slabs // 2)),
            dma((2,)), dma((2,)),
            dma((2,)), dma((2,)),
            dma((slabs,)), dma((slabs,)),
            dma((2 * cols,)), dma((2 * cols,)),
            dma,
        ],
        compiler_params=pltpu.CompilerParams(collective_id=0, has_side_effects=True),
    )(*operands)
    return field, energy.reshape(1)


def solution(mesh):
    split_all = ("grp", "slab", "blk", "sub")
    in_specs = (
        P(split_all), P(split_all), P(split_all), P(None, split_all), P(split_all), P(split_all), P(),
        P(("grp", "slab"), "blk", "sub"),
    )
    out_specs = (P(("grp", "slab"), "blk", "sub"), P("grp"))
    return jax.shard_map(on_device, mesh=mesh, in_specs=in_specs, out_specs=out_specs, check_vma=False)
```
